32 devices in a mesh: row: 4 (over z), col: 4 (over y, x), layer: 2 (over core).
Axes of the slice: x: 2, y: 2, z: 4, core: 2. Of those that a mesh axis runs over, the one named last changes fastest.
Arguments:
- expression: bfloat16 [6144, 1024], P(('row', 'col'), 'layer'), may hold values from -240 to 240
Outputs:
- connectivity: float32 [6144], P(('row', 'col', 'layer'))
The draws below stay inside these ranges and needn't reach their ends.
All inputs are finite; a program needn't handle non-finite values.
Results may differ from the reference program's by a relative error of at most 0.00048.
Values may be sent and summed in bfloat16 or wider, within the bound.
A program may use at most 64 MiB of HBM per device.

```python
import math
import jax
import jax.numpy as jnp
from jax import lax

S = 1024
G = 6144


module_count = 384


membership = 3


def draw_expression(key, part):
    keys = jax.random.split(key, 7)
    modules = jax.random.randint(keys[0], (G, membership), 0, module_count)
    loading = jax.random.uniform(keys[1], (G, membership), jnp.float32, -1.0, 1.0)
    factor = jax.random.truncated_normal(keys[2], -3.0, 3.0, (module_count, S), jnp.float32)
    white = jax.random.truncated_normal(keys[3], -4.0, 4.0, (G, S), jnp.float32)
    mixing = jax.random.truncated_normal(keys[6], -4.0, 4.0, (S, S), jnp.float32) / jnp.sqrt(jnp.float32(S))
    spread = jnp.exp(jax.random.uniform(keys[4], (G,), jnp.float32, jnp.log(0.5), jnp.log(2.0)))
    offset = jax.random.uniform(keys[5], (G,), jnp.float32, -3.0, 3.0)
    exponent = 0.3
    decay = (1.0 + jnp.arange(S).astype(jnp.float32)) ** (-exponent)
    decay = decay / jnp.sqrt(jnp.mean(decay * decay))
    noise = jnp.dot(white * decay[None, :], mixing, precision=lax.Precision.HIGHEST)
    noise = jnp.clip(noise, -5.0, 5.0)
    columns = jnp.arange(module_count)
    load_matrix = jnp.zeros((G, module_count), jnp.float32)
    for member in range(membership):
        picked = (modules[:, member][:, None] == columns[None, :]).astype(jnp.float32)
        load_matrix = load_matrix + picked * loading[:, member][:, None]
    signal = jnp.dot(load_matrix, factor, precision=lax.Precision.HIGHEST)
    weights = 1.0 + 2.0 * jnp.arange(S).astype(jnp.float32) / (S - 1)
    values = offset[:, None] + spread[:, None] * weights[None, :] * (noise + 1.5 * signal)
    return values.astype(jnp.bfloat16)


def setup_inputs(seed: int = 0) -> dict:
    key_of = jax.random.split(jax.random.key(seed), 2)
    return {
        "expression": draw_expression(jax.random.fold_in(key_of[1], 71), 0),
    }


epsilon = 1e-05

def adjacency(correlation):
    shifted = (1.0 + correlation) * 0.5
    square = shifted * shifted
    fourth = square * square
    eighth = fourth * fourth
    return eighth * fourth

def reference(expression):
    values = expression.astype(jnp.float32)
    total = lax.optimization_barrier(jnp.sum(values, axis=1))
    squares = lax.optimization_barrier(jnp.sum(values * values, axis=1))
    average = total / S
    variance = squares / S - average * average
    scaled = ((values - average[:, None]) * lax.rsqrt(variance + epsilon)[:, None]).astype(jnp.bfloat16)
    block_rows = math.gcd(G, 1024)
    grouped = scaled.reshape(G // block_rows, block_rows, S)

    def one_block(segment):
        tile_sum = lax.dot_general(segment, scaled, (((1,), (1,)), ((), ())), preferred_element_type=jnp.float32)
        return lax.optimization_barrier(jnp.sum(adjacency(tile_sum / S), axis=1))
    totals = lax.map(one_block, grouped).reshape(G)
    return totals - 1.0
```

```python
import functools

import jax
import jax.numpy as jnp
from jax import lax
from jax.experimental import pallas as pl
from jax.experimental.pallas import tpu as pltpu
from jax.sharding import PartitionSpec as P

MESH = pl.DeviceIdType.MESH
epsilon = 1e-05


def flip(c, k):
    bit = 1
    while bit <= k:
        if k & bit:
            c = c + bit - 2 * bit * lax.rem(lax.div(c, bit), 2)
        bit *= 2
    return c


def kernel(rows, cols, x_ref, out_ref, raw, own, panel, far_raw, far, pacc, racc, psrc, pdst, rsrc, rdst,
           in_sem, ex_sem, ps_sem, pr_sem, zs_sem, zr_sem, xs_sem, xr_sem, qs_sem, qr_sem, ts_sem, tr_sem):
    p, c, l = lax.axis_index("row"), lax.axis_index("col"), lax.axis_index("layer")
    genes, part = x_ref.shape
    half = genes // 2
    samples = 2 * part
    depth, pieces, piece = far.shape[0], far.shape[1], far.shape[2]
    other = 1 - l
    order = [k for k in range(cols) if k != 3] + [3]
    last = cols - 1

    def rows_of(first, stop):
        return pl.ds(first * half, (stop - first) * half)

    def remote(src, dst, send, recv, device):
        return pltpu.make_async_remote_copy(
            src_ref=src, dst_ref=dst, send_sem=send, recv_sem=recv, device_id=device, device_id_type=MESH
        )

    load = pltpu.make_async_copy(x_ref, raw.at[l], in_sem)
    load.start()

    barrier = pltpu.get_barrier_semaphore()
    greeted = [(lax.rem(p + r, rows), c, h) for r in range(1, rows) for h in range(2)]
    greeted += [(p, flip(c, k), l) for k in range(1, cols)] + [(p, c, other)]
    for device in greeted:
        pl.semaphore_signal(barrier, inc=1, device_id=device, device_id_type=MESH)
    pacc[...] = jnp.zeros_like(pacc)
    racc[...] = jnp.zeros_like(racc)
    load.wait()
    pl.semaphore_wait(barrier, len(greeted))

    odd = lax.rem(lax.rem(p, depth), 2) == 1
    is_low = p < depth
    sends_last = odd == is_low
    receives_last = odd != is_low

    def far_copy(d, i):
        at = pl.ds(pl.multiple_of(i * piece, piece), piece)
        return remote(raw.at[l, at], far_raw.at[d, i, l], zs_sem.at[d, i], zr_sem.at[d, i],
                      (lax.rem(p + d + 1, rows), c, l))

    def relay(d, i):
        return remote(far_raw.at[d, i, l], far_raw.at[d, i, l], xs_sem.at[d, i], xr_sem.at[d, i], (p, c, other))

    for d in range(depth - 1):
        for i in range(pieces):
            far_copy(d, i).start()

    @pl.when(sends_last)
    def _():
        for i in range(pieces):
            far_copy(depth - 1, i).start()

    exchange = remote(raw.at[l], raw.at[l], ex_sem.at[0], ex_sem.at[1], (p, c, other))
    exchange.start()
    exchange.wait_recv()

    step = 32

    def scale(low, high):
        low, high = low.astype(jnp.float32), high.astype(jnp.float32)
        total = jnp.sum(low, axis=1, keepdims=True) + jnp.sum(high, axis=1, keepdims=True)
        squares = jnp.sum(low * low + high * high, axis=1, keepdims=True)
        average = total / samples
        variance = squares / samples - average * average
        gain = lax.rsqrt(variance + epsilon)
        return (((low - average) * gain).astype(jnp.bfloat16), ((high - average) * gain).astype(jnp.bfloat16))

    def standardize(h):
        for i in range(half // step):
            at = pl.ds(pl.multiple_of(h * half + i * step, step), step)
            low, high = scale(raw[0, at, :], raw[1, at, :])
            own[at, 0:part] = low
            own[at, part:samples] = high

    def standardize_far(d, i):
        for j in range(piece // step):
            at = pl.ds(j * step, step)
            low, high = scale(far_raw[d, i, 0, at, :], far_raw[d, i, 1, at, :])
            far[d, i, at, 0:part] = low
            far[d, i, at, part:samples] = high

    standardize(l)
    mine_at = pl.ds(pl.multiple_of(l * half, half), half)
    cut = half // 2

    def panel_copy(k, s):
        at = pl.ds(pl.multiple_of(l * half + s * cut, cut), cut)
        return remote(own.at[at], panel.at[pl.ds(order.index(k) * half + s * cut, cut)], ps_sem.at[k - 1, s], pr_sem.at[k - 1, s],
                      (p, flip(c, k), l))

    def pass_on(s):
        source, target = (2, 1) if s == 0 else (1, 2)
        return remote(panel.at[pl.ds(source * half + s * cut, cut)], panel.at[pl.ds(last * half + s * cut, cut)],
                      ps_sem.at[2, s], pr_sem.at[2, s], (p, flip(c, target), l))

    direct = [k for k in range(1, cols) if k != 3]
    panel_copies = {(k, s): panel_copy(k, s) for k in direct for s in range(2)}
    panel_copies.update({(3, s): pass_on(s) for s in range(2)})
    for k, s in [(1, 1), (2, 0), (1, 0), (2, 1)] + [(k, s) for k in direct[2:] for s in range(2)]:
        panel_copies[k, s].start()

    standardize(other)
    panel[rows_of(0, 1), :] = own[mine_at, :]

    def adjacency(at, block):
        product = lax.dot_general(
            panel[at, :], block, (((1,), (1,)), ((), ())), preferred_element_type=jnp.float32
        )
        shifted = product * (0.5 / samples) + 0.5
        square = shifted * shifted
        fourth = square * square
        eighth = fourth * fourth
        return eighth * fourth

    def own_pairs(first, stop):
        at = rows_of(first, stop)
        value = adjacency(at, own[...])
        lanes = value[:, 0:128]
        for j in range(1, genes // 128):
            lanes = lanes + value[:, j * 128:(j + 1) * 128]
        pacc[at, :] += lanes

    def far_pairs(first, stop, e):
        d, i = event(e)
        at = rows_of(first, stop)
        value = adjacency(at, far[d, i])
        pacc[at, :] += value
        racc[d, i] += jnp.sum(value.reshape(value.shape[0] // 8, 8, piece), axis=0)

    count = pieces * jnp.where(receives_last, depth, depth - 1)

    def event(e):
        return lax.div(e, pieces), lax.rem(e, pieces)

    own_pairs(0, 1)
    for s in range(2):
        panel_copies[2 - s, s].wait_recv()
        panel_copies[3, s].start()

    def take(e):
        d, i = event(e)
        far_copy(d, i).wait_recv()
        relay(d, i).start()

    def ready(e):
        d, i = event(e)
        relay(d, i).wait_recv()
        standardize_far(d, i)

    take(0)
    ready(0)
    take(1)
    take(2)
    ready(1)
    for s in range(2):
        panel_copies[1 + s, s].wait_recv()
    for k in direct[2:]:
        for s in range(2):
            panel_copies[k, s].wait_recv()
    own_pairs(1, last)
    longer = count > 3

    @pl.when(longer)
    def _():
        take(3)

    @pl.loop(0, count - 2)
    def _(e):
        @pl.when(e > 1)
        def _():
            @pl.when(e > 3)
            def _():
                take(e)

            ready(e)

        far_pairs(0, last, e)

    for s in range(2):
        panel_copies[3, s].wait_recv()
    own_pairs(last, cols)

    @pl.loop(0, count - 2)
    def _(e):
        far_pairs(last, cols, e)

    @pl.when(longer)
    def _():
        take(count - 2)
        take(count - 1)
        ready(count - 2)

    far_pairs(0, last, count - 2)
    far_pairs(last, cols, count - 2)
    ready(count - 1)
    far_pairs(0, last, count - 1)
    far_pairs(last, cols, count - 1)

    def fold(k):
        at = order.index(k)
        turned = pacc[rows_of(at, at + 1), :].T
        return jnp.sum(turned.reshape(128 // 8, 8, half), axis=0)

    def give_back(d):
        total = jnp.concatenate([racc[d, i] for i in range(pieces)], axis=1)
        home = lax.rem(p + rows - d - 1, rows)
        for h in range(2):
            rsrc[d, h] = total[:, h * half:(h + 1) * half]
            remote(rsrc.at[d, h], rdst.at[d, l], ts_sem.at[d, h], tr_sem.at[d, l], (home, c, h)).start()

    for d in range(depth - 1):
        give_back(d)

    @pl.when(receives_last)
    def _():
        give_back(depth - 1)

    part_copies = []
    for k in range(cols - 1, 0, -1):
        psrc[k - 1] = fold(k)
        copy = remote(psrc.at[k - 1], pdst.at[k - 1], qs_sem.at[k - 1], qr_sem.at[k - 1], (p, flip(c, k), l))
        copy.start()
        part_copies.append(copy)
    total = fold(0) - 1.0 / 8
    for copy in part_copies:
        copy.wait_recv()
    for k in range(1, cols):
        total = total + pdst[k - 1]

    def back_copy(d, h):
        return remote(rsrc.at[d, h], rdst.at[d, h], ts_sem.at[d, h], tr_sem.at[d, h], (p, c, other))

    for d in range(depth - 1):
        for h in range(2):
            back_copy(d, h).wait_recv()
            total = total + rdst[d, h]

    out_ref[...] = jnp.sum(total, axis=0)

    @pl.when(sends_last)
    def _():
        extra = jnp.zeros_like(total)
        for h in range(2):
            back_copy(depth - 1, h).wait_recv()
            extra = extra + rdst[depth - 1, h]
        out_ref[...] += jnp.sum(extra, axis=0)
        for i in range(pieces):
            far_copy(depth - 1, i).wait_send()

    exchange.wait_send()
    for copy in list(panel_copies.values()) + part_copies:
        copy.wait_send()
    for d in range(depth - 1):
        for i in range(pieces):
            far_copy(d, i).wait_send()
            relay(d, i).wait_send()
        for h in range(2):
            back_copy(d, h).wait_send()

    @pl.when(receives_last)
    def _():
        for i in range(pieces):
            relay(depth - 1, i).wait_send()
        for h in range(2):
            back_copy(depth - 1, h).wait_send()


def solution(mesh):
    rows, cols = mesh.shape["row"], mesh.shape["col"]
    depth = rows // 2
    piece = 128
    dma = lambda *shape: pltpu.SemaphoreType.DMA(shape)

    def on_device(expression):
        genes, part = expression.shape
        half, samples, pieces = genes // 2, 2 * part, genes // piece
        summed = pl.pallas_call(
            functools.partial(kernel, rows, cols),
            out_shape=jax.ShapeDtypeStruct((half,), jnp.float32),
            in_specs=[pl.BlockSpec(memory_space=pl.ANY)],
            out_specs=pl.BlockSpec(memory_space=pltpu.VMEM),
            scratch_shapes=[
                pltpu.VMEM((2, genes, part), jnp.bfloat16),
                pltpu.VMEM((genes, samples), jnp.bfloat16),
                pltpu.VMEM((cols * half, samples), jnp.bfloat16),
                pltpu.VMEM((depth, pieces, 2, piece, part), jnp.bfloat16),
                pltpu.VMEM((depth, pieces, piece, samples), jnp.bfloat16),
                pltpu.VMEM((cols * half, 128), jnp.float32),
                pltpu.VMEM((depth, pieces, 8, piece), jnp.float32),
                pltpu.VMEM((cols - 1, 8, half), jnp.float32),
                pltpu.VMEM((cols - 1, 8, half), jnp.float32),
                pltpu.VMEM((depth, 2, 8, half), jnp.float32),
                pltpu.VMEM((depth, 2, 8, half), jnp.float32),
                pltpu.SemaphoreType.DMA,
                dma(2),
                dma(cols - 1, 2), dma(cols - 1, 2),
                dma(depth, pieces), dma(depth, pieces),
                dma(depth, pieces), dma(depth, pieces),
                dma(cols - 1), dma(cols - 1),
                dma(depth, 2), dma(depth, 2),
            ],
            compiler_params=pltpu.CompilerParams(collective_id=0, has_side_effects=True, vmem_limit_bytes=48000000),
        )(pltpu.with_memory_space_constraint(expression, pltpu.HBM))
        return summed

    return jax.shard_map(
        on_device,
        mesh=mesh,
        in_specs=(P(("row", "col"), "layer"),),
        out_specs=P(("row", "col", "layer")),
        check_vma=False,
    )
```

```python
import functools

import jax
import jax.numpy as jnp
from jax import lax
from jax.experimental import pallas as pl
from jax.experimental.pallas import tpu as pltpu
from jax.sharding import PartitionSpec as P

MESH = pl.DeviceIdType.MESH
epsilon = 1e-05


def flip(c, k):
    bit = 1
    while bit <= k:
        if k & bit:
            c = c + bit - 2 * bit * lax.rem(lax.div(c, bit), 2)
        bit *= 2
    return c


def is_above(c, k):
    top = 1 << (k.bit_length() - 1)
    return lax.rem(lax.div(c, top), 2) == 0


def plan(rows):
    if rows == 4:
        return [(1, 0, None), (3, 1, None), (3, 0, 1), (0, 2, None), (1, 2, None), (2, 3, None)]
    flows = []
    for d in range(1, rows // 2 + 1):
        for s in range(rows if 2 * d < rows else rows // 2):
            flows.append((s, (s + d) % rows, None))
    return flows


def kernel(rows, cols, x_ref, out_ref, praw, panel, far_raw, far, pacc, racc, psrc, pdst, rsrc, rdst,
           in_sem, ex_sem, ps_sem, pr_sem, fs_sem, fr_sem, zs_sem, zr_sem, xs_sem, qs_sem, qr_sem, ts_sem, tr_sem,
           x_ready, z_ready):
    p, c, l = lax.axis_index("row"), lax.axis_index("col"), lax.axis_index("layer")
    genes, part = x_ref.shape
    half = genes // 2
    piece = half // 2
    samples = 2 * part
    other = 1 - l
    order = [k for k in range(cols) if k != 3] + [3]
    direct = [k for k in range(1, cols) if k != 3]
    last = cols - 1
    flows = plan(rows)
    slots = {t: [f for f in flows if f[1] == t] for t in range(rows)}
    outs = {s: [f for f in flows if f[0] == s and f[2] is None] for s in range(rows)}
    back = {s: [f for f in flows if f[0] == s] for s in range(rows)}
    pairs_of = {q: sorted({f[1] for f in flows if f[0] == q} | {f[0] for f in flows if f[1] == q}) for q in range(rows)}

    def remote(src, dst, send, recv, device):
        return pltpu.make_async_remote_copy(
            src_ref=src, dst_ref=dst, send_sem=send, recv_sem=recv, device_id=device, device_id_type=MESH
        )

    def by_row(values):
        value = values[0]
        for q in range(1, rows):
            value = jnp.where(p == q, values[q], value)
        return value

    def at_row(q, condition=True):
        return pl.when(p == q)

    load = pltpu.make_async_copy(x_ref, praw.at[0, l], in_sem)
    load.start()

    barrier = pltpu.get_barrier_semaphore()

    def greet(device):
        pl.semaphore_signal(barrier, inc=1, device_id=device, device_id_type=MESH)

    greet((p, c, other))
    for k in direct:
        @pl.when(is_above(c, k))
        def _():
            greet((p, flip(c, k), l))
    for q in range(rows):
        above = [t for t in pairs_of[q] if t > q]
        if above:
            @pl.when(p == q)
            def _():
                for t in above:
                    for h in range(2):
                        greet((t, c, h))
    greetings = 1 + by_row([2 * len([t for t in pairs_of[q] if t < q]) for q in range(rows)])
    for k in direct:
        greetings = greetings + jnp.where(is_above(c, k), 0, 1)

    pacc[...] = jnp.zeros_like(pacc)
    racc[...] = jnp.zeros_like(racc)
    pl.semaphore_wait(barrier, greetings)
    for k in direct:
        @pl.when(jnp.logical_not(is_above(c, k)))
        def _():
            pl.semaphore_signal(x_ready.at[k - 1], inc=1, device_id=(p, flip(c, k), l), device_id_type=MESH)
    for t in range(rows):
        below = [f for f in slots[t] if f[2] is None and f[0] < t]
        if below:
            @pl.when(p == t)
            def _():
                for f in below:
                    for h in range(2):
                        pl.semaphore_signal(z_ready.at[outs[f[0]].index(f)], inc=1, device_id=(f[0], c, h), device_id_type=MESH)
    load.wait()

    def z_copy(f, h, i):
        source = praw.at[0, l, pl.ds(h * half + i * piece, piece)]
        return remote(source, far_raw.at[slots[f[1]].index(f), l, pl.ds(i * piece, piece)],
                      zs_sem.at[outs[f[0]].index(f), h, i], zr_sem.at[slots[f[1]].index(f), l, i], (f[1], c, h))

    def z_arrival(t, b, i):
        at = far_raw.at[t, b, pl.ds(pl.multiple_of(i * piece, piece), piece)]
        return remote(at, at, zs_sem.at[0, 0, 0], zr_sem.at[t, b, i], (p, c, other))

    def held_back(f):
        return rows == 4 and f == (1, 2, None)

    def send_row(f):
        for i in range(1 if held_back(f) else 2):
            for h in range(2):
                z_copy(f, h, i).start()

    exchange = remote(praw.at[0, l], praw.at[0, l], ex_sem.at[0], ex_sem.at[1], (p, c, other))
    exchange.start()
    for q in range(rows):
        down = [f for f in outs[q] if f[1] < q]
        if down:
            @pl.when(p == q)
            def _():
                for f in down:
                    send_row(f)

    def panel_copy(k, s):
        at = pl.ds(s * half, half)
        return remote(praw.at[0, l, at], praw.at[order.index(k), l, at], ps_sem.at[k - 1, s], pr_sem.at[k - 1, s],
                      (p, flip(c, k), l))

    def pass_on(s):
        source, target = (2, 1) if s == 0 else (1, 2)
        at = pl.ds(s * half, half)
        return remote(praw.at[order.index(source), l, at], praw.at[last, l, at], ps_sem.at[2, s], pr_sem.at[2, s],
                      (p, flip(c, target), l))

    panel_copies = {(k, s): panel_copy(k, s) for k in direct for s in range(2)}
    panel_copies.update({(3, s): pass_on(s) for s in range(2)})

    def forward(k, s):
        at = praw.at[order.index(k), l, pl.ds(s * half, half)]
        return remote(at, at, fs_sem.at[k - 1, s], fr_sem.at[k - 1, s], (p, c, other))

    first = {1: (1, 0), 2: (0, 1)}
    for k in direct:
        @pl.when(jnp.logical_not(is_above(c, k)))
        def _():
            for s in first.get(k, (0, 1)):
                panel_copies[k, s].start()
    for k in direct:
        @pl.when(is_above(c, k))
        def _():
            pl.semaphore_wait(x_ready.at[k - 1], 1)
            for s in first.get(k, (0, 1)):
                panel_copies[k, s].start()
    for q in range(rows):
        up = [f for f in outs[q] if f[1] > q]
        if up:
            @pl.when(p == q)
            def _():
                for f in up:
                    pl.semaphore_wait(z_ready.at[outs[q].index(f)], 2)
                    send_row(f)

    step = 32

    def scale(low, high):
        low, high = low.astype(jnp.float32), high.astype(jnp.float32)
        total = jnp.sum(low, axis=1, keepdims=True) + jnp.sum(high, axis=1, keepdims=True)
        squares = jnp.sum(low * low + high * high, axis=1, keepdims=True)
        average = total / samples
        variance = squares / samples - average * average
        gain = lax.rsqrt(variance + epsilon)
        return (((low - average) * gain).astype(jnp.bfloat16), ((high - average) * gain).astype(jnp.bfloat16))

    def standardize(k):
        n = order.index(k)
        for i in range(genes // step):
            low, high = scale(praw[n, 0, pl.ds(i * step, step), :], praw[n, 1, pl.ds(i * step, step), :])
            at = pl.ds(n * genes + i * step, step)
            panel[at, 0:part] = low
            panel[at, part:samples] = high

    def standardize_far(t, i):
        for j in range(piece // step):
            at = pl.ds(pl.multiple_of(i * piece + j * step, step), step)
            low, high = scale(far_raw[t, 0, at, :], far_raw[t, 1, at, :])
            far[t, at, 0:part] = low
            far[t, at, part:samples] = high

    def adjacency(block, start, stop):
        product = lax.dot_general(
            block, panel[start * genes:stop * genes, :], (((1,), (1,)), ((), ())), preferred_element_type=jnp.float32
        )
        shifted = product * (0.5 / samples) + 0.5
        square = shifted * shifted
        fourth = square * square
        eighth = fourth * fourth
        return eighth * fourth

    def own_pairs(start, stop):
        at = pl.ds(pl.multiple_of(l * half, half), half)
        value = adjacency(panel[at, :], start, stop)
        pacc[:, start * genes:stop * genes] += jnp.sum(value.reshape(half // 8, 8, value.shape[1]), axis=0)

    def far_pairs(t, i, start, stop):
        at = pl.ds(pl.multiple_of(i * piece, piece), piece)
        value = adjacency(far[t, at, :], start, stop)
        pacc[:, start * genes:stop * genes] += jnp.sum(value.reshape(piece // 8, 8, value.shape[1]), axis=0)
        lanes = value[:, 0:128]
        for j in range(1, value.shape[1] // 128):
            lanes = lanes + value[:, j * 128:(j + 1) * 128]
        racc[t, at, :] += lanes

    exchange.wait_recv()
    standardize(0)
    own_pairs(0, 1)

    relays = [f for f in flows if f[2] is not None]

    def relay_copy(f, b, i):
        t = slots[f[2]].index((f[0], f[2], None))
        at = pl.ds(i * piece, piece)
        return remote(far_raw.at[t, b, at], far_raw.at[slots[f[1]].index(f), b, at],
                      xs_sem.at[b, i], zr_sem.at[slots[f[1]].index(f), b, i], (f[1], c, l))

    def relay(i):
        for f in relays:
            @pl.when(p == f[2])
            def _():
                for b in range(2):
                    z_arrival(slots[f[2]].index((f[0], f[2], None)), b, i).wait_recv()
                    relay_copy(f, b, i).start()

    for s in range(2):
        panel_copies[2 - s, s].wait_recv()
        panel_copies[3, s].start()
        forward(2 - s, s).start()
    relay(0)
    for s in range(2):
        panel_copies[1 + s, s].wait_recv()
        forward(1 + s, s).start()
    for k in direct[2:]:
        for s in range(2):
            panel_copies[k, s].wait_recv()
            forward(k, s).start()
    relay(1)
    for f in flows:
        if held_back(f):
            @pl.when(p == f[0])
            def _():
                for h in range(2):
                    z_copy(f, h, 1).start()
    for k in direct:
        for s in range(2):
            forward(k, s).wait_recv()
        standardize(k)
    own_pairs(1, last)

    def take_far(t, i):
        passing = [f[2] for f in relays if slots[f[2]].index((f[0], f[2], None)) == t]
        if passing:
            @pl.when(p != passing[0])
            def _():
                for b in range(2):
                    z_arrival(t, b, i).wait_recv()
        else:
            for b in range(2):
                z_arrival(t, b, i).wait_recv()
        standardize_far(t, i)

    def give_back(t):
        turned = racc[t].T
        rsrc[t] = jnp.sum(turned.reshape(128 // 8, 8, half), axis=0)
        for q in range(rows):
            if t < len(slots[q]):
                @pl.when(p == q)
                def _():
                    back_copy(slots[q][t]).start()

    def back_copy(f):
        t, j = slots[f[1]].index(f), back[f[0]].index(f)
        return remote(rsrc.at[t], rdst.at[j], ts_sem.at[t], tr_sem.at[j], (f[0], c, l))

    @pl.loop(0, 2)
    def _(i):
        take_far(0, i)
        far_pairs(0, i, 0, last)

    for s in range(2):
        panel_copies[3, s].wait_recv()
        forward(3, s).start()
    for s in range(2):
        forward(3, s).wait_recv()
    standardize(3)
    own_pairs(last, cols)

    @pl.loop(0, 2)
    def _(i):
        far_pairs(0, i, last, cols)

    give_back(0)
    depth = max(len(slots[q]) for q in range(rows))
    for t in range(1, depth):
        @pl.when(by_row([len(slots[q]) for q in range(rows)]) > t)
        def _():
            @pl.loop(0, 2)
            def _(i):
                take_far(t, i)
                far_pairs(t, i, 0, cols)

            give_back(t)

    def part_copy(k, h):
        return remote(psrc.at[k, h], pdst.at[k, l], qs_sem.at[k, h], qr_sem.at[k, l], (p, flip(c, k), h))

    def part_arrival(k, b):
        return remote(psrc.at[k, b], pdst.at[k, b], qs_sem.at[k, b], qr_sem.at[k, b], (p, c, other))

    for k in [k for k in reversed(order)]:
        n = order.index(k)
        for h in range(2):
            psrc[k, h] = pacc[:, n * genes + h * half:n * genes + (h + 1) * half]
            if k:
                part_copy(k, h).start()
    part_copy(0, other).start()
    total = psrc[0, l] - 1.0 / 8
    part_arrival(0, other).wait_recv()
    total = total + pdst[0, other]
    for k in range(1, cols):
        for b in range(2):
            part_arrival(k, b).wait_recv()
            total = total + pdst[k, b]

    def back_arrival(j):
        return remote(rsrc.at[0], rdst.at[j], ts_sem.at[0], tr_sem.at[j], (p, c, other))

    n_back = by_row([len(back[q]) for q in range(rows)])
    least = min(len(back[q]) for q in range(rows))
    for j in range(least):
        back_arrival(j).wait_recv()
        total = total + rdst[j]
    psrc[0, l] = total
    for j in range(least, max(len(back[q]) for q in range(rows))):
        @pl.when(n_back > j)
        def _():
            back_arrival(j).wait_recv()
            psrc[0, l] += rdst[j]
    out_ref[...] = jnp.sum(psrc[0, l], axis=0)

    exchange.wait_send()
    for k, s in panel_copies:
        panel_copies[k, s].wait_send()
        forward(k, s).wait_send()
    for k in range(1, cols):
        for h in range(2):
            part_copy(k, h).wait_send()
    part_copy(0, other).wait_send()
    for q in range(rows):
        @pl.when(p == q)
        def _():
            for f in outs[q]:
                for h in range(2):
                    for i in range(2):
                        z_copy(f, h, i).wait_send()
            for f in relays:
                if f[2] == q:
                    for b in range(2):
                        for i in range(2):
                            relay_copy(f, b, i).wait_send()
            for f in slots[q]:
                back_copy(f).wait_send()


def solution(mesh):
    rows, cols = mesh.shape["row"], mesh.shape["col"]
    flows = plan(rows)
    depth = max(len([f for f in flows if f[1] == q]) for q in range(rows))
    fan = max(len([f for f in flows if f[0] == q]) for q in range(rows))
    dma = lambda *shape: pltpu.SemaphoreType.DMA(shape)

    def on_device(expression):
        genes, part = expression.shape
        half, samples = genes // 2, 2 * part
        bf16, f32 = jnp.bfloat16, jnp.float32
        summed = pl.pallas_call(
            functools.partial(kernel, rows, cols),
            out_shape=jax.ShapeDtypeStruct((half,), f32),
            in_specs=[pl.BlockSpec(memory_space=pl.ANY)],
            out_specs=pl.BlockSpec(memory_space=pltpu.VMEM),
            scratch_shapes=[
                pltpu.VMEM((cols, 2, genes, part), bf16),
                pltpu.VMEM((cols * genes, samples), bf16),
                pltpu.VMEM((depth, 2, half, part), bf16),
                pltpu.VMEM((depth, half, samples), bf16),
                pltpu.VMEM((8, cols * genes), f32),
                pltpu.VMEM((depth, half, 128), f32),
                pltpu.VMEM((cols, 2, 8, half), f32),
                pltpu.VMEM((cols, 2, 8, half), f32),
                pltpu.VMEM((depth, 8, half), f32),
                pltpu.VMEM((fan, 8, half), f32),
                pltpu.SemaphoreType.DMA,
                dma(2),
                dma(cols - 1, 2), dma(cols - 1, 2),
                dma(cols - 1, 2), dma(cols - 1, 2),
                dma(fan, 2, 2), dma(depth, 2, 2),
                dma(2, 2),
                dma(cols, 2), dma(cols, 2),
                dma(depth), dma(fan),
                pltpu.SemaphoreType.REGULAR((cols - 1,)),
                pltpu.SemaphoreType.REGULAR((fan,)),
            ],
            compiler_params=pltpu.CompilerParams(collective_id=0, has_side_effects=True, vmem_limit_bytes=48000000),
        )(pltpu.with_memory_space_constraint(expression, pltpu.HBM))
        return summed

    return jax.shard_map(
        on_device,
        mesh=mesh,
        in_specs=(P(("row", "col"), "layer"),),
        out_specs=P(("row", "col", "layer")),
        check_vma=False,
    )
```

```python
import functools

import jax
import jax.numpy as jnp
from jax import lax
from jax.experimental import pallas as pl
from jax.experimental.pallas import tpu as pltpu
from jax.sharding import PartitionSpec as P

MESH = pl.DeviceIdType.MESH
epsilon = 1e-05


def flip(c, k):
    bit = 1
    while bit <= k:
        if k & bit:
            c = c + bit - 2 * bit * lax.rem(lax.div(c, bit), 2)
        bit *= 2
    return c


def is_above(c, k):
    top = 1 << (k.bit_length() - 1)
    return lax.rem(lax.div(c, top), 2) == 0


def plan(rows):
    if rows == 4:
        return [(3, 1, None), (0, 1, None), (3, 0, 1), (1, 2, None), (0, 2, 1), (2, 3, None)]
    flows = []
    for d in range(1, rows // 2 + 1):
        for s in range(rows if 2 * d < rows else rows // 2):
            flows.append((s, (s + d) % rows, None))
    return flows


def kernel(rows, cols, x_ref, out_ref, praw, panel, far_raw, stack, pacc, racc, psrc, pdst, rsrc, rdst,
           in_sem, ex_sem, ps_sem, pr_sem, fs_sem, fr_sem, zs_sem, zr_sem, xs_sem, qs_sem, qr_sem, ts_sem, tr_sem,
           x_ready, z_ready):
    p, c, l = lax.axis_index("row"), lax.axis_index("col"), lax.axis_index("layer")
    genes, part = x_ref.shape
    half = genes // 2
    piece = half // 2
    samples = 2 * part
    other = 1 - l
    order = [k for k in range(cols) if k != 3] + [3]
    direct = [k for k in range(1, cols) if k != 3]
    last = cols - 1
    flows = plan(rows)
    slots = {t: [f for f in flows if f[1] == t] for t in range(rows)}
    outs = {s: [f for f in flows if f[0] == s and f[2] is None] for s in range(rows)}
    back = {s: [f for f in flows if f[0] == s] for s in range(rows)}
    pairs_of = {q: sorted({f[1] for f in flows if f[0] == q} | {f[0] for f in flows if f[1] == q}) for q in range(rows)}

    def remote(src, dst, send, recv, device):
        return pltpu.make_async_remote_copy(
            src_ref=src, dst_ref=dst, send_sem=send, recv_sem=recv, device_id=device, device_id_type=MESH
        )

    def by_row(values):
        value = values[0]
        for q in range(1, rows):
            value = jnp.where(p == q, values[q], value)
        return value

    def at_row(q, condition=True):
        return pl.when(p == q)

    load = pltpu.make_async_copy(x_ref, praw.at[0, l], in_sem)
    load.start()

    barrier = pltpu.get_barrier_semaphore()

    def greet(device):
        pl.semaphore_signal(barrier, inc=1, device_id=device, device_id_type=MESH)

    greet((p, c, other))
    for k in direct:
        @pl.when(is_above(c, k))
        def _():
            greet((p, flip(c, k), l))
    for q in range(rows):
        above = [t for t in pairs_of[q] if t > q]
        if above:
            @pl.when(p == q)
            def _():
                for t in above:
                    for h in range(2):
                        greet((t, c, h))
    greetings = 1 + by_row([2 * len([t for t in pairs_of[q] if t < q]) for q in range(rows)])
    for k in direct:
        greetings = greetings + jnp.where(is_above(c, k), 0, 1)

    pacc[...] = jnp.zeros_like(pacc)
    racc[...] = jnp.zeros_like(racc)
    pl.semaphore_wait(barrier, greetings)
    for k in direct:
        @pl.when(jnp.logical_not(is_above(c, k)))
        def _():
            pl.semaphore_signal(x_ready.at[k - 1], inc=1, device_id=(p, flip(c, k), l), device_id_type=MESH)
    for t in range(rows):
        below = [f for f in slots[t] if f[2] is None and f[0] < t]
        if below:
            @pl.when(p == t)
            def _():
                for f in below:
                    for h in range(2):
                        pl.semaphore_signal(z_ready.at[outs[f[0]].index(f)], inc=1, device_id=(f[0], c, h), device_id_type=MESH)
    load.wait()

    def z_copy(f, h, i):
        source = praw.at[0, l, pl.ds(h * half + i * piece, piece)]
        return remote(source, far_raw.at[slots[f[1]].index(f), l, pl.ds(i * piece, piece)],
                      zs_sem.at[outs[f[0]].index(f), h, i], zr_sem.at[slots[f[1]].index(f), l, i], (f[1], c, h))

    def z_arrival(t, b, i):
        at = far_raw.at[t, b, pl.ds(pl.multiple_of(i * piece, piece), piece)]
        return remote(at, at, zs_sem.at[0, 0, 0], zr_sem.at[t, b, i], (p, c, other))

    def held_back(f):
        return rows == 4 and f == (1, 2, None)

    def send_row(f):
        for i in range(1 if held_back(f) else 2):
            for h in range(2):
                z_copy(f, h, i).start()

    exchange = remote(praw.at[0, l], praw.at[0, l], ex_sem.at[0], ex_sem.at[1], (p, c, other))
    exchange.start()
    for q in range(rows):
        down = [f for f in outs[q] if f[1] < q]
        if down:
            @pl.when(p == q)
            def _():
                for f in down:
                    send_row(f)

    def panel_copy(k, s):
        at = pl.ds(s * half, half)
        return remote(praw.at[0, l, at], praw.at[order.index(k), l, at], ps_sem.at[k - 1, s], pr_sem.at[k - 1, s],
                      (p, flip(c, k), l))

    def pass_on(s):
        source, target = (2, 1) if s == 0 else (1, 2)
        at = pl.ds(s * half, half)
        return remote(praw.at[order.index(source), l, at], praw.at[last, l, at], ps_sem.at[2, s], pr_sem.at[2, s],
                      (p, flip(c, target), l))

    panel_copies = {(k, s): panel_copy(k, s) for k in direct for s in range(2)}
    panel_copies.update({(3, s): pass_on(s) for s in range(2)})

    def forward(k, s):
        at = praw.at[order.index(k), l, pl.ds(s * half, half)]
        return remote(at, at, fs_sem.at[k - 1, s], fr_sem.at[k - 1, s], (p, c, other))

    first = {1: (1, 0), 2: (0, 1)}
    for k in direct:
        @pl.when(jnp.logical_not(is_above(c, k)))
        def _():
            for s in first.get(k, (0, 1)):
                panel_copies[k, s].start()
    for k in direct:
        @pl.when(is_above(c, k))
        def _():
            pl.semaphore_wait(x_ready.at[k - 1], 1)
            for s in first.get(k, (0, 1)):
                panel_copies[k, s].start()
    for q in range(rows):
        up = [f for f in outs[q] if f[1] > q]
        if up:
            @pl.when(p == q)
            def _():
                for f in up:
                    pl.semaphore_wait(z_ready.at[outs[q].index(f)], 2)
                    send_row(f)

    step = 32

    def scale(low, high):
        low, high = low.astype(jnp.float32), high.astype(jnp.float32)
        total = jnp.sum(low, axis=1, keepdims=True) + jnp.sum(high, axis=1, keepdims=True)
        squares = jnp.sum(low * low + high * high, axis=1, keepdims=True)
        average = total / samples
        variance = squares / samples - average * average
        gain = lax.rsqrt(variance + epsilon)
        return (((low - average) * gain).astype(jnp.bfloat16), ((high - average) * gain).astype(jnp.bfloat16))

    def standardize(k, s):
        n = order.index(k)
        for i in range(half // step):
            at = pl.ds(s * half + i * step, step)
            low, high = scale(praw[n, 0, at, :], praw[n, 1, at, :])
            at = pl.ds(n * genes + s * half + i * step, step)
            panel[at, 0:part] = low
            panel[at, part:samples] = high

    def slot_at(t):
        return (1 + t) * half

    def standardize_far(t, first, stop):
        for j in range(first // step, stop // step):
            at = pl.ds(j * step, step)
            low, high = scale(far_raw[t, 0, at, :], far_raw[t, 1, at, :])
            at = pl.ds(slot_at(t) + j * step, step)
            stack[at, 0:part] = low
            stack[at, part:samples] = high

    def pairs(first, stop, start, end):
        product = lax.dot_general(
            stack[first:stop, :], panel[start * genes:end * genes, :], (((1,), (1,)), ((), ())),
            preferred_element_type=jnp.float32
        )
        shifted = product * (0.5 / samples) + 0.5
        square = shifted * shifted
        fourth = square * square
        eighth = fourth * fourth
        value = eighth * fourth
        width = value.shape[1]
        pacc[:, start * genes:end * genes] += jnp.sum(value.reshape((stop - first) // 8, 8, width), axis=0)
        skipped = max(half - first, 0)
        if first + skipped < stop:
            value = value[skipped:]
            lanes = value[:, 0:128]
            for j in range(1, width // 128):
                lanes = lanes + value[:, j * 128:(j + 1) * 128]
            racc[first + skipped - half:stop - half, :] += lanes

    exchange.wait_recv()
    for s in range(2):
        standardize(0, s)
    stack[0:half, :] = panel[pl.ds(pl.multiple_of(l * half, half), half), :]
    pairs(0, half, 0, 1)

    relays = [f for f in flows if f[2] is not None]

    def passed(f):
        return slots[f[2]].index((f[0], f[2], None))

    def relay_copy(f, b, i):
        at, t = pl.ds(i * piece, piece), slots[f[1]].index(f)
        return remote(far_raw.at[passed(f), b, at], far_raw.at[t, b, at],
                      xs_sem.at[relays.index(f), b, i], zr_sem.at[t, b, i], (f[1], c, l))

    def relay(n, i):
        for f in relays[n:n + 1]:
            @pl.when(p == f[2])
            def _():
                for b in range(2):
                    z_arrival(passed(f), b, i).wait_recv()
                    relay_copy(f, b, i).start()

    relay(1, 0)
    for s in range(2):
        panel_copies[2 - s, s].wait_recv()
        panel_copies[3, s].start()
        forward(2 - s, s).start()
    relay(0, 0)
    for s in range(2):
        forward(2 - s, s).wait_recv()
        standardize(2 - s, s)
    relay(1, 1)
    for f in flows:
        if held_back(f):
            @pl.when(p == f[0])
            def _():
                for h in range(2):
                    z_copy(f, h, 1).start()
    for s in range(2):
        panel_copies[1 + s, s].wait_recv()
        forward(1 + s, s).start()
    relay(0, 1)
    for s in range(2):
        forward(1 + s, s).wait_recv()
        standardize(1 + s, s)
    for k in direct[2:]:
        for s in range(2):
            panel_copies[k, s].wait_recv()
            forward(k, s).start()
        for s in range(2):
            forward(k, s).wait_recv()
            standardize(k, s)
    pairs(0, half, 1, last)
    for s in range(2):
        panel_copies[3, s].wait_recv()
        forward(3, s).start()

    def take_far(t, i):
        passing = [f[2] for f in relays if passed(f) == t]
        if passing:
            @pl.when(p != passing[0])
            def _():
                for b in range(2):
                    z_arrival(t, b, i).wait_recv()
        else:
            for b in range(2):
                z_arrival(t, b, i).wait_recv()

    def back_copy(f):
        t, j = slots[f[1]].index(f), back[f[0]].index(f)
        return remote(rsrc.at[t], rdst.at[j], ts_sem.at[t], tr_sem.at[j], (f[0], c, l))

    def give_back(t):
        turned = racc[t * half:(t + 1) * half, :].T
        rsrc[t] = jnp.sum(turned.reshape(128 // 8, 8, half), axis=0)
        for q in range(rows):
            if t < len(slots[q]):
                @pl.when(p == q)
                def _():
                    back_copy(slots[q][t]).start()

    depth = max(len(slots[q]) for q in range(rows))
    n_slots = by_row([len(slots[q]) for q in range(rows)])
    for t in range(1, depth):
        @pl.when(n_slots > t)
        def _():
            for i in range(2):
                take_far(t, i)
            standardize_far(t, 0, half)
            pairs(slot_at(t), slot_at(t) + half, 0, last)

    take_far(0, 0)
    standardize_far(0, 0, piece)
    pairs(half, half + piece, 0, last)
    for s in range(2):
        forward(3, s).wait_recv()
        standardize(3, s)
    pairs(0, half + piece, last, cols)
    for t in range(1, depth):
        @pl.when(n_slots > t)
        def _():
            pairs(slot_at(t), slot_at(t) + half, last, cols)
            give_back(t)

    take_far(0, 1)
    standardize_far(0, piece, half)
    pairs(half + piece, 2 * half, 0, cols)
    give_back(0)

    def part_copy(k, h):
        return remote(psrc.at[k, h], pdst.at[k, l], qs_sem.at[k, h], qr_sem.at[k, l], (p, flip(c, k), h))

    def part_arrival(k, b):
        return remote(psrc.at[k, b], pdst.at[k, b], qs_sem.at[k, b], qr_sem.at[k, b], (p, c, other))

    for k in [k for k in reversed(order)]:
        n = order.index(k)
        for h in range(2):
            psrc[k, h] = pacc[:, n * genes + h * half:n * genes + (h + 1) * half]
            if k:
                part_copy(k, h).start()
    part_copy(0, other).start()
    total = psrc[0, l] - 1.0 / 8
    part_arrival(0, other).wait_recv()
    total = total + pdst[0, other]
    for k in range(1, cols):
        for b in range(2):
            part_arrival(k, b).wait_recv()
            total = total + pdst[k, b]

    def back_arrival(j):
        return remote(rsrc.at[0], rdst.at[j], ts_sem.at[0], tr_sem.at[j], (p, c, other))

    n_back = by_row([len(back[q]) for q in range(rows)])
    least = min(len(back[q]) for q in range(rows))
    for j in range(least):
        back_arrival(j).wait_recv()
        total = total + rdst[j]
    psrc[0, l] = total
    for j in range(least, max(len(back[q]) for q in range(rows))):
        @pl.when(n_back > j)
        def _():
            back_arrival(j).wait_recv()
            psrc[0, l] += rdst[j]
    out_ref[...] = jnp.sum(psrc[0, l], axis=0)

    exchange.wait_send()
    for k, s in panel_copies:
        panel_copies[k, s].wait_send()
        forward(k, s).wait_send()
    for k in range(1, cols):
        for h in range(2):
            part_copy(k, h).wait_send()
    part_copy(0, other).wait_send()
    for q in range(rows):
        @pl.when(p == q)
        def _():
            for f in outs[q]:
                for h in range(2):
                    for i in range(2):
                        z_copy(f, h, i).wait_send()
            for f in relays:
                if f[2] == q:
                    for b in range(2):
                        for i in range(2):
                            relay_copy(f, b, i).wait_send()
            for f in slots[q]:
                back_copy(f).wait_send()


def solution(mesh):
    rows, cols = mesh.shape["row"], mesh.shape["col"]
    flows = plan(rows)
    depth = max(len([f for f in flows if f[1] == q]) for q in range(rows))
    fan = max(len([f for f in flows if f[0] == q]) for q in range(rows))
    dma = lambda *shape: pltpu.SemaphoreType.DMA(shape)

    def on_device(expression):
        genes, part = expression.shape
        half, samples = genes // 2, 2 * part
        bf16, f32 = jnp.bfloat16, jnp.float32
        summed = pl.pallas_call(
            functools.partial(kernel, rows, cols),
            out_shape=jax.ShapeDtypeStruct((half,), f32),
            in_specs=[pl.BlockSpec(memory_space=pl.ANY)],
            out_specs=pl.BlockSpec(memory_space=pltpu.VMEM),
            scratch_shapes=[
                pltpu.VMEM((cols, 2, genes, part), bf16),
                pltpu.VMEM((cols * genes, samples), bf16),
                pltpu.VMEM((depth, 2, half, part), bf16),
                pltpu.VMEM(((1 + depth) * half, samples), bf16),
                pltpu.VMEM((8, cols * genes), f32),
                pltpu.VMEM((depth * half, 128), f32),
                pltpu.VMEM((cols, 2, 8, half), f32),
                pltpu.VMEM((cols, 2, 8, half), f32),
                pltpu.VMEM((depth, 8, half), f32),
                pltpu.VMEM((fan, 8, half), f32),
                pltpu.SemaphoreType.DMA,
                dma(2),
                dma(cols - 1, 2), dma(cols - 1, 2),
                dma(cols - 1, 2), dma(cols - 1, 2),
                dma(fan, 2, 2), dma(depth, 2, 2),
                dma(max(len([f for f in flows if f[2] is not None]), 1), 2, 2),
                dma(cols, 2), dma(cols, 2),
                dma(depth), dma(fan),
                pltpu.SemaphoreType.REGULAR((cols - 1,)),
                pltpu.SemaphoreType.REGULAR((fan,)),
            ],
            compiler_params=pltpu.CompilerParams(collective_id=0, has_side_effects=True, vmem_limit_bytes=48000000),
        )(pltpu.with_memory_space_constraint(expression, pltpu.HBM))
        return summed

    return jax.shard_map(
        on_device,
        mesh=mesh,
        in_specs=(P(("row", "col"), "layer"),),
        out_specs=P(("row", "col", "layer")),
        check_vma=False,
    )
```

```python
import functools

import jax
import jax.numpy as jnp
from jax import lax
from jax.experimental import pallas as pl
from jax.experimental.pallas import tpu as pltpu
from jax.sharding import PartitionSpec as P

MESH = pl.DeviceIdType.MESH
epsilon = 1e-05


def flip(c, k):
    bit = 1
    while bit <= k:
        if k & bit:
            c = c + bit - 2 * bit * lax.rem(lax.div(c, bit), 2)
        bit *= 2
    return c


def is_above(c, k):
    top = 1 << (k.bit_length() - 1)
    return lax.rem(lax.div(c, top), 2) == 0


def plan(rows):
    if rows == 4:
        return [(3, 1, None), (0, 1, None), (3, 0, 1), (1, 2, None), (0, 2, 1), (2, 3, None)]
    flows = []
    for d in range(1, rows // 2 + 1):
        for s in range(rows if 2 * d < rows else rows // 2):
            flows.append((s, (s + d) % rows, None))
    return flows


def kernel(rows, cols, x_ref, out_ref, praw, panel, far_raw, stack, pacc, racc, psrc, pdst, rsrc, rdst,
           in_sem, ex_sem, ps_sem, pr_sem, fs_sem, fr_sem, zs_sem, zr_sem, xs_sem, qs_sem, qr_sem, ts_sem, tr_sem,
           x_ready, z_ready):
    p, c, l = lax.axis_index("row"), lax.axis_index("col"), lax.axis_index("layer")
    genes, part = x_ref.shape
    half = genes // 2
    cuts = 4
    piece = half // cuts
    samples = 2 * part
    other = 1 - l
    order = [k for k in range(cols) if k != 3] + [3]
    direct = [k for k in range(1, cols) if k != 3]
    last = cols - 1
    places = [(0, 0), (0, 1), (1, 1), (2, 0), (1, 0), (2, 1)] + [(k, s) for k in order[3:] for s in range(2)]
    ends = len(places)
    flows = plan(rows)
    slots = {t: [f for f in flows if f[1] == t] for t in range(rows)}
    outs = {s: [f for f in flows if f[0] == s and f[2] is None] for s in range(rows)}
    back = {s: [f for f in flows if f[0] == s] for s in range(rows)}
    pairs_of = {q: sorted({f[1] for f in flows if f[0] == q} | {f[0] for f in flows if f[1] == q}) for q in range(rows)}

    def remote(src, dst, send, recv, device):
        return pltpu.make_async_remote_copy(
            src_ref=src, dst_ref=dst, send_sem=send, recv_sem=recv, device_id=device, device_id_type=MESH
        )

    def by_row(values):
        value = values[0]
        for q in range(1, rows):
            value = jnp.where(p == q, values[q], value)
        return value

    def at_row(q, condition=True):
        return pl.when(p == q)

    load = pltpu.make_async_copy(x_ref, praw.at[0, l], in_sem)
    load.start()

    barrier = pltpu.get_barrier_semaphore()

    def greet(device):
        pl.semaphore_signal(barrier, inc=1, device_id=device, device_id_type=MESH)

    greet((p, c, other))
    for k in direct:
        @pl.when(is_above(c, k))
        def _():
            greet((p, flip(c, k), l))
    for q in range(rows):
        above = [t for t in pairs_of[q] if t > q]
        if above:
            @pl.when(p == q)
            def _():
                for t in above:
                    for h in range(2):
                        greet((t, c, h))
    greetings = 1 + by_row([2 * len([t for t in pairs_of[q] if t < q]) for q in range(rows)])
    for k in direct:
        greetings = greetings + jnp.where(is_above(c, k), 0, 1)

    pacc[...] = jnp.zeros_like(pacc)
    racc[...] = jnp.zeros_like(racc)
    pl.semaphore_wait(barrier, greetings)
    for k in direct:
        @pl.when(jnp.logical_not(is_above(c, k)))
        def _():
            pl.semaphore_signal(x_ready.at[k - 1], inc=1, device_id=(p, flip(c, k), l), device_id_type=MESH)
    for t in range(rows):
        below = [f for f in slots[t] if f[2] is None and f[0] < t]
        if below:
            @pl.when(p == t)
            def _():
                for f in below:
                    for h in range(2):
                        pl.semaphore_signal(z_ready.at[outs[f[0]].index(f)], inc=1, device_id=(f[0], c, h), device_id_type=MESH)
    load.wait()

    def z_copy(f, h, i):
        source = praw.at[0, l, pl.ds(h * half + i * piece, piece)]
        return remote(source, far_raw.at[slots[f[1]].index(f), l, pl.ds(i * piece, piece)],
                      zs_sem.at[outs[f[0]].index(f), h, i], zr_sem.at[slots[f[1]].index(f), l, i], (f[1], c, h))

    def z_arrival(t, b, i):
        at = far_raw.at[t, b, pl.ds(pl.multiple_of(i * piece, piece), piece)]
        return remote(at, at, zs_sem.at[0, 0, 0], zr_sem.at[t, b, i], (p, c, other))

    def held_back(f):
        return rows == 4 and f == (1, 2, None)

    def send_row(f):
        for i in range(cuts // 2 if held_back(f) else cuts):
            for h in range(2):
                z_copy(f, h, i).start()

    exchange = remote(praw.at[0, l], praw.at[0, l], ex_sem.at[0], ex_sem.at[1], (p, c, other))
    exchange.start()
    for q in range(rows):
        down = [f for f in outs[q] if f[1] < q]
        if down:
            @pl.when(p == q)
            def _():
                for f in down:
                    send_row(f)

    def panel_copy(k, s):
        at = pl.ds(s * half, half)
        return remote(praw.at[0, l, at], praw.at[order.index(k), l, at], ps_sem.at[k - 1, s], pr_sem.at[k - 1, s],
                      (p, flip(c, k), l))

    def pass_on(s):
        source, target = (2, 1) if s == 0 else (1, 2)
        at = pl.ds(s * half, half)
        return remote(praw.at[order.index(source), l, at], praw.at[last, l, at], ps_sem.at[2, s], pr_sem.at[2, s],
                      (p, flip(c, target), l))

    panel_copies = {(k, s): panel_copy(k, s) for k in direct for s in range(2)}
    panel_copies.update({(3, s): pass_on(s) for s in range(2)})

    def forward(k, s):
        at = praw.at[order.index(k), l, pl.ds(s * half, half)]
        return remote(at, at, fs_sem.at[k - 1, s], fr_sem.at[k - 1, s], (p, c, other))

    first = {1: (1, 0), 2: (0, 1)}
    for k in direct:
        @pl.when(jnp.logical_not(is_above(c, k)))
        def _():
            for s in first.get(k, (0, 1)):
                panel_copies[k, s].start()
    for k in direct:
        @pl.when(is_above(c, k))
        def _():
            pl.semaphore_wait(x_ready.at[k - 1], 1)
            for s in first.get(k, (0, 1)):
                panel_copies[k, s].start()
    for q in range(rows):
        up = [f for f in outs[q] if f[1] > q]
        if up:
            @pl.when(p == q)
            def _():
                for f in up:
                    pl.semaphore_wait(z_ready.at[outs[q].index(f)], 2)
                    send_row(f)

    step = 32

    def scale(low, high):
        low, high = low.astype(jnp.float32), high.astype(jnp.float32)
        total = jnp.sum(low, axis=1, keepdims=True) + jnp.sum(high, axis=1, keepdims=True)
        squares = jnp.sum(low * low + high * high, axis=1, keepdims=True)
        average = total / samples
        variance = squares / samples - average * average
        gain = lax.rsqrt(variance + epsilon)
        return (((low - average) * gain).astype(jnp.bfloat16), ((high - average) * gain).astype(jnp.bfloat16))

    def standardize(k, s):
        n, place = order.index(k), places.index((k, s))
        for i in range(half // step):
            at = pl.ds(s * half + i * step, step)
            low, high = scale(praw[n, 0, at, :], praw[n, 1, at, :])
            at = pl.ds(place * half + i * step, step)
            panel[at, 0:part] = low
            panel[at, part:samples] = high

    def slot_at(t):
        return (1 + t) * half

    def standardize_far(t, first, stop):
        for j in range(first // step, stop // step):
            at = pl.ds(j * step, step)
            low, high = scale(far_raw[t, 0, at, :], far_raw[t, 1, at, :])
            at = pl.ds(slot_at(t) + j * step, step)
            stack[at, 0:part] = low
            stack[at, part:samples] = high

    def pairs(first, stop, start, end):
        product = lax.dot_general(
            stack[first:stop, :], panel[start * half:end * half, :], (((1,), (1,)), ((), ())),
            preferred_element_type=jnp.float32
        )
        shifted = product * (0.5 / samples) + 0.5
        square = shifted * shifted
        fourth = square * square
        eighth = fourth * fourth
        value = eighth * fourth
        width = value.shape[1]
        pacc[:, start * half:end * half] += jnp.sum(value.reshape((stop - first) // 8, 8, width), axis=0)
        skipped = max(half - first, 0)
        if first + skipped < stop:
            value = value[skipped:]
            lanes = value[:, 0:128]
            for j in range(1, width // 128):
                lanes = lanes + value[:, j * 128:(j + 1) * 128]
            racc[first + skipped - half:stop - half, :] += lanes

    exchange.wait_recv()
    for s in range(2):
        standardize(0, s)
    stack[0:half, :] = panel[pl.ds(pl.multiple_of(l * half, half), half), :]
    pairs(0, half, 0, 2)

    relays = [f for f in flows if f[2] is not None]

    def passed(f):
        return slots[f[2]].index((f[0], f[2], None))

    def relay_copy(f, b, i):
        at, t = pl.ds(i * piece, piece), slots[f[1]].index(f)
        return remote(far_raw.at[passed(f), b, at], far_raw.at[t, b, at],
                      xs_sem.at[relays.index(f), b, i], zr_sem.at[t, b, i], (f[1], c, l))

    def relay(n, i):
        for f in relays[n:n + 1]:
            @pl.when(p == f[2])
            def _():
                for b in range(2):
                    z_arrival(passed(f), b, i).wait_recv()
                    relay_copy(f, b, i).start()

    for n, i in [(1, 0), (1, 1), (0, 0)]:
        relay(n, i)
    for s in range(2):
        panel_copies[2 - s, s].wait_recv()
        panel_copies[3, s].start()
        forward(2 - s, s).start()
    for n, i in [(0, 1), (1, 2)]:
        relay(n, i)
    for s in range(2):
        forward(2 - s, s).wait_recv()
        standardize(2 - s, s)
    pairs(0, half, 2, 4)
    for n, i in [(1, 3), (0, 2)]:
        relay(n, i)
    for f in flows:
        if held_back(f):
            @pl.when(p == f[0])
            def _():
                for i in range(cuts // 2, cuts):
                    for h in range(2):
                        z_copy(f, h, i).start()
    for s in range(2):
        panel_copies[1 + s, s].wait_recv()
        forward(1 + s, s).start()
    relay(0, 3)

    def take_far(t, i):
        passing = [f[2] for f in relays if passed(f) == t]
        if passing:
            @pl.when(p != passing[0])
            def _():
                for b in range(2):
                    z_arrival(t, b, i).wait_recv()
        else:
            for b in range(2):
                z_arrival(t, b, i).wait_recv()

    def back_copy(f):
        t, j = slots[f[1]].index(f), back[f[0]].index(f)
        return remote(rsrc.at[t], rdst.at[j], ts_sem.at[t], tr_sem.at[j], (f[0], c, l))

    def give_back(t):
        turned = racc[t * half:(t + 1) * half, :].T
        rsrc[t] = jnp.sum(turned.reshape(128 // 8, 8, half), axis=0)
        for q in range(rows):
            if t < len(slots[q]):
                @pl.when(p == q)
                def _():
                    back_copy(slots[q][t]).start()

    depth = max(len(slots[q]) for q in range(rows))
    n_slots = by_row([len(slots[q]) for q in range(rows)])
    middle = half + half // 2

    def take_block(t):
        for i in range(cuts):
            take_far(t, i)
        standardize_far(t, 0, half)

    soon = by_row([2 if any(f[2] == q for f in flows) else 1 for q in range(rows)])
    for i in range(cuts // 2):
        take_far(0, i)
    standardize_far(0, 0, half // 2)
    pairs(half, middle, 0, 4)
    for t in range(1, depth):
        @pl.when(jnp.minimum(n_slots, soon) > t)
        def _():
            take_block(t)
            pairs(slot_at(t), slot_at(t) + half, 0, 4)

    for s in range(2):
        forward(1 + s, s).wait_recv()
        standardize(1 + s, s)
    for k in direct[2:]:
        for s in range(2):
            panel_copies[k, s].wait_recv()
            forward(k, s).start()
        for s in range(2):
            forward(k, s).wait_recv()
            standardize(k, s)
    pairs(0, middle, 4, ends - 2)
    for s in range(2):
        panel_copies[3, s].wait_recv()
        forward(3, s).start()
    for t in range(1, depth):
        @pl.when(n_slots > t)
        def _():
            @pl.when(soon > t)
            def _():
                pairs(slot_at(t), slot_at(t) + half, 4, ends - 2)

            @pl.when(soon <= t)
            def _():
                take_block(t)
                pairs(slot_at(t), slot_at(t) + half, 0, ends - 2)

    for s in range(2):
        forward(3, s).wait_recv()
        standardize(3, s)
    pairs(0, middle, ends - 2, ends)
    for t in range(1, depth):
        @pl.when(n_slots > t)
        def _():
            pairs(slot_at(t), slot_at(t) + half, ends - 2, ends)
            give_back(t)

    for i in range(cuts // 2, cuts):
        take_far(0, i)
    standardize_far(0, half // 2, half)

    def part_copy(k, h):
        return remote(psrc.at[k, h], pdst.at[k, l], qs_sem.at[k, h], qr_sem.at[k, l], (p, flip(c, k), h))

    def part_arrival(k, b):
        return remote(psrc.at[k, b], pdst.at[k, b], qs_sem.at[k, b], qr_sem.at[k, b], (p, c, other))

    def send_parts(k):
        for h in range(2):
            place = places.index((k, h))
            psrc[k, h] = pacc[:, place * half:(place + 1) * half]
            if k:
                part_copy(k, h).start()

    pairs(middle, 2 * half, ends - 2, ends)
    send_parts(3)
    pairs(middle, 2 * half, 2, ends - 2)
    for k in direct:
        send_parts(k)
    pairs(middle, 2 * half, 0, 2)
    send_parts(0)
    part_copy(0, other).start()
    give_back(0)
    total = psrc[0, l] - 1.0 / 8
    part_arrival(0, other).wait_recv()
    total = total + pdst[0, other]
    for k in range(1, cols):
        for b in range(2):
            part_arrival(k, b).wait_recv()
            total = total + pdst[k, b]

    def back_arrival(j):
        return remote(rsrc.at[0], rdst.at[j], ts_sem.at[0], tr_sem.at[j], (p, c, other))

    n_back = by_row([len(back[q]) for q in range(rows)])
    least = min(len(back[q]) for q in range(rows))
    for j in range(least):
        back_arrival(j).wait_recv()
        total = total + rdst[j]
    psrc[0, l] = total
    for j in range(least, max(len(back[q]) for q in range(rows))):
        @pl.when(n_back > j)
        def _():
            back_arrival(j).wait_recv()
            psrc[0, l] += rdst[j]
    out_ref[...] = jnp.sum(psrc[0, l], axis=0)

    exchange.wait_send()
    for k, s in panel_copies:
        panel_copies[k, s].wait_send()
        forward(k, s).wait_send()
    for k in range(1, cols):
        for h in range(2):
            part_copy(k, h).wait_send()
    part_copy(0, other).wait_send()
    for q in range(rows):
        @pl.when(p == q)
        def _():
            for f in outs[q]:
                for h in range(2):
                    for i in range(cuts):
                        z_copy(f, h, i).wait_send()
            for f in relays:
                if f[2] == q:
                    for b in range(2):
                        for i in range(cuts):
                            relay_copy(f, b, i).wait_send()
            for f in slots[q]:
                back_copy(f).wait_send()


def solution(mesh):
    rows, cols = mesh.shape["row"], mesh.shape["col"]
    flows = plan(rows)
    depth = max(len([f for f in flows if f[1] == q]) for q in range(rows))
    fan = max(len([f for f in flows if f[0] == q]) for q in range(rows))
    dma = lambda *shape: pltpu.SemaphoreType.DMA(shape)

    def on_device(expression):
        genes, part = expression.shape
        half, samples = genes // 2, 2 * part
        bf16, f32 = jnp.bfloat16, jnp.float32
        summed = pl.pallas_call(
            functools.partial(kernel, rows, cols),
            out_shape=jax.ShapeDtypeStruct((half,), f32),
            in_specs=[pl.BlockSpec(memory_space=pl.ANY)],
            out_specs=pl.BlockSpec(memory_space=pltpu.VMEM),
            scratch_shapes=[
                pltpu.VMEM((cols, 2, genes, part), bf16),
                pltpu.VMEM((cols * genes, samples), bf16),
                pltpu.VMEM((depth, 2, half, part), bf16),
                pltpu.VMEM(((1 + depth) * half, samples), bf16),
                pltpu.VMEM((8, cols * genes), f32),
                pltpu.VMEM((depth * half, 128), f32),
                pltpu.VMEM((cols, 2, 8, half), f32),
                pltpu.VMEM((cols, 2, 8, half), f32),
                pltpu.VMEM((depth, 8, half), f32),
                pltpu.VMEM((fan, 8, half), f32),
                pltpu.SemaphoreType.DMA,
                dma(2),
                dma(cols - 1, 2), dma(cols - 1, 2),
                dma(cols - 1, 2), dma(cols - 1, 2),
                dma(fan, 2, 4), dma(depth, 2, 4),
                dma(max(len([f for f in flows if f[2] is not None]), 1), 2, 4),
                dma(cols, 2), dma(cols, 2),
                dma(depth), dma(fan),
                pltpu.SemaphoreType.REGULAR((cols - 1,)),
                pltpu.SemaphoreType.REGULAR((fan,)),
            ],
            compiler_params=pltpu.CompilerParams(collective_id=0, has_side_effects=True, vmem_limit_bytes=48000000),
        )(pltpu.with_memory_space_constraint(expression, pltpu.HBM))
        return summed

    return jax.shard_map(
        on_device,
        mesh=mesh,
        in_specs=(P(("row", "col"), "layer"),),
        out_specs=P(("row", "col", "layer")),
        check_vma=False,
    )
```

```python
import functools

import jax
import jax.numpy as jnp
from jax import lax
from jax.experimental import pallas as pl
from jax.experimental.pallas import tpu as pltpu
from jax.sharding import PartitionSpec as P

MESH = pl.DeviceIdType.MESH
epsilon = 1e-05


def flip(c, k):
    bit = 1
    while bit <= k:
        if k & bit:
            c = c + bit - 2 * bit * lax.rem(lax.div(c, bit), 2)
        bit *= 2
    return c


def is_above(c, k):
    top = 1 << (k.bit_length() - 1)
    return lax.rem(lax.div(c, top), 2) == 0


def plan(rows):
    if rows == 4:
        return [(3, 1, None), (0, 1, None), (3, 0, 1), (1, 2, None), (0, 2, 1), (2, 3, None)]
    flows = []
    for d in range(1, rows // 2 + 1):
        for s in range(rows if 2 * d < rows else rows // 2):
            flows.append((s, (s + d) % rows, None))
    return flows


def kernel(rows, cols, x_ref, out_ref, praw, panel, across, far_raw, stack, pacc, racc, psrc, pdst, rsrc, rdst,
           in_sem, ex_sem, ps_sem, pr_sem, fs_sem, fr_sem, zs_sem, zr_sem, xs_sem, qs_sem, qr_sem, ts_sem, tr_sem,
           x_ready, z_ready):
    p, c, l = lax.axis_index("row"), lax.axis_index("col"), lax.axis_index("layer")
    genes, part = x_ref.shape
    half = genes // 2
    cuts = 4
    piece = half // cuts
    samples = 2 * part
    other = 1 - l
    order = [k for k in range(cols) if k != 3] + [3]
    direct = [k for k in range(1, cols) if k != 3]
    last = cols - 1
    places = [(0, 0), (0, 1), (1, 1), (2, 0), (1, 0), (2, 1)] + [(k, s) for k in order[3:] for s in range(2)]
    ends = len(places)
    flows = plan(rows)
    slots = {t: [f for f in flows if f[1] == t] for t in range(rows)}
    outs = {s: [f for f in flows if f[0] == s and f[2] is None] for s in range(rows)}
    back = {s: [f for f in flows if f[0] == s] for s in range(rows)}
    pairs_of = {q: sorted({f[1] for f in flows if f[0] == q} | {f[0] for f in flows if f[1] == q}) for q in range(rows)}

    def remote(src, dst, send, recv, device):
        return pltpu.make_async_remote_copy(
            src_ref=src, dst_ref=dst, send_sem=send, recv_sem=recv, device_id=device, device_id_type=MESH
        )

    def by_row(values):
        value = values[0]
        for q in range(1, rows):
            value = jnp.where(p == q, values[q], value)
        return value

    def at_row(q, condition=True):
        return pl.when(p == q)

    load = pltpu.make_async_copy(x_ref, praw.at[0, l], in_sem)
    load.start()

    barrier = pltpu.get_barrier_semaphore()

    def greet(device):
        pl.semaphore_signal(barrier, inc=1, device_id=device, device_id_type=MESH)

    alone = jnp.logical_and(p == 0, c == 0)

    @pl.when(jnp.logical_or(alone, l == 1))
    def _():
        greet((p, c, other))

    for k in direct:
        @pl.when(is_above(c, k))
        def _():
            greet((p, flip(c, k), l))
    for q in range(rows):
        above = [t for t in pairs_of[q] if t > q]
        if above:
            @pl.when(p == q)
            def _():
                for t in above:
                    for h in range(2):
                        greet((t, c, h))
    greetings = jnp.where(alone, 1, other) + by_row([2 * len([t for t in pairs_of[q] if t < q]) for q in range(rows)])
    for k in direct:
        greetings = greetings + jnp.where(is_above(c, k), 0, 1)

    pacc[...] = jnp.zeros_like(pacc)
    racc[...] = jnp.zeros_like(racc)
    pl.semaphore_wait(barrier, greetings)
    for k in direct:
        @pl.when(jnp.logical_not(is_above(c, k)))
        def _():
            pl.semaphore_signal(x_ready.at[k - 1], inc=1, device_id=(p, flip(c, k), l), device_id_type=MESH)
    for t in range(rows):
        below = [f for f in slots[t] if f[2] is None and f[0] < t]
        if below:
            @pl.when(p == t)
            def _():
                for f in below:
                    for h in range(2):
                        pl.semaphore_signal(z_ready.at[outs[f[0]].index(f), l], inc=1, device_id=(f[0], c, h), device_id_type=MESH)

    @pl.when(l == 0)
    def _():
        pl.semaphore_signal(x_ready.at[2], inc=1, device_id=(p, c, other), device_id_type=MESH)

    load.wait()

    def z_copy(f, h, i):
        source = praw.at[0, l, pl.ds(h * half + i * piece, piece)]
        return remote(source, far_raw.at[slots[f[1]].index(f), l, pl.ds(i * piece, piece)],
                      zs_sem.at[outs[f[0]].index(f), h, i], zr_sem.at[slots[f[1]].index(f), l, i], (f[1], c, h))

    def z_arrival(t, b, i):
        at = far_raw.at[t, b, pl.ds(pl.multiple_of(i * piece, piece), piece)]
        return remote(at, at, zs_sem.at[0, 0, 0], zr_sem.at[t, b, i], (p, c, other))

    def held_back(f):
        return rows == 4 and f == (1, 2, None)

    def send_row(f, ask=False):
        for i in range(cuts // 2 if held_back(f) else cuts):
            for h in (1, 0):
                if ask and i == 0:
                    pl.semaphore_wait(z_ready.at[outs[f[0]].index(f), h], 1)
                z_copy(f, h, i).start()

    exchange = remote(praw.at[0, l], praw.at[0, l], ex_sem.at[0], ex_sem.at[1], (p, c, other))

    @pl.when(l == 1)
    def _():
        pl.semaphore_wait(x_ready.at[2], 1)

    exchange.start()
    for q in range(rows):
        down = [f for f in outs[q] if f[1] < q]
        if down:
            @pl.when(p == q)
            def _():
                for f in down:
                    send_row(f)

    def panel_copy(k, s):
        at = pl.ds(s * half, half)
        return remote(praw.at[0, l, at], praw.at[order.index(k), l, at], ps_sem.at[k - 1, s], pr_sem.at[k - 1, s],
                      (p, flip(c, k), l))

    def pass_on(s):
        source, target = (2, 1) if s == 0 else (1, 2)
        at = pl.ds(s * half, half)
        return remote(praw.at[order.index(source), l, at], praw.at[last, l, at], ps_sem.at[2, s], pr_sem.at[2, s],
                      (p, flip(c, target), l))

    panel_copies = {(k, s): panel_copy(k, s) for k in direct for s in range(2)}
    panel_copies.update({(3, s): pass_on(s) for s in range(2)})

    def forward(k, s):
        at = praw.at[order.index(k), l, pl.ds(s * half, half)]
        return remote(at, at, fs_sem.at[k - 1, s], fr_sem.at[k - 1, s], (p, c, other))

    first = {1: (1, 0), 2: (0, 1)}
    for k in direct:
        @pl.when(jnp.logical_not(is_above(c, k)))
        def _():
            for s in first.get(k, (0, 1)):
                panel_copies[k, s].start()
    for k in direct:
        @pl.when(is_above(c, k))
        def _():
            pl.semaphore_wait(x_ready.at[k - 1], 1)
            for s in first.get(k, (0, 1)):
                panel_copies[k, s].start()
    for q in range(rows):
        up = [f for f in outs[q] if f[1] > q]
        if up:
            @pl.when(p == q)
            def _():
                for f in up:
                    send_row(f, ask=True)

    step = 32

    def scale(low, high):
        low, high = low.astype(jnp.float32), high.astype(jnp.float32)
        total = jnp.sum(low, axis=1, keepdims=True) + jnp.sum(high, axis=1, keepdims=True)
        squares = jnp.sum(low * low + high * high, axis=1, keepdims=True)
        average = total / samples
        variance = squares / samples - average * average
        gain = lax.rsqrt(variance + epsilon)
        return (((low - average) * gain).astype(jnp.bfloat16), ((high - average) * gain).astype(jnp.bfloat16))

    def standardize(k, s):
        n, place = order.index(k), places.index((k, s))
        for i in range(half // step):
            at = pl.ds(s * half + i * step, step)
            low, high = scale(praw[n, 0, at, :], praw[n, 1, at, :])
            at = pl.ds(place * half + i * step, step)
            panel[at, 0:part] = low
            panel[at, part:samples] = high

    def slot_at(t):
        return (1 + t) * half

    def standardize_far(t, first, stop):
        for j in range(first // step, stop // step):
            at = pl.ds(j * step, step)
            low, high = scale(far_raw[t, 0, at, :], far_raw[t, 1, at, :])
            at = pl.ds(slot_at(t) + j * step, step)
            stack[at, 0:part] = low
            stack[at, part:samples] = high

    def turn(start, end):
        for at in range(start * half, end * half, 128):
            across[:, at:at + 128] = panel[at:at + 128, :].T

    def pairs(first, stop, start, end, turned=False):
        if turned:
            product = jnp.dot(stack[first:stop, :], across[:, start * half:end * half], preferred_element_type=jnp.float32)
        else:
            product = lax.dot_general(
                stack[first:stop, :], panel[start * half:end * half, :], (((1,), (1,)), ((), ())),
                preferred_element_type=jnp.float32
            )
        shifted = product * (0.5 / samples) + 0.5
        square = shifted * shifted
        fourth = square * square
        eighth = fourth * fourth
        value = eighth * fourth
        width = value.shape[1]
        pacc[:, start * half:end * half] += jnp.sum(value.reshape((stop - first) // 8, 8, width), axis=0)
        skipped = max(half - first, 0)
        if first + skipped < stop:
            value = value[skipped:]
            lanes = value[:, 0:128]
            for j in range(1, width // 128):
                lanes = lanes + value[:, j * 128:(j + 1) * 128]
            racc[first + skipped - half:stop - half, :] += lanes

    exchange.wait_recv()
    for s in range(2):
        standardize(0, s)
    stack[0:half, :] = panel[pl.ds(pl.multiple_of(l * half, half), half), :]
    pairs(0, half, 0, 2)
    turn(0, 2)

    relays = [f for f in flows if f[2] is not None]

    def passed(f):
        return slots[f[2]].index((f[0], f[2], None))

    def relay_copy(f, b, i):
        at, t = pl.ds(i * piece, piece), slots[f[1]].index(f)
        return remote(far_raw.at[passed(f), b, at], far_raw.at[t, b, at],
                      xs_sem.at[relays.index(f), b, i], zr_sem.at[t, b, i], (f[1], c, l))

    def relay(n, i):
        for f in relays[n:n + 1]:
            @pl.when(p == f[2])
            def _():
                for b in range(2):
                    z_arrival(passed(f), b, i).wait_recv()
                    relay_copy(f, b, i).start()

    for n, i in [(1, 0), (0, 0), (1, 1)]:
        relay(n, i)
    for s in range(2):
        panel_copies[2 - s, s].wait_recv()
        panel_copies[3, s].start()
        forward(2 - s, s).start()
    for n, i in [(0, 1), (1, 2)]:
        relay(n, i)
    for s in range(2):
        forward(2 - s, s).wait_recv()
        standardize(2 - s, s)
    pairs(0, half, 2, 4)
    turn(2, 4)
    for n, i in [(1, 3), (0, 2)]:
        relay(n, i)
    for f in flows:
        if held_back(f):
            @pl.when(p == f[0])
            def _():
                for i in range(cuts // 2, cuts):
                    for h in (1, 0):
                        z_copy(f, h, i).start()
    for s in range(2):
        panel_copies[1 + s, s].wait_recv()
        forward(1 + s, s).start()
    relay(0, 3)

    def take_far(t, i):
        passing = [f[2] for f in relays if passed(f) == t]
        if passing:
            @pl.when(p != passing[0])
            def _():
                for b in range(2):
                    z_arrival(t, b, i).wait_recv()
        else:
            for b in range(2):
                z_arrival(t, b, i).wait_recv()

    def back_copy(f):
        t, j = slots[f[1]].index(f), back[f[0]].index(f)
        return remote(rsrc.at[t], rdst.at[j], ts_sem.at[t], tr_sem.at[j], (f[0], c, l))

    def give_back(t):
        turned = racc[t * half:(t + 1) * half, :].T
        rsrc[t] = jnp.sum(turned.reshape(128 // 8, 8, half), axis=0)
        for q in range(rows):
            if t < len(slots[q]):
                @pl.when(p == q)
                def _():
                    back_copy(slots[q][t]).start()

    depth = max(len(slots[q]) for q in range(rows))
    n_slots = by_row([len(slots[q]) for q in range(rows)])
    middle = half + half // 2

    def take_block(t):
        for i in range(cuts):
            take_far(t, i)
        standardize_far(t, 0, half)

    soon = by_row([2 if any(f[2] == q for f in flows) else 1 for q in range(rows)])
    for i in range(cuts // 2):
        take_far(0, i)
    standardize_far(0, 0, half // 2)
    pairs(half, middle, 0, 4, True)
    for t in range(1, depth):
        @pl.when(jnp.minimum(n_slots, soon) > t)
        def _():
            take_block(t)
            pairs(slot_at(t), slot_at(t) + half, 0, 4, True)

    for s in range(2):
        forward(1 + s, s).wait_recv()
        standardize(1 + s, s)
    for k in direct[2:]:
        for s in range(2):
            panel_copies[k, s].wait_recv()
            forward(k, s).start()
        for s in range(2):
            forward(k, s).wait_recv()
            standardize(k, s)
    pairs(0, middle, 4, ends - 2)
    for s in range(2):
        panel_copies[3, s].wait_recv()
        forward(3, s).start()
    turn(4, ends - 2)
    for t in range(1, depth):
        @pl.when(n_slots > t)
        def _():
            @pl.when(soon > t)
            def _():
                pairs(slot_at(t), slot_at(t) + half, 4, ends - 2, True)

            @pl.when(soon <= t)
            def _():
                take_block(t)
                pairs(slot_at(t), slot_at(t) + half, 0, ends - 2, True)

    for s in range(2):
        forward(3, s).wait_recv()
        standardize(3, s)
    pairs(0, middle, ends - 2, ends)
    for t in range(1, depth):
        @pl.when(n_slots > t)
        def _():
            pairs(slot_at(t), slot_at(t) + half, ends - 2, ends)
            give_back(t)

    turn(ends - 2, ends)
    for i in range(cuts // 2, cuts):
        take_far(0, i)
    standardize_far(0, half // 2, half)

    def part_copy(k, h):
        return remote(psrc.at[k, h], pdst.at[k, l], qs_sem.at[k, h], qr_sem.at[k, l], (p, flip(c, k), h))

    def part_arrival(k, b):
        return remote(psrc.at[k, b], pdst.at[k, b], qs_sem.at[k, b], qr_sem.at[k, b], (p, c, other))

    def send_parts(k):
        for h in range(2):
            place = places.index((k, h))
            psrc[k, h] = pacc[:, place * half:(place + 1) * half]
            if k:
                part_copy(k, h).start()

    pairs(middle, 2 * half, ends - 2, ends, True)
    send_parts(3)
    pairs(middle, 2 * half, 2, ends - 2, True)
    for k in direct:
        send_parts(k)
    pairs(middle, 2 * half, 0, 2, True)
    send_parts(0)
    part_copy(0, other).start()
    give_back(0)
    total = psrc[0, l] - 1.0 / 8
    part_arrival(0, other).wait_recv()
    total = total + pdst[0, other]
    for k in range(1, cols):
        for b in range(2):
            part_arrival(k, b).wait_recv()
            total = total + pdst[k, b]

    def back_arrival(j):
        return remote(rsrc.at[0], rdst.at[j], ts_sem.at[0], tr_sem.at[j], (p, c, other))

    n_back = by_row([len(back[q]) for q in range(rows)])
    least = min(len(back[q]) for q in range(rows))
    for j in range(least):
        back_arrival(j).wait_recv()
        total = total + rdst[j]
    psrc[0, l] = total
    for j in range(least, max(len(back[q]) for q in range(rows))):
        @pl.when(n_back > j)
        def _():
            back_arrival(j).wait_recv()
            psrc[0, l] += rdst[j]
    out_ref[...] = jnp.sum(psrc[0, l], axis=0)

    exchange.wait_send()
    for k, s in panel_copies:
        panel_copies[k, s].wait_send()
        forward(k, s).wait_send()
    for k in range(1, cols):
        for h in range(2):
            part_copy(k, h).wait_send()
    part_copy(0, other).wait_send()
    for q in range(rows):
        @pl.when(p == q)
        def _():
            for f in outs[q]:
                for h in range(2):
                    for i in range(cuts):
                        z_copy(f, h, i).wait_send()
            for f in relays:
                if f[2] == q:
                    for b in range(2):
                        for i in range(cuts):
                            relay_copy(f, b, i).wait_send()
            for f in slots[q]:
                back_copy(f).wait_send()


def solution(mesh):
    rows, cols = mesh.shape["row"], mesh.shape["col"]
    flows = plan(rows)
    depth = max(len([f for f in flows if f[1] == q]) for q in range(rows))
    fan = max(len([f for f in flows if f[0] == q]) for q in range(rows))
    dma = lambda *shape: pltpu.SemaphoreType.DMA(shape)

    def on_device(expression):
        genes, part = expression.shape
        half, samples = genes // 2, 2 * part
        bf16, f32 = jnp.bfloat16, jnp.float32
        summed = pl.pallas_call(
            functools.partial(kernel, rows, cols),
            out_shape=jax.ShapeDtypeStruct((half,), f32),
            in_specs=[pl.BlockSpec(memory_space=pl.ANY)],
            out_specs=pl.BlockSpec(memory_space=pltpu.VMEM),
            scratch_shapes=[
                pltpu.VMEM((cols, 2, genes, part), bf16),
                pltpu.VMEM((cols * genes, samples), bf16),
                pltpu.VMEM((samples, cols * genes), bf16),
                pltpu.VMEM((depth, 2, half, part), bf16),
                pltpu.VMEM(((1 + depth) * half, samples), bf16),
                pltpu.VMEM((8, cols * genes), f32),
                pltpu.VMEM((depth * half, 128), f32),
                pltpu.VMEM((cols, 2, 8, half), f32),
                pltpu.VMEM((cols, 2, 8, half), f32),
                pltpu.VMEM((depth, 8, half), f32),
                pltpu.VMEM((fan, 8, half), f32),
                pltpu.SemaphoreType.DMA,
                dma(2),
                dma(cols - 1, 2), dma(cols - 1, 2),
                dma(cols - 1, 2), dma(cols - 1, 2),
                dma(fan, 2, 4), dma(depth, 2, 4),
                dma(max(len([f for f in flows if f[2] is not None]), 1), 2, 4),
                dma(cols, 2), dma(cols, 2),
                dma(depth), dma(fan),
                pltpu.SemaphoreType.REGULAR((cols - 1,)),
                pltpu.SemaphoreType.REGULAR((fan, 2)),
            ],
            compiler_params=pltpu.CompilerParams(collective_id=0, has_side_effects=True, vmem_limit_bytes=48000000),
        )(pltpu.with_memory_space_constraint(expression, pltpu.HBM))
        return summed

    return jax.shard_map(
        on_device,
        mesh=mesh,
        in_specs=(P(("row", "col"), "layer"),),
        out_specs=P(("row", "col", "layer")),
        check_vma=False,
    )
```

```python
import functools

import jax
import jax.numpy as jnp
from jax import lax
from jax.experimental import pallas as pl
from jax.experimental.pallas import tpu as pltpu
from jax.sharding import PartitionSpec as P

MESH = pl.DeviceIdType.MESH
epsilon = 1e-05


def flip(c, k):
    bit = 1
    while bit <= k:
        if k & bit:
            c = c + bit - 2 * bit * lax.rem(lax.div(c, bit), 2)
        bit *= 2
    return c


def is_above(c, k):
    top = 1 << (k.bit_length() - 1)
    return lax.rem(lax.div(c, top), 2) == 0


def plan(rows):
    if rows == 4:
        return [(3, 1, None), (0, 1, None), (3, 0, 1), (1, 2, None), (0, 2, 1), (2, 3, None)]
    flows = []
    for d in range(1, rows // 2 + 1):
        for s in range(rows if 2 * d < rows else rows // 2):
            flows.append((s, (s + d) % rows, None))
    return flows


def kernel(rows, cols, x_ref, out_ref, praw, panel, across, far_raw, stack, pacc, racc, psrc, pdst, rsrc, rdst,
           in_sem, ex_sem, ps_sem, pr_sem, fs_sem, fr_sem, zs_sem, zr_sem, xs_sem, qs_sem, qr_sem, ts_sem, tr_sem,
           x_ready, z_ready):
    p, c, l = lax.axis_index("row"), lax.axis_index("col"), lax.axis_index("layer")
    genes, part = x_ref.shape
    half = genes // 2
    cuts = 4
    piece = half // cuts
    samples = 2 * part
    other = 1 - l
    order = [k for k in range(cols) if k != 3] + [3]
    direct = [k for k in range(1, cols) if k != 3]
    last = cols - 1
    places = [(0, 0), (0, 1), (1, 1), (2, 0), (1, 0), (2, 1)] + [(k, s) for k in order[3:] for s in range(2)]
    ends = len(places)
    flows = plan(rows)
    slots = {t: [f for f in flows if f[1] == t] for t in range(rows)}
    outs = {s: [f for f in flows if f[0] == s and f[2] is None] for s in range(rows)}
    back = {s: [f for f in flows if f[0] == s] for s in range(rows)}
    pairs_of = {q: sorted({f[1] for f in flows if f[0] == q} | {f[0] for f in flows if f[1] == q}) for q in range(rows)}

    def remote(src, dst, send, recv, device):
        return pltpu.make_async_remote_copy(
            src_ref=src, dst_ref=dst, send_sem=send, recv_sem=recv, device_id=device, device_id_type=MESH
        )

    def by_row(values):
        value = values[0]
        for q in range(1, rows):
            value = jnp.where(p == q, values[q], value)
        return value

    def at_row(q, condition=True):
        return pl.when(p == q)

    load = pltpu.make_async_copy(x_ref, praw.at[0, l], in_sem)
    load.start()

    barrier = pltpu.get_barrier_semaphore()

    def greet(device):
        pl.semaphore_signal(barrier, inc=1, device_id=device, device_id_type=MESH)

    alone = jnp.logical_and(p == 0, c == 0)

    @pl.when(jnp.logical_or(alone, l == 1))
    def _():
        greet((p, c, other))

    for k in direct:
        @pl.when(is_above(c, k))
        def _():
            greet((p, flip(c, k), l))
    for q in range(rows):
        above = [t for t in pairs_of[q] if t > q]
        if above:
            @pl.when(p == q)
            def _():
                for t in above:
                    for h in range(2):
                        greet((t, c, h))
    greetings = jnp.where(alone, 1, other) + by_row([2 * len([t for t in pairs_of[q] if t < q]) for q in range(rows)])
    for k in direct:
        greetings = greetings + jnp.where(is_above(c, k), 0, 1)

    pacc[...] = jnp.zeros_like(pacc)
    racc[...] = jnp.zeros_like(racc)
    pl.semaphore_wait(barrier, greetings)
    for k in direct:
        @pl.when(jnp.logical_not(is_above(c, k)))
        def _():
            pl.semaphore_signal(x_ready.at[k - 1], inc=1, device_id=(p, flip(c, k), l), device_id_type=MESH)
    for t in range(rows):
        below = [f for f in slots[t] if f[2] is None and f[0] < t]
        if below:
            @pl.when(p == t)
            def _():
                for f in below:
                    for h in range(2):
                        pl.semaphore_signal(z_ready.at[outs[f[0]].index(f), l], inc=1, device_id=(f[0], c, h), device_id_type=MESH)

    @pl.when(l == 0)
    def _():
        pl.semaphore_signal(x_ready.at[2], inc=1, device_id=(p, c, other), device_id_type=MESH)

    load.wait()

    def z_copy(f, h, i):
        source = praw.at[0, l, pl.ds(h * half + i * piece, piece)]
        return remote(source, far_raw.at[slots[f[1]].index(f), l, pl.ds(i * piece, piece)],
                      zs_sem.at[outs[f[0]].index(f), h, i], zr_sem.at[slots[f[1]].index(f), l, i], (f[1], c, h))

    def z_arrival(t, b, i):
        at = far_raw.at[t, b, pl.ds(pl.multiple_of(i * piece, piece), piece)]
        return remote(at, at, zs_sem.at[0, 0, 0], zr_sem.at[t, b, i], (p, c, other))

    def held_back(f):
        return rows == 4 and f == (1, 2, None)

    def send_row(f, ask=False):
        for i in range(cuts // 2 if held_back(f) else cuts):
            for h in (1, 0):
                if ask and i == 0:
                    pl.semaphore_wait(z_ready.at[outs[f[0]].index(f), h], 1)
                z_copy(f, h, i).start()

    exchange = remote(praw.at[0, l], praw.at[0, l], ex_sem.at[0], ex_sem.at[1], (p, c, other))

    @pl.when(l == 1)
    def _():
        pl.semaphore_wait(x_ready.at[2], 1)

    exchange.start()
    for q in range(rows):
        down = [f for f in outs[q] if f[1] < q]
        if down:
            @pl.when(p == q)
            def _():
                for f in down:
                    send_row(f)

    def panel_copy(k, s):
        at = pl.ds(s * half, half)
        return remote(praw.at[0, l, at], praw.at[order.index(k), l, at], ps_sem.at[k - 1, s], pr_sem.at[k - 1, s],
                      (p, flip(c, k), l))

    def pass_on(s):
        source, target = (2, 1) if s == 0 else (1, 2)
        at = pl.ds(s * half, half)
        return remote(praw.at[order.index(source), l, at], praw.at[last, l, at], ps_sem.at[2, s], pr_sem.at[2, s],
                      (p, flip(c, target), l))

    panel_copies = {(k, s): panel_copy(k, s) for k in direct for s in range(2)}
    panel_copies.update({(3, s): pass_on(s) for s in range(2)})

    def forward(k, s):
        at = praw.at[order.index(k), l, pl.ds(s * half, half)]
        return remote(at, at, fs_sem.at[k - 1, s], fr_sem.at[k - 1, s], (p, c, other))

    first = {1: (1, 0), 2: (0, 1)}
    for k in direct:
        @pl.when(jnp.logical_not(is_above(c, k)))
        def _():
            for s in first.get(k, (0, 1)):
                panel_copies[k, s].start()
    for k in direct:
        @pl.when(is_above(c, k))
        def _():
            pl.semaphore_wait(x_ready.at[k - 1], 1)
            for s in first.get(k, (0, 1)):
                panel_copies[k, s].start()
    for q in range(rows):
        up = [f for f in outs[q] if f[1] > q]
        if up:
            @pl.when(p == q)
            def _():
                for f in up:
                    send_row(f, ask=True)

    step = 32

    def scale(low, high):
        low, high = low.astype(jnp.float32), high.astype(jnp.float32)
        total = jnp.sum(low, axis=1, keepdims=True) + jnp.sum(high, axis=1, keepdims=True)
        squares = jnp.sum(low * low + high * high, axis=1, keepdims=True)
        average = total / samples
        variance = squares / samples - average * average
        gain = lax.rsqrt(variance + epsilon)
        return (((low - average) * gain).astype(jnp.bfloat16), ((high - average) * gain).astype(jnp.bfloat16))

    def standardize(k, s):
        n, place = order.index(k), places.index((k, s))
        for i in range(half // step):
            at = pl.ds(s * half + i * step, step)
            low, high = scale(praw[n, 0, at, :], praw[n, 1, at, :])
            at = pl.ds(place * half + i * step, step)
            panel[at, 0:part] = low
            panel[at, part:samples] = high

    def slot_at(t):
        return (1 + t) * half

    def standardize_far(t, first, stop):
        for j in range(first // step, stop // step):
            at = pl.ds(j * step, step)
            low, high = scale(far_raw[t, 0, at, :], far_raw[t, 1, at, :])
            at = pl.ds(slot_at(t) + j * step, step)
            stack[at, 0:part] = low
            stack[at, part:samples] = high

    def turn(start, end):
        for at in range(start * half, end * half, 128):
            across[:, at:at + 128] = panel[at:at + 128, :].T

    def pairs(first, stop, start, end, turned=False):
        if turned:
            product = jnp.dot(stack[first:stop, :], across[:, start * half:end * half], preferred_element_type=jnp.float32)
        else:
            product = lax.dot_general(
                stack[first:stop, :], panel[start * half:end * half, :], (((1,), (1,)), ((), ())),
                preferred_element_type=jnp.float32
            )
        shifted = product * (0.5 / samples) + 0.5
        square = shifted * shifted
        fourth = square * square
        eighth = fourth * fourth
        value = eighth * fourth
        width = value.shape[1]
        pacc[:, start * half:end * half] += jnp.sum(value.reshape((stop - first) // 8, 8, width), axis=0)
        skipped = max(half - first, 0)
        if first + skipped < stop:
            value = value[skipped:]
            lanes = value[:, 0:128]
            for j in range(1, width // 128):
                lanes = lanes + value[:, j * 128:(j + 1) * 128]
            racc[first + skipped - half:stop - half, :] += lanes

    exchange.wait_recv()
    for s in range(2):
        standardize(0, s)
    stack[0:half, :] = panel[pl.ds(pl.multiple_of(l * half, half), half), :]
    pairs(0, half, 0, 2)
    turn(0, 2)

    relays = [f for f in flows if f[2] is not None]

    def passed(f):
        return slots[f[2]].index((f[0], f[2], None))

    def relay_copy(f, b, i):
        at, t = pl.ds(i * piece, piece), slots[f[1]].index(f)
        return remote(far_raw.at[passed(f), b, at], far_raw.at[t, b, at],
                      xs_sem.at[relays.index(f), b, i], zr_sem.at[t, b, i], (f[1], c, l))

    def relay(n, i):
        for f in relays[n:n + 1]:
            @pl.when(p == f[2])
            def _():
                for b in range(2):
                    z_arrival(passed(f), b, i).wait_recv()
                    relay_copy(f, b, i).start()

    for n, i in [(1, 0), (0, 0), (1, 1)]:
        relay(n, i)
    for s in range(2):
        panel_copies[2 - s, s].wait_recv()
        panel_copies[3, s].start()
        forward(2 - s, s).start()
    for n, i in [(0, 1), (1, 2)]:
        relay(n, i)
    for s in range(2):
        forward(2 - s, s).wait_recv()
        standardize(2 - s, s)
    pairs(0, half, 2, 4)
    turn(2, 4)
    for n, i in [(1, 3), (0, 2)]:
        relay(n, i)
    for f in flows:
        if held_back(f):
            @pl.when(p == f[0])
            def _():
                for i in range(cuts // 2, cuts):
                    for h in (1, 0):
                        z_copy(f, h, i).start()
    for s in range(2):
        panel_copies[1 + s, s].wait_recv()
        forward(1 + s, s).start()
    relay(0, 3)

    def take_far(t, i):
        passing = [f[2] for f in relays if passed(f) == t]
        if passing:
            @pl.when(p != passing[0])
            def _():
                for b in range(2):
                    z_arrival(t, b, i).wait_recv()
        else:
            for b in range(2):
                z_arrival(t, b, i).wait_recv()

    def back_copy(f):
        t, j = slots[f[1]].index(f), back[f[0]].index(f)
        return remote(rsrc.at[t], rdst.at[j], ts_sem.at[t], tr_sem.at[j], (f[0], c, l))

    def give_back(t):
        turned = racc[t * half:(t + 1) * half, :].T
        rsrc[t] = jnp.sum(turned.reshape(128 // 8, 8, half), axis=0)
        for q in range(rows):
            if t < len(slots[q]):
                @pl.when(p == q)
                def _():
                    back_copy(slots[q][t]).start()

    depth = max(len(slots[q]) for q in range(rows))
    n_slots = by_row([len(slots[q]) for q in range(rows)])
    middle = half + half // 2

    def take_block(t):
        for i in range(cuts):
            take_far(t, i)
        standardize_far(t, 0, half)

    soon = by_row([2 if any(f[2] == q for f in flows) else 1 for q in range(rows)])
    for i in range(cuts // 2):
        take_far(0, i)
    standardize_far(0, 0, half // 2)
    pairs(half, middle, 0, 4, True)
    for t in range(1, depth):
        @pl.when(jnp.minimum(n_slots, soon) > t)
        def _():
            take_block(t)
            pairs(slot_at(t), slot_at(t) + half, 0, 4, True)

    for s in range(2):
        forward(1 + s, s).wait_recv()
        standardize(1 + s, s)
    for k in direct[2:]:
        for s in range(2):
            panel_copies[k, s].wait_recv()
            forward(k, s).start()
        for s in range(2):
            forward(k, s).wait_recv()
            standardize(k, s)
    pairs(0, middle, 4, ends - 2)
    for s in range(2):
        panel_copies[3, s].wait_recv()
        forward(3, s).start()
    turn(4, ends - 2)
    for t in range(1, depth):
        @pl.when(n_slots > t)
        def _():
            @pl.when(soon > t)
            def _():
                pairs(slot_at(t), slot_at(t) + half, 4, ends - 2, True)

            @pl.when(soon <= t)
            def _():
                take_block(t)
                pairs(slot_at(t), slot_at(t) + half, 0, ends - 2, True)

    for s in range(2):
        forward(3, s).wait_recv()
        standardize(3, s)
    for t in range(1, depth):
        @pl.when(n_slots > t)
        def _():
            pairs(slot_at(t), slot_at(t) + half, ends - 2, ends)
            give_back(t)

    pairs(0, middle, ends - 2, ends)
    turn(ends - 2, ends)
    for i in range(cuts // 2, cuts):
        take_far(0, i)
    standardize_far(0, half // 2, half)

    def part_copy(k, h):
        return remote(psrc.at[k, h], pdst.at[k, l], qs_sem.at[k, h], qr_sem.at[k, l], (p, flip(c, k), h))

    def part_arrival(k, b):
        return remote(psrc.at[k, b], pdst.at[k, b], qs_sem.at[k, b], qr_sem.at[k, b], (p, c, other))

    def send_parts(k):
        for h in range(2):
            place = places.index((k, h))
            psrc[k, h] = pacc[:, place * half:(place + 1) * half]
            if k:
                part_copy(k, h).start()

    pairs(middle, 2 * half, ends - 2, ends, True)
    send_parts(3)
    pairs(middle, 2 * half, 0, ends - 2, True)
    sums_first = p < rows // 2

    @pl.when(jnp.logical_not(sums_first))
    def _():
        give_back(0)

    for k in direct + [0]:
        send_parts(k)
    part_copy(0, other).start()

    @pl.when(sums_first)
    def _():
        give_back(0)

    exchange.wait_send()
    for k, s in panel_copies:
        panel_copies[k, s].wait_send()
        forward(k, s).wait_send()
    for k in range(1, cols):
        for h in range(2):
            part_copy(k, h).wait_send()
    part_copy(0, other).wait_send()
    for q in range(rows):
        @pl.when(p == q)
        def _():
            for f in outs[q]:
                for h in range(2):
                    for i in range(cuts):
                        z_copy(f, h, i).wait_send()
            for f in relays:
                if f[2] == q:
                    for b in range(2):
                        for i in range(cuts):
                            relay_copy(f, b, i).wait_send()
            for f in slots[q]:
                back_copy(f).wait_send()

    total = psrc[0, l] - 1.0 / 8
    part_arrival(0, other).wait_recv()
    total = total + pdst[0, other]
    for k in range(1, cols):
        for b in range(2):
            part_arrival(k, b).wait_recv()
            total = total + pdst[k, b]

    def back_arrival(j):
        return remote(rsrc.at[0], rdst.at[j], ts_sem.at[0], tr_sem.at[j], (p, c, other))

    n_back = by_row([len(back[q]) for q in range(rows)])
    least = min(len(back[q]) for q in range(rows))
    for j in range(least):
        back_arrival(j).wait_recv()
        total = total + rdst[j]
    psrc[0, l] = total
    for j in range(least, max(len(back[q]) for q in range(rows))):
        @pl.when(n_back > j)
        def _():
            back_arrival(j).wait_recv()
            psrc[0, l] += rdst[j]
    out_ref[...] = jnp.sum(psrc[0, l], axis=0)


def solution(mesh):
    rows, cols = mesh.shape["row"], mesh.shape["col"]
    flows = plan(rows)
    depth = max(len([f for f in flows if f[1] == q]) for q in range(rows))
    fan = max(len([f for f in flows if f[0] == q]) for q in range(rows))
    dma = lambda *shape: pltpu.SemaphoreType.DMA(shape)

    def on_device(expression):
        genes, part = expression.shape
        half, samples = genes // 2, 2 * part
        bf16, f32 = jnp.bfloat16, jnp.float32
        summed = pl.pallas_call(
            functools.partial(kernel, rows, cols),
            out_shape=jax.ShapeDtypeStruct((half,), f32),
            in_specs=[pl.BlockSpec(memory_space=pl.ANY)],
            out_specs=pl.BlockSpec(memory_space=pltpu.VMEM),
            scratch_shapes=[
                pltpu.VMEM((cols, 2, genes, part), bf16),
                pltpu.VMEM((cols * genes, samples), bf16),
                pltpu.VMEM((samples, cols * genes), bf16),
                pltpu.VMEM((depth, 2, half, part), bf16),
                pltpu.VMEM(((1 + depth) * half, samples), bf16),
                pltpu.VMEM((8, cols * genes), f32),
                pltpu.VMEM((depth * half, 128), f32),
                pltpu.VMEM((cols, 2, 8, half), f32),
                pltpu.VMEM((cols, 2, 8, half), f32),
                pltpu.VMEM((depth, 8, half), f32),
                pltpu.VMEM((fan, 8, half), f32),
                pltpu.SemaphoreType.DMA,
                dma(2),
                dma(cols - 1, 2), dma(cols - 1, 2),
                dma(cols - 1, 2), dma(cols - 1, 2),
                dma(fan, 2, 4), dma(depth, 2, 4),
                dma(max(len([f for f in flows if f[2] is not None]), 1), 2, 4),
                dma(cols, 2), dma(cols, 2),
                dma(depth), dma(fan),
                pltpu.SemaphoreType.REGULAR((cols - 1,)),
                pltpu.SemaphoreType.REGULAR((fan, 2)),
            ],
            compiler_params=pltpu.CompilerParams(collective_id=0, has_side_effects=True, vmem_limit_bytes=48000000),
        )(pltpu.with_memory_space_constraint(expression, pltpu.HBM))
        return summed

    return jax.shard_map(
        on_device,
        mesh=mesh,
        in_specs=(P(("row", "col"), "layer"),),
        out_specs=P(("row", "col", "layer")),
        check_vma=False,
    )
```

```python
import functools

import jax
import jax.numpy as jnp
from jax import lax
from jax.experimental import pallas as pl
from jax.experimental.pallas import tpu as pltpu
from jax.sharding import PartitionSpec as P

MESH = pl.DeviceIdType.MESH
epsilon = 1e-05


def flip(c, k):
    bit = 1
    while bit <= k:
        if k & bit:
            c = c + bit - 2 * bit * lax.rem(lax.div(c, bit), 2)
        bit *= 2
    return c


def is_above(c, k):
    top = 1 << (k.bit_length() - 1)
    return lax.rem(lax.div(c, top), 2) == 0


def plan(rows):
    if rows == 4:
        return [(3, 1, None), (0, 1, None), (3, 0, 1), (1, 2, None), (0, 2, 1), (2, 3, None)]
    flows = []
    for d in range(1, rows // 2 + 1):
        for s in range(rows if 2 * d < rows else rows // 2):
            flows.append((s, (s + d) % rows, None))
    return flows


def kernel(rows, cols, x_ref, out_ref, praw, panel, across, far_raw, stack, pacc, racc, psrc, pdst, rsrc, rdst,
           in_sem, ex_sem, own_sent, passed_sent, far_sent, parts_sent, back_sent,
           pr_sem, fr_sem, zr_sem, parts_here, back_here, x_ready, z_ready):
    p, c, l = lax.axis_index("row"), lax.axis_index("col"), lax.axis_index("layer")
    genes, part = x_ref.shape
    half = genes // 2
    cuts = 4
    piece = half // cuts
    samples = 2 * part
    other = 1 - l
    order = [k for k in range(cols) if k != 3] + [3]
    direct = [k for k in range(1, cols) if k != 3]
    last = cols - 1
    places = [(0, 0), (0, 1), (1, 1), (2, 0), (1, 0), (2, 1)] + [(k, s) for k in order[3:] for s in range(2)]
    ends = len(places)
    flows = plan(rows)
    slots = {t: [f for f in flows if f[1] == t] for t in range(rows)}
    outs = {s: [f for f in flows if f[0] == s and f[2] is None] for s in range(rows)}
    back = {s: [f for f in flows if f[0] == s] for s in range(rows)}
    pairs_of = {q: sorted({f[1] for f in flows if f[0] == q} | {f[0] for f in flows if f[1] == q}) for q in range(rows)}

    def held_back(f):
        return rows == 4 and f == (1, 2, None)

    def remote(src, dst, send, recv, device):
        return pltpu.make_async_remote_copy(
            src_ref=src, dst_ref=dst, send_sem=send, recv_sem=recv, device_id=device, device_id_type=MESH
        )

    def by_row(values):
        value = values[0]
        for q in range(1, rows):
            value = jnp.where(p == q, values[q], value)
        return value

    def at_row(q, condition=True):
        return pl.when(p == q)

    load = pltpu.make_async_copy(x_ref, praw.at[0, l], in_sem)
    load.start()

    barrier = pltpu.get_barrier_semaphore()

    def greet(device):
        pl.semaphore_signal(barrier, inc=1, device_id=device, device_id_type=MESH)

    alone = jnp.logical_and(p == 0, c == 0)

    @pl.when(jnp.logical_or(alone, l == 1))
    def _():
        greet((p, c, other))

    for k in direct:
        @pl.when(is_above(c, k))
        def _():
            for h in range(2):
                greet((p, flip(c, k), h))
    for q in range(rows):
        above = [t for t in pairs_of[q] if t > q]
        if above or any(held_back(f) for f in slots[q]):
            @pl.when(p == q)
            def _():
                for t in above:
                    for h in range(2):
                        greet((t, c, h))
                for f in slots[q]:
                    if held_back(f):
                        greet((f[0], c, 1))
    greetings = jnp.where(alone, 1, other) + by_row([2 * len([t for t in pairs_of[q] if t < q]) for q in range(rows)])
    for k in direct:
        greetings = greetings + jnp.where(is_above(c, k), 0, 2)

    greetings = greetings + l * by_row([2 * len([f for f in outs[q] if held_back(f)]) for q in range(rows)])
    pacc[...] = jnp.zeros_like(pacc)
    racc[...] = jnp.zeros_like(racc)
    pl.semaphore_wait(barrier, greetings)

    @pl.when(l == 0)
    def _():
        for t in range(rows):
            below = [f for f in slots[t] if f[2] is None and f[0] < t]
            if below:
                @pl.when(p == t)
                def _():
                    for f in below:
                        for b in range(1 if held_back(f) else 2):
                            pl.semaphore_signal(z_ready.at[outs[f[0]].index(f)], inc=2, device_id=(f[0], c, b), device_id_type=MESH)
        for k in direct:
            @pl.when(jnp.logical_not(is_above(c, k)))
            def _():
                for h in range(2):
                    pl.semaphore_signal(x_ready.at[k - 1], inc=1, device_id=(p, flip(c, k), h), device_id_type=MESH)
        pl.semaphore_signal(x_ready.at[2], inc=1, device_id=(p, c, other), device_id_type=MESH)

    load.wait()

    def z_copy(f, h, i):
        source = praw.at[0, l, pl.ds(h * half + i * piece, piece)]
        return remote(source, far_raw.at[slots[f[1]].index(f), l, pl.ds(i * piece, piece)],
                      far_sent, zr_sem.at[slots[f[1]].index(f), i], (f[1], c, h))

    def landed(ref, sem):
        remote(ref, ref, far_sent, sem, (p, c, other)).wait_recv()

    def left(ref, sem):
        remote(ref, ref, sem, zr_sem.at[0, 0], (p, c, other)).wait_send()

    def far_here(t, i):
        landed(far_raw.at[t, :, pl.ds(i * piece, piece)], zr_sem.at[t, i])

    def send_row(f, ask=False):
        if ask:
            if held_back(f):
                @pl.when(l == 0)
                def _():
                    pl.semaphore_wait(z_ready.at[outs[f[0]].index(f)], 2)
            else:
                pl.semaphore_wait(z_ready.at[outs[f[0]].index(f)], 2)
        for i in range(cuts // 2 if held_back(f) else cuts):
            for h in (1, 0):
                z_copy(f, h, i).start()

    exchange = remote(praw.at[0, l], praw.at[0, l], own_sent, ex_sem, (p, c, other))

    @pl.when(l == 1)
    def _():
        pl.semaphore_wait(x_ready.at[2], 1)

    exchange.start()
    for q in range(rows):
        down = [f for f in outs[q] if f[1] < q]
        if down:
            @pl.when(p == q)
            def _():
                for f in down:
                    send_row(f)

    def stage(k, s):
        return {1: 1 - s, 2: s, 3: 2}.get(k, k - 1)

    def stage_here(n, u):
        landed(praw.at[0, l, pl.ds(0, half)], pr_sem.at[n, u])

    def panel_copy(k, s, u):
        at = pl.ds(s * half + u * half // 2, half // 2)
        return remote(praw.at[0, l, at], praw.at[order.index(k), l, at], own_sent, pr_sem.at[stage(k, s), u],
                      (p, flip(c, k), l))

    def pass_on(s, u):
        source, target = (2, 1) if s == 0 else (1, 2)
        at = pl.ds(s * half + u * half // 2, half // 2)
        return remote(praw.at[order.index(source), l, at], praw.at[last, l, at], passed_sent, pr_sem.at[2, u],
                      (p, flip(c, target), l))

    panel_copies = {(k, s, u): panel_copy(k, s, u) for k in direct for s in range(2) for u in range(2)}
    panel_copies.update({(3, s, u): pass_on(s, u) for s in range(2) for u in range(2)})

    def forward(k, s, u):
        at = praw.at[order.index(k), l, pl.ds(s * half + u * half // 2, half // 2)]
        return remote(at, at, passed_sent, fr_sem.at[stage(k, s)], (p, c, other))

    def complete(n):
        landed(praw.at[0, other], fr_sem.at[n])
        for k, s in places:
            if k and stage(k, s) == n:
                standardize(k, s)

    first = {1: (1, 0), 2: (0, 1)}
    for k in direct:
        @pl.when(jnp.logical_not(is_above(c, k)))
        def _():
            for s in first.get(k, (0, 1)):
                for u in range(2):
                    panel_copies[k, s, u].start()
    for k in direct:
        @pl.when(is_above(c, k))
        def _():
            pl.semaphore_wait(x_ready.at[k - 1], 1)
            for s in first.get(k, (0, 1)):
                for u in range(2):
                    panel_copies[k, s, u].start()
    for q in range(rows):
        up = [f for f in outs[q] if f[1] > q]
        if up:
            @pl.when(p == q)
            def _():
                for f in up:
                    send_row(f, ask=True)

    step = 32

    def scale(low, high):
        low, high = low.astype(jnp.float32), high.astype(jnp.float32)
        total = jnp.sum(low, axis=1, keepdims=True) + jnp.sum(high, axis=1, keepdims=True)
        squares = jnp.sum(low * low + high * high, axis=1, keepdims=True)
        average = total / samples
        variance = squares / samples - average * average
        gain = lax.rsqrt(variance + epsilon)
        return (((low - average) * gain).astype(jnp.bfloat16), ((high - average) * gain).astype(jnp.bfloat16))

    def standardize(k, s):
        n, place = order.index(k), places.index((k, s))
        for i in range(half // step):
            at = pl.ds(s * half + i * step, step)
            low, high = scale(praw[n, 0, at, :], praw[n, 1, at, :])
            at = pl.ds(place * half + i * step, step)
            panel[at, 0:part] = low
            panel[at, part:samples] = high

    def slot_at(t):
        return (1 + t) * half

    def standardize_far(t, first, stop):
        for j in range(first // step, stop // step):
            at = pl.ds(j * step, step)
            low, high = scale(far_raw[t, 0, at, :], far_raw[t, 1, at, :])
            at = pl.ds(slot_at(t) + j * step, step)
            stack[at, 0:part] = low
            stack[at, part:samples] = high

    def turn(start, end):
        for at in range(start * half, end * half, 128):
            across[:, at:at + 128] = panel[at:at + 128, :].T

    def pairs(first, stop, start, end, turned=False):
        if turned:
            product = jnp.dot(stack[first:stop, :], across[:, start * half:end * half], preferred_element_type=jnp.float32)
        else:
            product = lax.dot_general(
                stack[first:stop, :], panel[start * half:end * half, :], (((1,), (1,)), ((), ())),
                preferred_element_type=jnp.float32
            )
        shifted = product * (0.5 / samples) + 0.5
        square = shifted * shifted
        fourth = square * square
        eighth = fourth * fourth
        value = eighth * fourth
        width = value.shape[1]
        pacc[:, start * half:end * half] += jnp.sum(value.reshape((stop - first) // 8, 8, width), axis=0)
        skipped = max(half - first, 0)
        if first + skipped < stop:
            value = value[skipped:]
            lanes = value[:, 0:128]
            for j in range(1, width // 128):
                lanes = lanes + value[:, j * 128:(j + 1) * 128]
            racc[first + skipped - half:stop - half, :] += lanes

    exchange.wait_recv()
    for s in range(2):
        standardize(0, s)
    stack[0:half, :] = panel[pl.ds(pl.multiple_of(l * half, half), half), :]
    pairs(0, half, 0, 2)
    turn(0, 2)

    relays = [f for f in flows if f[2] is not None]

    def passed(f):
        return slots[f[2]].index((f[0], f[2], None))

    def relay_copy(f, b, i):
        at, t = pl.ds(i * piece, piece), slots[f[1]].index(f)
        return remote(far_raw.at[passed(f), b, at], far_raw.at[t, b, at],
                      far_sent, zr_sem.at[t, i], (f[1], c, l))

    def relay(n, i):
        for f in relays[n:n + 1]:
            @pl.when(p == f[2])
            def _():
                far_here(passed(f), i)
                for b in range(2):
                    relay_copy(f, b, i).start()

    for n, i in [(1, 0), (0, 0), (1, 1)]:
        relay(n, i)
    for u in range(2):
        stage_here(0, u)
        for s in range(2):
            panel_copies[3, s, u].start()
            forward(2 - s, s, u).start()
    for n, i in [(0, 1), (1, 2)]:
        relay(n, i)
    complete(0)
    pairs(0, half, 2, 4)
    turn(2, 4)
    for n, i in [(1, 3), (0, 2)]:
        relay(n, i)
    for f in flows:
        if held_back(f):
            @pl.when(p == f[0])
            def _():
                for i in range(cuts // 2, cuts):
                    for h in (1, 0):
                        z_copy(f, h, i).start()
    for u in range(2):
        stage_here(1, u)
        for s in range(2):
            forward(1 + s, s, u).start()
    relay(0, 3)

    def take_far(t, i):
        passing = [f[2] for f in relays if passed(f) == t]
        if passing:
            @pl.when(p != passing[0])
            def _():
                far_here(t, i)
        else:
            far_here(t, i)

    def back_copy(f):
        t, j = slots[f[1]].index(f), back[f[0]].index(f)
        return remote(rsrc.at[t], rdst.at[j], back_sent, back_here, (f[0], c, l))

    def give_back(t):
        turned = racc[t * half:(t + 1) * half, :].T
        rsrc[t] = jnp.sum(turned.reshape(128 // 8, 8, half), axis=0)
        for q in range(rows):
            if t < len(slots[q]):
                @pl.when(p == q)
                def _():
                    back_copy(slots[q][t]).start()

    depth = max(len(slots[q]) for q in range(rows))
    n_slots = by_row([len(slots[q]) for q in range(rows)])
    middle = half + half // 2

    def take_block(t):
        for i in range(cuts):
            take_far(t, i)
        standardize_far(t, 0, half)

    soon = by_row([2 if any(f[2] == q for f in flows) else 1 for q in range(rows)])
    for i in range(cuts // 2):
        take_far(0, i)
    standardize_far(0, 0, half // 2)
    pairs(half, middle, 0, 4, True)
    for t in range(1, depth):
        @pl.when(jnp.minimum(n_slots, soon) > t)
        def _():
            take_block(t)
            pairs(slot_at(t), slot_at(t) + half, 0, 4, True)

    complete(1)
    for k in direct[2:]:
        for u in range(2):
            stage_here(stage(k, 0), u)
            for s in range(2):
                forward(k, s, u).start()
        complete(stage(k, 0))
    pairs(0, middle, 4, ends - 2)
    for u in range(2):
        stage_here(2, u)
        for s in range(2):
            forward(3, s, u).start()
    turn(4, ends - 2)
    for t in range(1, depth):
        @pl.when(n_slots > t)
        def _():
            @pl.when(soon > t)
            def _():
                pairs(slot_at(t), slot_at(t) + half, 4, ends - 2, True)

            @pl.when(soon <= t)
            def _():
                take_block(t)
                pairs(slot_at(t), slot_at(t) + half, 0, ends - 2, True)

    def part_copy(k, h):
        return remote(psrc.at[2 * k + h], pdst.at[2 * k + l], parts_sent, parts_here, (p, flip(c, k), h))

    def take_last():
        for i in range(cuts // 2, cuts):
            take_far(0, i)
        standardize_far(0, half // 2, half)

    def finish_panel():
        complete(2)
        for t in range(1, depth):
            @pl.when(n_slots > t)
            def _():
                pairs(slot_at(t), slot_at(t) + half, ends - 2, ends)
                give_back(t)

    def send_parts(k):
        for h in range(2):
            place = places.index((k, h))
            psrc[2 * k + h] = pacc[:, place * half:(place + 1) * half]
            if k:
                part_copy(k, h).start()

    waits = by_row([1 if any(held_back(f) or f[2] is not None for f in slots[q]) else 0 for q in range(rows)]) == 1

    @pl.when(waits)
    def _():
        finish_panel()
        pairs(0, middle, ends - 2, ends)
        turn(ends - 2, ends)
        take_last()
        pairs(middle, 2 * half, ends - 2, ends, True)
        send_parts(3)
        pairs(middle, 2 * half, 0, ends - 2, True)

    @pl.when(jnp.logical_not(waits))
    def _():
        take_last()
        pairs(middle, 2 * half, 0, ends - 2, True)
        finish_panel()
        pairs(0, 2 * half, ends - 2, ends)
        send_parts(3)

    sums_first = p < rows // 2

    @pl.when(jnp.logical_not(sums_first))
    def _():
        give_back(0)

    for k in direct + [0]:
        send_parts(k)
    part_copy(0, other).start()

    @pl.when(sums_first)
    def _():
        give_back(0)

    left(praw.at[pl.ds(0, last), l], own_sent)
    left(praw.at[:, l], passed_sent)
    left(psrc.at[pl.ds(0, 2 * cols - 1)], parts_sent)
    for q in range(rows):
        @pl.when(p == q)
        def _():
            blocks = len(outs[q]) + len([f for f in relays if f[2] == q])
            if blocks:
                left(praw.at[pl.ds(0, blocks), l], far_sent)
            if slots[q]:
                left(rsrc.at[pl.ds(0, len(slots[q]))], back_sent)

    total = psrc[l] - 1.0 / 8
    landed(pdst.at[pl.ds(0, 2 * cols - 1)], parts_here)
    total = total + pdst[other]
    for n in range(2, 2 * cols):
        total = total + pdst[n]
    psrc[l] = total
    for q in range(rows):
        if back[q]:
            @pl.when(p == q)
            def _():
                landed(rdst.at[pl.ds(0, len(back[q]))], back_here)
                more = rdst[0]
                for j in range(1, len(back[q])):
                    more = more + rdst[j]
                psrc[l] += more
    out_ref[...] = jnp.sum(psrc[l], axis=0)


def solution(mesh):
    rows, cols = mesh.shape["row"], mesh.shape["col"]
    flows = plan(rows)
    depth = max(len([f for f in flows if f[1] == q]) for q in range(rows))
    fan = max(len([f for f in flows if f[0] == q]) for q in range(rows))
    dma = lambda *shape: pltpu.SemaphoreType.DMA(shape)

    def on_device(expression):
        genes, part = expression.shape
        half, samples = genes // 2, 2 * part
        bf16, f32 = jnp.bfloat16, jnp.float32
        summed = pl.pallas_call(
            functools.partial(kernel, rows, cols),
            out_shape=jax.ShapeDtypeStruct((half,), f32),
            in_specs=[pl.BlockSpec(memory_space=pl.ANY)],
            out_specs=pl.BlockSpec(memory_space=pltpu.VMEM),
            scratch_shapes=[
                pltpu.VMEM((cols, 2, genes, part), bf16),
                pltpu.VMEM((cols * genes, samples), bf16),
                pltpu.VMEM((samples, cols * genes), bf16),
                pltpu.VMEM((depth, 2, half, part), bf16),
                pltpu.VMEM(((1 + depth) * half, samples), bf16),
                pltpu.VMEM((8, cols * genes), f32),
                pltpu.VMEM((depth * half, 128), f32),
                pltpu.VMEM((2 * cols, 8, half), f32),
                pltpu.VMEM((2 * cols, 8, half), f32),
                pltpu.VMEM((depth, 8, half), f32),
                pltpu.VMEM((fan, 8, half), f32),
                *[pltpu.SemaphoreType.DMA] * 7,
                dma(cols - 1, 2), dma(cols - 1), dma(depth, 4),
                pltpu.SemaphoreType.DMA, pltpu.SemaphoreType.DMA,
                pltpu.SemaphoreType.REGULAR((cols - 1,)),
                pltpu.SemaphoreType.REGULAR((fan,)),
            ],
            compiler_params=pltpu.CompilerParams(collective_id=0, has_side_effects=True, vmem_limit_bytes=48000000),
        )(pltpu.with_memory_space_constraint(expression, pltpu.HBM))
        return summed

    return jax.shard_map(
        on_device,
        mesh=mesh,
        in_specs=(P(("row", "col"), "layer"),),
        out_specs=P(("row", "col", "layer")),
        check_vma=False,
    )
```

```python
import functools

import jax
import jax.numpy as jnp
from jax import lax
from jax.experimental import pallas as pl
from jax.experimental.pallas import tpu as pltpu
from jax.sharding import PartitionSpec as P

MESH = pl.DeviceIdType.MESH
epsilon = 1e-05


def flip(c, k):
    bit = 1
    while bit <= k:
        if k & bit:
            c = c + bit - 2 * bit * lax.rem(lax.div(c, bit), 2)
        bit *= 2
    return c


def is_above(c, k):
    top = 1 << (k.bit_length() - 1)
    return lax.rem(lax.div(c, top), 2) == 0


def plan(rows):
    if rows == 4:
        return [(3, 1, None), (0, 1, None), (3, 0, 1), (1, 2, None), (0, 2, 1), (2, 3, None)]
    flows = []
    for d in range(1, rows // 2 + 1):
        for s in range(rows if 2 * d < rows else rows // 2):
            flows.append((s, (s + d) % rows, None))
    return flows


def kernel(rows, cols, x_ref, out_ref, praw, panel, across, far_raw, stack, pacc, racc, psrc, pdst, rsrc, rdst,
           in_sem, ex_sem, own_sent, passed_sent, far_sent, parts_sent, back_sent,
           pr_sem, fr_sem, zr_sem, parts_here, back_here, x_ready, z_ready):
    p, c, l = lax.axis_index("row"), lax.axis_index("col"), lax.axis_index("layer")
    genes, part = x_ref.shape
    half = genes // 2
    cuts = 4
    piece = half // cuts
    samples = 2 * part
    other = 1 - l
    order = [k for k in range(cols) if k != 3] + [3]
    direct = [k for k in range(1, cols) if k != 3]
    last = cols - 1
    places = [(0, 0), (0, 1), (1, 1), (2, 0), (1, 0), (2, 1)] + [(k, s) for k in order[3:] for s in range(2)]
    ends = len(places)
    flows = plan(rows)
    slots = {t: [f for f in flows if f[1] == t] for t in range(rows)}
    outs = {s: [f for f in flows if f[0] == s and f[2] is None] for s in range(rows)}
    back = {s: [f for f in flows if f[0] == s] for s in range(rows)}
    pairs_of = {q: sorted({f[1] for f in flows if f[0] == q} | {f[0] for f in flows if f[1] == q}) for q in range(rows)}

    def held_back(f):
        return rows == 4 and f == (1, 2, None)

    def remote(src, dst, send, recv, device):
        return pltpu.make_async_remote_copy(
            src_ref=src, dst_ref=dst, send_sem=send, recv_sem=recv, device_id=device, device_id_type=MESH
        )

    def by_row(values):
        value = values[0]
        for q in range(1, rows):
            value = jnp.where(p == q, values[q], value)
        return value

    def at_row(q, condition=True):
        return pl.when(p == q)

    load = pltpu.make_async_copy(x_ref, praw.at[0, l], in_sem)
    load.start()

    barrier = pltpu.get_barrier_semaphore()

    def greet(device):
        pl.semaphore_signal(barrier, inc=1, device_id=device, device_id_type=MESH)

    alone = jnp.logical_and(p == 0, c == 0)

    @pl.when(jnp.logical_or(alone, l == 1))
    def _():
        greet((p, c, other))

    for k in direct:
        @pl.when(is_above(c, k))
        def _():
            for h in range(2):
                greet((p, flip(c, k), h))
    for q in range(rows):
        above = [t for t in pairs_of[q] if t > q]
        if above or any(held_back(f) for f in slots[q]):
            @pl.when(p == q)
            def _():
                for t in above:
                    for h in range(2):
                        greet((t, c, h))
                for f in slots[q]:
                    if held_back(f):
                        @pl.when(l == 1)
                        def _():
                            greet((f[0], c, 1))
    greetings = jnp.where(alone, 1, other) + by_row([2 * len([t for t in pairs_of[q] if t < q]) for q in range(rows)])
    for k in direct:
        greetings = greetings + jnp.where(is_above(c, k), 0, 2)

    greetings = greetings + l * by_row([len([f for f in outs[q] if held_back(f)]) for q in range(rows)])
    pacc[...] = jnp.zeros_like(pacc)
    racc[...] = jnp.zeros_like(racc)
    pl.semaphore_wait(barrier, greetings)

    @pl.when(l == 0)
    def _():
        for t in range(rows):
            below = [f for f in slots[t] if f[2] is None and f[0] < t]
            if below:
                @pl.when(p == t)
                def _():
                    for f in below:
                        for b in range(2):
                            pl.semaphore_signal(z_ready.at[outs[f[0]].index(f)], inc=2, device_id=(f[0], c, b), device_id_type=MESH)
        for k in direct:
            @pl.when(jnp.logical_not(is_above(c, k)))
            def _():
                for h in range(2):
                    pl.semaphore_signal(x_ready.at[k - 1], inc=1, device_id=(p, flip(c, k), h), device_id_type=MESH)
        pl.semaphore_signal(x_ready.at[2], inc=1, device_id=(p, c, other), device_id_type=MESH)

    load.wait()

    def z_copy(f, h, i):
        source = praw.at[0, l, pl.ds(h * half + i * piece, piece)]
        return remote(source, far_raw.at[slots[f[1]].index(f), l, pl.ds(i * piece, piece)],
                      far_sent, zr_sem.at[slots[f[1]].index(f), i], (f[1], c, h))

    def landed(ref, sem):
        remote(ref, ref, far_sent, sem, (p, c, other)).wait_recv()

    def left(ref, sem):
        remote(ref, ref, sem, zr_sem.at[0, 0], (p, c, other)).wait_send()

    def far_here(t, i):
        landed(far_raw.at[t, :, pl.ds(i * piece, piece)], zr_sem.at[t, i])

    def send_row(f, ask=False):
        ready = z_ready.at[outs[f[0]].index(f)]
        if held_back(f):
            for h in (1, 0):
                @pl.when(l == 1 - h)
                def _():
                    pl.semaphore_wait(ready, 2)

                for i in range(cuts // 2):
                    z_copy(f, h, i).start()
        else:
            if ask:
                pl.semaphore_wait(ready, 2)
            for i in range(cuts):
                for h in (1, 0):
                    z_copy(f, h, i).start()

    exchange = remote(praw.at[0, l], praw.at[0, l], own_sent, ex_sem, (p, c, other))

    @pl.when(l == 1)
    def _():
        pl.semaphore_wait(x_ready.at[2], 1)

    exchange.start()
    for q in range(rows):
        down = [f for f in outs[q] if f[1] < q]
        if down:
            @pl.when(p == q)
            def _():
                for f in down:
                    send_row(f)

    def stage(k, s):
        return {1: 1 - s, 2: s, 3: 2}.get(k, k - 1)

    def stage_here(n, u):
        landed(praw.at[0, l, pl.ds(0, half)], pr_sem.at[n, u])

    def panel_copy(k, s, u):
        at = pl.ds(s * half + u * half // 2, half // 2)
        return remote(praw.at[0, l, at], praw.at[order.index(k), l, at], own_sent, pr_sem.at[stage(k, s), u],
                      (p, flip(c, k), l))

    def pass_on(s, u):
        source, target = (2, 1) if s == 0 else (1, 2)
        at = pl.ds(s * half + u * half // 2, half // 2)
        return remote(praw.at[order.index(source), l, at], praw.at[last, l, at], passed_sent, pr_sem.at[2, u],
                      (p, flip(c, target), l))

    panel_copies = {(k, s, u): panel_copy(k, s, u) for k in direct for s in range(2) for u in range(2)}
    panel_copies.update({(3, s, u): pass_on(s, u) for s in range(2) for u in range(2)})

    def forward(k, s, u):
        at = praw.at[order.index(k), l, pl.ds(s * half + u * half // 2, half // 2)]
        return remote(at, at, passed_sent, fr_sem.at[stage(k, s)], (p, c, other))

    def complete(n):
        landed(praw.at[0, other], fr_sem.at[n])
        for k, s in places:
            if k and stage(k, s) == n:
                standardize(k, s)

    first = {1: (1, 0), 2: (0, 1)}
    for k in direct:
        @pl.when(jnp.logical_not(is_above(c, k)))
        def _():
            for s in first.get(k, (0, 1)):
                for u in range(2):
                    panel_copies[k, s, u].start()
    for k in direct:
        @pl.when(is_above(c, k))
        def _():
            pl.semaphore_wait(x_ready.at[k - 1], 1)
            for s in first.get(k, (0, 1)):
                for u in range(2):
                    panel_copies[k, s, u].start()
    for q in range(rows):
        up = [f for f in outs[q] if f[1] > q]
        if up:
            @pl.when(p == q)
            def _():
                for f in up:
                    send_row(f, ask=True)

    step = 32

    def scale(low, high):
        low, high = low.astype(jnp.float32), high.astype(jnp.float32)
        total = jnp.sum(low, axis=1, keepdims=True) + jnp.sum(high, axis=1, keepdims=True)
        squares = jnp.sum(low * low + high * high, axis=1, keepdims=True)
        average = total / samples
        variance = squares / samples - average * average
        gain = lax.rsqrt(variance + epsilon)
        return (((low - average) * gain).astype(jnp.bfloat16), ((high - average) * gain).astype(jnp.bfloat16))

    def standardize(k, s):
        n, place = order.index(k), places.index((k, s))
        for i in range(half // step):
            at = pl.ds(s * half + i * step, step)
            low, high = scale(praw[n, 0, at, :], praw[n, 1, at, :])
            at = pl.ds(place * half + i * step, step)
            panel[at, 0:part] = low
            panel[at, part:samples] = high

    def slot_at(t):
        return (1 + t) * half

    def standardize_far(t, first, stop):
        for j in range(first // piece, stop // piece):
            at = pl.ds(j * piece, piece)
            low, high = scale(far_raw[t, 0, at, :], far_raw[t, 1, at, :])
            at = pl.ds(slot_at(t) + j * piece, piece)
            stack[at, 0:part] = low
            stack[at, part:samples] = high

    def turn(start, end):
        for at in range(start * half, end * half, 128):
            across[:, at:at + 128] = panel[at:at + 128, :].T

    def pairs(first, stop, start, end, turned=False):
        if turned:
            product = jnp.dot(stack[first:stop, :], across[:, start * half:end * half], preferred_element_type=jnp.float32)
        else:
            product = lax.dot_general(
                stack[first:stop, :], panel[start * half:end * half, :], (((1,), (1,)), ((), ())),
                preferred_element_type=jnp.float32
            )
        shifted = product * (0.5 / samples) + 0.5
        square = shifted * shifted
        fourth = square * square
        eighth = fourth * fourth
        value = eighth * fourth
        width = value.shape[1]
        pacc[:, start * half:end * half] += jnp.sum(value.reshape((stop - first) // 8, 8, width), axis=0)
        skipped = max(half - first, 0)
        if first + skipped < stop:
            value = value[skipped:]
            lanes = value[:, 0:128]
            for j in range(1, width // 128):
                lanes = lanes + value[:, j * 128:(j + 1) * 128]
            racc[first + skipped - half:stop - half, :] += lanes

    exchange.wait_recv()
    for s in range(2):
        standardize(0, s)
    stack[0:half, :] = panel[pl.ds(pl.multiple_of(l * half, half), half), :]
    pairs(0, half, 0, 2)
    turn(0, 2)

    relays = [f for f in flows if f[2] is not None]

    def passed(f):
        return slots[f[2]].index((f[0], f[2], None))

    def relay_copy(f, b, i):
        at, t = pl.ds(i * piece, piece), slots[f[1]].index(f)
        return remote(far_raw.at[passed(f), b, at], far_raw.at[t, b, at],
                      far_sent, zr_sem.at[t, i], (f[1], c, l))

    def relay(n, i):
        for f in relays[n:n + 1]:
            @pl.when(p == f[2])
            def _():
                far_here(passed(f), i)
                for b in range(2):
                    relay_copy(f, b, i).start()

    for n, i in [(1, 0), (0, 0), (1, 1)]:
        relay(n, i)
    for u in range(2):
        stage_here(0, u)
        for s in range(2):
            panel_copies[3, s, u].start()
            forward(2 - s, s, u).start()
    for n, i in [(0, 1), (1, 2)]:
        relay(n, i)
    complete(0)
    pairs(0, half, 2, 4)
    turn(2, 4)
    for n, i in [(1, 3), (0, 2)]:
        relay(n, i)
    for f in flows:
        if held_back(f):
            @pl.when(p == f[0])
            def _():
                for i in range(cuts // 2, cuts):
                    for h in ((1, 0) if i < cuts - 1 else (0, 1)):
                        z_copy(f, h, i).start()
    for u in range(2):
        stage_here(1, u)
        for s in range(2):
            forward(1 + s, s, u).start()
    relay(0, 3)

    def take_far(t, i):
        passing = [f[2] for f in relays if passed(f) == t]
        if passing:
            @pl.when(p != passing[0])
            def _():
                far_here(t, i)
        else:
            far_here(t, i)

    def back_copy(f):
        t, j = slots[f[1]].index(f), back[f[0]].index(f)
        return remote(rsrc.at[t], rdst.at[j], back_sent, back_here, (f[0], c, l))

    def give_back(t):
        turned = racc[t * half:(t + 1) * half, :].T
        rsrc[t] = jnp.sum(turned.reshape(128 // 8, 8, half), axis=0)
        for q in range(rows):
            if t < len(slots[q]):
                @pl.when(p == q)
                def _():
                    back_copy(slots[q][t]).start()

    depth = max(len(slots[q]) for q in range(rows))
    n_slots = by_row([len(slots[q]) for q in range(rows)])
    middle = half + half // 2

    def take_block(t):
        for i in range(cuts):
            take_far(t, i)
        standardize_far(t, 0, half)

    soon = by_row([2 if any(f[2] == q for f in flows) else 1 for q in range(rows)])
    for i in range(cuts // 2):
        take_far(0, i)
    standardize_far(0, 0, half // 2)
    pairs(half, middle, 0, 4, True)
    for t in range(1, depth):
        @pl.when(jnp.minimum(n_slots, soon) > t)
        def _():
            take_block(t)
            pairs(slot_at(t), slot_at(t) + half, 0, 4, True)

    complete(1)
    for k in direct[2:]:
        for u in range(2):
            stage_here(stage(k, 0), u)
            for s in range(2):
                forward(k, s, u).start()
        complete(stage(k, 0))
    pairs(0, middle, 4, ends - 2)
    for u in range(2):
        stage_here(2, u)
        for s in range(2):
            forward(3, s, u).start()
    turn(4, ends - 2)
    for t in range(1, depth):
        @pl.when(n_slots > t)
        def _():
            @pl.when(soon > t)
            def _():
                pairs(slot_at(t), slot_at(t) + half, 4, ends - 2, True)

            @pl.when(soon <= t)
            def _():
                take_block(t)
                pairs(slot_at(t), slot_at(t) + half, 0, ends - 2, True)

    def part_copy(k, h):
        return remote(psrc.at[2 * k + h], pdst.at[2 * k + l], parts_sent, parts_here, (p, flip(c, k), h))

    def take_last():
        for i in range(cuts // 2, cuts):
            take_far(0, i)
        standardize_far(0, half // 2, half)

    def finish_panel():
        complete(2)
        for t in range(1, depth):
            @pl.when(n_slots > t)
            def _():
                pairs(slot_at(t), slot_at(t) + half, ends - 2, ends)
                give_back(t)

    def send_parts(k):
        for h in range(2):
            place = places.index((k, h))
            psrc[2 * k + h] = pacc[:, place * half:(place + 1) * half]
            if k:
                part_copy(k, h).start()

    kind = by_row([2 if any(held_back(f) for f in slots[q]) else 1 if slots[q] and slots[q][0][2] is not None else 0
                   for q in range(rows)])

    @pl.when(kind == 2)
    def _():
        finish_panel()
        pairs(0, middle, ends - 2, ends)
        turn(ends - 2, ends)
        final = 2 * half - piece
        for i in range(cuts // 2, cuts - 1):
            take_far(0, i)
        standardize_far(0, half // 2, half - piece)
        pairs(middle, final, 0, ends, True)
        take_far(0, cuts - 1)
        standardize_far(0, half - piece, half)
        pairs(final, 2 * half, ends - 2, ends, True)
        send_parts(3)
        pairs(final, 2 * half, 0, ends - 2, True)

    @pl.when(kind == 1)
    def _():
        finish_panel()
        take_last()
        pairs(0, 2 * half, ends - 2, ends)
        send_parts(3)
        pairs(middle, 2 * half, 0, ends - 2, True)

    @pl.when(kind == 0)
    def _():
        take_last()
        pairs(middle, 2 * half, 0, ends - 2, True)
        finish_panel()
        pairs(0, 2 * half, ends - 2, ends)
        send_parts(3)

    sums_first = p < rows // 2

    for k in direct:
        send_parts(k)

    @pl.when(jnp.logical_not(sums_first))
    def _():
        give_back(0)

    send_parts(0)
    part_copy(0, other).start()

    @pl.when(sums_first)
    def _():
        give_back(0)

    left(praw.at[pl.ds(0, last), l], own_sent)
    left(praw.at[:, l], passed_sent)
    left(psrc.at[pl.ds(0, 2 * cols - 1)], parts_sent)
    for q in range(rows):
        @pl.when(p == q)
        def _():
            blocks = len(outs[q]) + len([f for f in relays if f[2] == q])
            if blocks:
                left(praw.at[pl.ds(0, blocks), l], far_sent)
            if slots[q]:
                left(rsrc.at[pl.ds(0, len(slots[q]))], back_sent)

    total = psrc[l] - 1.0 / 8
    landed(pdst.at[pl.ds(0, 2 * cols - 1)], parts_here)
    total = total + pdst[other]
    for n in range(2, 2 * cols):
        total = total + pdst[n]
    psrc[l] = total
    for q in range(rows):
        if back[q]:
            @pl.when(p == q)
            def _():
                landed(rdst.at[pl.ds(0, len(back[q]))], back_here)
                more = rdst[0]
                for j in range(1, len(back[q])):
                    more = more + rdst[j]
                psrc[l] += more
    out_ref[...] = jnp.sum(psrc[l], axis=0)


def solution(mesh):
    rows, cols = mesh.shape["row"], mesh.shape["col"]
    flows = plan(rows)
    depth = max(len([f for f in flows if f[1] == q]) for q in range(rows))
    fan = max(len([f for f in flows if f[0] == q]) for q in range(rows))
    dma = lambda *shape: pltpu.SemaphoreType.DMA(shape)

    def on_device(expression):
        genes, part = expression.shape
        half, samples = genes // 2, 2 * part
        bf16, f32 = jnp.bfloat16, jnp.float32
        summed = pl.pallas_call(
            functools.partial(kernel, rows, cols),
            out_shape=jax.ShapeDtypeStruct((half,), f32),
            in_specs=[pl.BlockSpec(memory_space=pl.ANY)],
            out_specs=pl.BlockSpec(memory_space=pltpu.VMEM),
            scratch_shapes=[
                pltpu.VMEM((cols, 2, genes, part), bf16),
                pltpu.VMEM((cols * genes, samples), bf16),
                pltpu.VMEM((samples, cols * genes), bf16),
                pltpu.VMEM((depth, 2, half, part), bf16),
                pltpu.VMEM(((1 + depth) * half, samples), bf16),
                pltpu.VMEM((8, cols * genes), f32),
                pltpu.VMEM((depth * half, 128), f32),
                pltpu.VMEM((2 * cols, 8, half), f32),
                pltpu.VMEM((2 * cols, 8, half), f32),
                pltpu.VMEM((depth, 8, half), f32),
                pltpu.VMEM((fan, 8, half), f32),
                *[pltpu.SemaphoreType.DMA] * 7,
                dma(cols - 1, 2), dma(cols - 1), dma(depth, 4),
                pltpu.SemaphoreType.DMA, pltpu.SemaphoreType.DMA,
                pltpu.SemaphoreType.REGULAR((cols - 1,)),
                pltpu.SemaphoreType.REGULAR((fan,)),
            ],
            compiler_params=pltpu.CompilerParams(collective_id=0, has_side_effects=True, vmem_limit_bytes=48000000),
        )(pltpu.with_memory_space_constraint(expression, pltpu.HBM))
        return summed

    return jax.shard_map(
        on_device,
        mesh=mesh,
        in_specs=(P(("row", "col"), "layer"),),
        out_specs=P(("row", "col", "layer")),
        check_vma=False,
    )
```

```python
import functools

import jax
import jax.numpy as jnp
from jax import lax
from jax.experimental import pallas as pl
from jax.experimental.pallas import tpu as pltpu
from jax.sharding import PartitionSpec as P

MESH = pl.DeviceIdType.MESH
epsilon = 1e-05


def flip(c, k):
    bit = 1
    while bit <= k:
        if k & bit:
            c = c + bit - 2 * bit * lax.rem(lax.div(c, bit), 2)
        bit *= 2
    return c


def is_above(c, k):
    top = 1 << (k.bit_length() - 1)
    return lax.rem(lax.div(c, top), 2) == 0


def plan(rows):
    if rows == 4:
        return [(3, 1, None), (0, 1, None), (3, 0, 1), (1, 2, None), (0, 2, 1), (2, 3, None)]
    flows = []
    for d in range(1, rows // 2 + 1):
        for s in range(rows if 2 * d < rows else rows // 2):
            flows.append((s, (s + d) % rows, None))
    return flows


def kernel(rows, cols, x_ref, out_ref, praw, panel, across, far_raw, stack, pacc, racc, psrc, pdst, rsrc, rdst,
           in_sem, ex_sem, own_sent, passed_sent, far_sent, parts_sent, back_sent,
           pr_sem, fr_sem, zr_sem, parts_here, back_here, x_ready, z_ready):
    p, c, l = lax.axis_index("row"), lax.axis_index("col"), lax.axis_index("layer")
    genes, part = x_ref.shape
    half = genes // 2
    cuts = 4
    piece = half // cuts
    samples = 2 * part
    other = 1 - l
    order = [k for k in range(cols) if k != 3] + [3]
    direct = [k for k in range(1, cols) if k != 3]
    last = cols - 1
    places = [(0, 0), (0, 1), (1, 1), (2, 0), (1, 0), (2, 1)] + [(k, s) for k in order[3:] for s in range(2)]
    ends = len(places)
    flows = plan(rows)
    slots = {t: [f for f in flows if f[1] == t] for t in range(rows)}
    outs = {s: [f for f in flows if f[0] == s and f[2] is None] for s in range(rows)}
    back = {s: [f for f in flows if f[0] == s] for s in range(rows)}
    pairs_of = {q: sorted({f[1] for f in flows if f[0] == q} | {f[0] for f in flows if f[1] == q}) for q in range(rows)}

    def held_back(f):
        return rows == 4 and f == (1, 2, None)

    def quick(f):
        return rows == 4 and f in ((0, 1, None), (1, 2, None))

    def remote(src, dst, send, recv, device):
        return pltpu.make_async_remote_copy(
            src_ref=src, dst_ref=dst, send_sem=send, recv_sem=recv, device_id=device, device_id_type=MESH
        )

    def by_row(values):
        value = values[0]
        for q in range(1, rows):
            value = jnp.where(p == q, values[q], value)
        return value

    def at_row(q, condition=True):
        return pl.when(p == q)

    load = pltpu.make_async_copy(x_ref, praw.at[0, l], in_sem)
    load.start()

    barrier = pltpu.get_barrier_semaphore()

    def greet(device):
        pl.semaphore_signal(barrier, inc=1, device_id=device, device_id_type=MESH)

    alone = jnp.logical_and(p == 0, c == 0)

    @pl.when(jnp.logical_or(alone, l == 1))
    def _():
        greet((p, c, other))

    for k in direct:
        @pl.when(is_above(c, k))
        def _():
            for h in range(2):
                greet((p, flip(c, k), h))
    for q in range(rows):
        above = [t for t in pairs_of[q] if t > q]
        if above or any(quick(f) for f in slots[q]):
            @pl.when(p == q)
            def _():
                for t in above:
                    for h in range(2):
                        greet((t, c, h))
                for f in slots[q]:
                    if quick(f):
                        @pl.when(l == 1)
                        def _():
                            greet((f[0], c, 1))
    greetings = jnp.where(alone, 1, other) + by_row([2 * len([t for t in pairs_of[q] if t < q]) for q in range(rows)])
    for k in direct:
        greetings = greetings + jnp.where(is_above(c, k), 0, 2)

    greetings = greetings + l * by_row([len([f for f in outs[q] if quick(f)]) for q in range(rows)])
    pacc[...] = jnp.zeros_like(pacc)
    racc[...] = jnp.zeros_like(racc)
    pl.semaphore_wait(barrier, greetings)

    @pl.when(l == 0)
    def _():
        for t in range(rows):
            below = [f for f in slots[t] if f[2] is None and f[0] < t]
            if below:
                @pl.when(p == t)
                def _():
                    for f in below:
                        for b in range(2):
                            pl.semaphore_signal(z_ready.at[outs[f[0]].index(f)], inc=2, device_id=(f[0], c, b), device_id_type=MESH)
        for k in direct:
            @pl.when(jnp.logical_not(is_above(c, k)))
            def _():
                for h in range(2):
                    pl.semaphore_signal(x_ready.at[k - 1], inc=1, device_id=(p, flip(c, k), h), device_id_type=MESH)
        pl.semaphore_signal(x_ready.at[2], inc=1, device_id=(p, c, other), device_id_type=MESH)

    load.wait()

    def z_copy(f, h, i):
        source = praw.at[0, l, pl.ds(h * half + i * piece, piece)]
        return remote(source, far_raw.at[slots[f[1]].index(f), l, pl.ds(i * piece, piece)],
                      far_sent, zr_sem.at[slots[f[1]].index(f), i], (f[1], c, h))

    def landed(ref, sem):
        remote(ref, ref, far_sent, sem, (p, c, other)).wait_recv()

    def left(ref, sem):
        remote(ref, ref, sem, zr_sem.at[0, 0], (p, c, other)).wait_send()

    def far_here(t, i):
        landed(far_raw.at[t, :, pl.ds(i * piece, piece)], zr_sem.at[t, i])

    def send_row(f, ask=False):
        ready = z_ready.at[outs[f[0]].index(f)]
        if held_back(f):
            order_of = [(h, i) for h in (1, 0) for i in range(cuts // 2)]
        else:
            order_of = [(h, i) for i in range(cuts) for h in (1, 0)]
        early = order_of.index((0, 0)) if quick(f) else 0
        for n, (h, i) in enumerate(order_of):
            if ask and n in (0, early):
                @pl.when(jnp.logical_or(early == 0, l == (1 if n else 0)))
                def _():
                    pl.semaphore_wait(ready, 2)

            z_copy(f, h, i).start()

    exchange = remote(praw.at[0, l], praw.at[0, l], own_sent, ex_sem, (p, c, other))

    @pl.when(l == 1)
    def _():
        pl.semaphore_wait(x_ready.at[2], 1)

    exchange.start()
    for q in range(rows):
        down = [f for f in outs[q] if f[1] < q]
        if down:
            @pl.when(p == q)
            def _():
                for f in down:
                    send_row(f)

    def stage(k, s):
        return {1: 1 - s, 2: s, 3: 2}.get(k, k - 1)

    def stage_here(n, u):
        landed(praw.at[0, l, pl.ds(0, half)], pr_sem.at[n, u])

    def panel_copy(k, s, u):
        at = pl.ds(s * half + u * half // 2, half // 2)
        return remote(praw.at[0, l, at], praw.at[order.index(k), l, at], own_sent, pr_sem.at[stage(k, s), u],
                      (p, flip(c, k), l))

    def pass_on(s, u):
        source, target = (2, 1) if s == 0 else (1, 2)
        at = pl.ds(s * half + u * half // 2, half // 2)
        return remote(praw.at[order.index(source), l, at], praw.at[last, l, at], passed_sent, pr_sem.at[2, u],
                      (p, flip(c, target), l))

    panel_copies = {(k, s, u): panel_copy(k, s, u) for k in direct for s in range(2) for u in range(2)}
    panel_copies.update({(3, s, u): pass_on(s, u) for s in range(2) for u in range(2)})

    def forward(k, s, u):
        at = praw.at[order.index(k), l, pl.ds(s * half + u * half // 2, half // 2)]
        return remote(at, at, passed_sent, fr_sem.at[stage(k, s)], (p, c, other))

    def complete(n):
        landed(praw.at[0, other], fr_sem.at[n])
        for k, s in places:
            if k and stage(k, s) == n:
                standardize(k, s)

    first = {1: (1, 0), 2: (0, 1)}
    for k in direct:
        @pl.when(jnp.logical_not(is_above(c, k)))
        def _():
            for s in first.get(k, (0, 1)):
                for u in range(2):
                    panel_copies[k, s, u].start()
    for k in direct:
        @pl.when(is_above(c, k))
        def _():
            pl.semaphore_wait(x_ready.at[k - 1], 1)
            for s in first.get(k, (0, 1)):
                for u in range(2):
                    panel_copies[k, s, u].start()
    for q in range(rows):
        up = [f for f in outs[q] if f[1] > q]
        if up:
            @pl.when(p == q)
            def _():
                for f in up:
                    send_row(f, ask=True)

    step = 32

    def scale(low, high):
        low, high = low.astype(jnp.float32), high.astype(jnp.float32)
        total = jnp.sum(low, axis=1, keepdims=True) + jnp.sum(high, axis=1, keepdims=True)
        squares = jnp.sum(low * low + high * high, axis=1, keepdims=True)
        average = total / samples
        variance = squares / samples - average * average
        gain = lax.rsqrt(variance + epsilon)
        return (((low - average) * gain).astype(jnp.bfloat16), ((high - average) * gain).astype(jnp.bfloat16))

    def standardize(k, s):
        n, place = order.index(k), places.index((k, s))
        for i in range(half // step):
            at = pl.ds(s * half + i * step, step)
            low, high = scale(praw[n, 0, at, :], praw[n, 1, at, :])
            at = pl.ds(place * half + i * step, step)
            panel[at, 0:part] = low
            panel[at, part:samples] = high

    def slot_at(t):
        return (1 + t) * half

    def standardize_far(t, first, stop):
        for j in range(first // piece, stop // piece):
            at = pl.ds(j * piece, piece)
            low, high = scale(far_raw[t, 0, at, :], far_raw[t, 1, at, :])
            at = pl.ds(slot_at(t) + j * piece, piece)
            stack[at, 0:part] = low
            stack[at, part:samples] = high

    def turn(start, end):
        for at in range(start * half, end * half, 128):
            across[:, at:at + 128] = panel[at:at + 128, :].T

    def pairs(first, stop, start, end, turned=False):
        if turned:
            product = jnp.dot(stack[first:stop, :], across[:, start * half:end * half], preferred_element_type=jnp.float32)
        else:
            product = lax.dot_general(
                stack[first:stop, :], panel[start * half:end * half, :], (((1,), (1,)), ((), ())),
                preferred_element_type=jnp.float32
            )
        shifted = product * (0.5 / samples) + 0.5
        square = shifted * shifted
        fourth = square * square
        eighth = fourth * fourth
        value = eighth * fourth
        width = value.shape[1]
        pacc[:, start * half:end * half] += jnp.sum(value.reshape((stop - first) // 8, 8, width), axis=0)
        skipped = max(half - first, 0)
        if first + skipped < stop:
            value = value[skipped:]
            lanes = value[:, 0:128]
            for j in range(1, width // 128):
                lanes = lanes + value[:, j * 128:(j + 1) * 128]
            racc[first + skipped - half:stop - half, :] += lanes

    exchange.wait_recv()
    for s in range(2):
        standardize(0, s)
    stack[0:half, :] = panel[pl.ds(pl.multiple_of(l * half, half), half), :]
    pairs(0, half, 0, 2)
    turn(0, 2)

    relays = [f for f in flows if f[2] is not None]

    def passed(f):
        return slots[f[2]].index((f[0], f[2], None))

    def relay_copy(f, b, i):
        at, t = pl.ds(i * piece, piece), slots[f[1]].index(f)
        return remote(far_raw.at[passed(f), b, at], far_raw.at[t, b, at],
                      far_sent, zr_sem.at[t, i], (f[1], c, l))

    def relay(n, i):
        for f in relays[n:n + 1]:
            @pl.when(p == f[2])
            def _():
                far_here(passed(f), i)
                for b in range(2):
                    relay_copy(f, b, i).start()

    for n, i in [(1, 0), (0, 0), (1, 1)]:
        relay(n, i)
    for u in range(2):
        stage_here(0, u)
        for s in range(2):
            panel_copies[3, s, u].start()
            forward(2 - s, s, u).start()
    for n, i in [(0, 1), (1, 2)]:
        relay(n, i)
    complete(0)
    pairs(0, half, 2, 4)
    relay(0, 2)
    relay(1, 3)
    for f in flows:
        if held_back(f):
            @pl.when(p == f[0])
            def _():
                for i in range(cuts // 2, cuts):
                    for h in ((1, 0) if i < cuts - 1 else (0, 1)):
                        z_copy(f, h, i).start()
    turn(2, 4)
    for u in range(2):
        stage_here(1, u)
        for s in range(2):
            forward(1 + s, s, u).start()
    relay(0, 3)

    def take_far(t, i):
        passing = [f[2] for f in relays if passed(f) == t]
        if passing:
            @pl.when(p != passing[0])
            def _():
                far_here(t, i)
        else:
            far_here(t, i)

    def back_copy(f):
        t, j = slots[f[1]].index(f), back[f[0]].index(f)
        return remote(rsrc.at[t], rdst.at[j], back_sent, back_here, (f[0], c, l))

    def give_back(t):
        turned = racc[t * half:(t + 1) * half, :].T
        rsrc[t] = jnp.sum(turned.reshape(128 // 8, 8, half), axis=0)
        for q in range(rows):
            if t < len(slots[q]):
                @pl.when(p == q)
                def _():
                    back_copy(slots[q][t]).start()

    depth = max(len(slots[q]) for q in range(rows))
    n_slots = by_row([len(slots[q]) for q in range(rows)])
    middle = half + half // 2

    def take_block(t):
        for i in range(cuts):
            take_far(t, i)
        standardize_far(t, 0, half)

    soon = by_row([2 if any(f[2] == q for f in flows) else 1 for q in range(rows)])
    for i in range(cuts // 2):
        take_far(0, i)
    standardize_far(0, 0, half // 2)
    pairs(half, middle, 0, 4, True)
    for t in range(1, depth):
        @pl.when(jnp.minimum(n_slots, soon) > t)
        def _():
            take_block(t)
            pairs(slot_at(t), slot_at(t) + half, 0, 4, True)

    complete(1)
    for k in direct[2:]:
        for u in range(2):
            stage_here(stage(k, 0), u)
            for s in range(2):
                forward(k, s, u).start()
        complete(stage(k, 0))
    pairs(0, middle, 4, ends - 2)
    for u in range(2):
        stage_here(2, u)
        for s in range(2):
            forward(3, s, u).start()
    turn(4, ends - 2)
    for t in range(1, depth):
        @pl.when(n_slots > t)
        def _():
            @pl.when(soon > t)
            def _():
                pairs(slot_at(t), slot_at(t) + half, 4, ends - 2, True)

            @pl.when(soon <= t)
            def _():
                take_block(t)
                pairs(slot_at(t), slot_at(t) + half, 0, ends - 2, True)

    def part_copy(k, h):
        return remote(psrc.at[2 * k + h], pdst.at[2 * k + l], parts_sent, parts_here, (p, flip(c, k), h))

    def take_last():
        for i in range(cuts // 2, cuts):
            take_far(0, i)
        standardize_far(0, half // 2, half)

    def finish_panel():
        complete(2)
        for t in range(1, depth):
            @pl.when(n_slots > t)
            def _():
                pairs(slot_at(t), slot_at(t) + half, ends - 2, ends)
                give_back(t)

    def send_parts(k):
        for h in range(2):
            place = places.index((k, h))
            psrc[2 * k + h] = pacc[:, place * half:(place + 1) * half]
            if k:
                part_copy(k, h).start()

    kind = by_row([2 if any(held_back(f) for f in slots[q]) else 1 if slots[q] and slots[q][0][2] is not None else 0
                   for q in range(rows)])

    @pl.when(kind == 2)
    def _():
        finish_panel()
        pairs(0, middle, ends - 2, ends)
        turn(ends - 2, ends)
        final = 2 * half - piece
        for i in range(cuts // 2, cuts - 1):
            take_far(0, i)
        standardize_far(0, half // 2, half - piece)
        pairs(middle, final, 0, ends, True)
        take_far(0, cuts - 1)
        standardize_far(0, half - piece, half)
        pairs(final, 2 * half, ends - 2, ends, True)
        send_parts(3)
        pairs(final, 2 * half, 0, ends - 2, True)

    @pl.when(kind == 1)
    def _():
        finish_panel()
        take_last()
        pairs(0, 2 * half, ends - 2, ends)
        send_parts(3)
        pairs(middle, 2 * half, 0, ends - 2, True)

    @pl.when(kind == 0)
    def _():
        take_last()
        pairs(middle, 2 * half, 0, ends - 2, True)
        finish_panel()
        pairs(0, 2 * half, ends - 2, ends)
        send_parts(3)

    sums_first = p < rows // 2

    for k in direct:
        send_parts(k)

    @pl.when(jnp.logical_not(sums_first))
    def _():
        give_back(0)

    send_parts(0)
    part_copy(0, other).start()

    @pl.when(sums_first)
    def _():
        give_back(0)

    left(praw.at[pl.ds(0, last), l], own_sent)
    left(praw.at[:, l], passed_sent)
    left(psrc.at[pl.ds(0, 2 * cols - 1)], parts_sent)
    for q in range(rows):
        @pl.when(p == q)
        def _():
            blocks = len(outs[q]) + len([f for f in relays if f[2] == q])
            if blocks:
                left(praw.at[pl.ds(0, blocks), l], far_sent)
            if slots[q]:
                left(rsrc.at[pl.ds(0, len(slots[q]))], back_sent)

    total = psrc[l] - 1.0 / 8
    landed(pdst.at[pl.ds(0, 2 * cols - 1)], parts_here)
    total = total + pdst[other]
    for n in range(2, 2 * cols):
        total = total + pdst[n]
    psrc[l] = total
    for q in range(rows):
        if back[q]:
            @pl.when(p == q)
            def _():
                landed(rdst.at[pl.ds(0, len(back[q]))], back_here)
                more = rdst[0]
                for j in range(1, len(back[q])):
                    more = more + rdst[j]
                psrc[l] += more
    out_ref[...] = jnp.sum(psrc[l], axis=0)


def solution(mesh):
    rows, cols = mesh.shape["row"], mesh.shape["col"]
    flows = plan(rows)
    depth = max(len([f for f in flows if f[1] == q]) for q in range(rows))
    fan = max(len([f for f in flows if f[0] == q]) for q in range(rows))
    dma = lambda *shape: pltpu.SemaphoreType.DMA(shape)

    def on_device(expression):
        genes, part = expression.shape
        half, samples = genes // 2, 2 * part
        bf16, f32 = jnp.bfloat16, jnp.float32
        summed = pl.pallas_call(
            functools.partial(kernel, rows, cols),
            out_shape=jax.ShapeDtypeStruct((half,), f32),
            in_specs=[pl.BlockSpec(memory_space=pl.ANY)],
            out_specs=pl.BlockSpec(memory_space=pltpu.VMEM),
            scratch_shapes=[
                pltpu.VMEM((cols, 2, genes, part), bf16),
                pltpu.VMEM((cols * genes, samples), bf16),
                pltpu.VMEM((samples, cols * genes), bf16),
                pltpu.VMEM((depth, 2, half, part), bf16),
                pltpu.VMEM(((1 + depth) * half, samples), bf16),
                pltpu.VMEM((8, cols * genes), f32),
                pltpu.VMEM((depth * half, 128), f32),
                pltpu.VMEM((2 * cols, 8, half), f32),
                pltpu.VMEM((2 * cols, 8, half), f32),
                pltpu.VMEM((depth, 8, half), f32),
                pltpu.VMEM((fan, 8, half), f32),
                *[pltpu.SemaphoreType.DMA] * 7,
                dma(cols - 1, 2), dma(cols - 1), dma(depth, 4),
                pltpu.SemaphoreType.DMA, pltpu.SemaphoreType.DMA,
                pltpu.SemaphoreType.REGULAR((cols - 1,)),
                pltpu.SemaphoreType.REGULAR((max(len([f for f in flows if f[0] == q and f[2] is None]) for q in range(rows)),)),
            ],
            compiler_params=pltpu.CompilerParams(collective_id=0, has_side_effects=True, vmem_limit_bytes=48000000),
        )(pltpu.with_memory_space_constraint(expression, pltpu.HBM))
        return summed

    return jax.shard_map(
        on_device,
        mesh=mesh,
        in_specs=(P(("row", "col"), "layer"),),
        out_specs=P(("row", "col", "layer")),
        check_vma=False,
    )
```

```python
import functools

import jax
import jax.numpy as jnp
from jax import lax
from jax.experimental import pallas as pl
from jax.experimental.pallas import tpu as pltpu
from jax.sharding import PartitionSpec as P

MESH = pl.DeviceIdType.MESH
epsilon = 1e-05


def flip(c, k):
    bit = 1
    while bit <= k:
        if k & bit:
            c = c + bit - 2 * bit * lax.rem(lax.div(c, bit), 2)
        bit *= 2
    return c


def is_above(c, k):
    top = 1 << (k.bit_length() - 1)
    return lax.rem(lax.div(c, top), 2) == 0


def plan(rows):
    if rows == 4:
        return [(3, 1, None), (0, 1, None), (3, 0, 1), (1, 2, None), (0, 2, 1), (2, 3, None)]
    flows = []
    for d in range(1, rows // 2 + 1):
        for s in range(rows if 2 * d < rows else rows // 2):
            flows.append((s, (s + d) % rows, None))
    return flows


def kernel(rows, cols, x_ref, out_ref, praw, panel, across, far_raw, stack, pacc, racc, psrc, pdst, rsrc, rdst,
           ex_sem, own_sent, far_sent, parts_sent,
           pr_sem, fr_sem, zr_sem, parts_here, x_ready, z_ready):
    p, c, l = lax.axis_index("row"), lax.axis_index("col"), lax.axis_index("layer")
    genes, part = x_ref.shape
    half = genes // 2
    cuts = 4
    piece = half // cuts
    samples = 2 * part
    other = 1 - l
    order = [k for k in range(cols) if k != 3] + [3]
    direct = [k for k in range(1, cols) if k != 3]
    last = cols - 1
    places = [(0, 0), (0, 1), (1, 1), (2, 0), (1, 0), (2, 1)] + [(k, s) for k in order[3:] for s in range(2)]
    ends = len(places)
    flows = plan(rows)
    slots = {t: [f for f in flows if f[1] == t] for t in range(rows)}
    outs = {s: [f for f in flows if f[0] == s and f[2] is None] for s in range(rows)}
    back = {s: [f for f in flows if f[0] == s] for s in range(rows)}
    pairs_of = {q: sorted({f[1] for f in flows if f[0] == q} | {f[0] for f in flows if f[1] == q}) for q in range(rows)}

    def held_back(f):
        return rows == 4 and f == (1, 2, None)

    def quick(f):
        return rows == 4 and f in ((0, 1, None), (1, 2, None))

    def remote(src, dst, send, recv, device):
        return pltpu.make_async_remote_copy(
            src_ref=src, dst_ref=dst, send_sem=send, recv_sem=recv, device_id=device, device_id_type=MESH
        )

    def by_row(values):
        value = values[0]
        for q in range(1, rows):
            value = jnp.where(p == q, values[q], value)
        return value

    def at_row(q, condition=True):
        return pl.when(p == q)

    load = pltpu.make_async_copy(x_ref, praw.at[0, l], parts_sent)
    load.start()

    barrier = pltpu.get_barrier_semaphore()

    def greet(device):
        pl.semaphore_signal(barrier, inc=1, device_id=device, device_id_type=MESH)

    alone = jnp.logical_and(p == 0, c == 0)

    @pl.when(jnp.logical_or(alone, l == 1))
    def _():
        greet((p, c, other))

    for k in direct:
        @pl.when(is_above(c, k))
        def _():
            for h in range(2):
                greet((p, flip(c, k), h))
    for q in range(rows):
        above = [t for t in pairs_of[q] if t > q]
        if above or any(quick(f) for f in slots[q]):
            @pl.when(p == q)
            def _():
                for t in above:
                    for h in range(2):
                        greet((t, c, h))
                for f in slots[q]:
                    if quick(f):
                        @pl.when(l == 1)
                        def _():
                            greet((f[0], c, 1))
    greetings = jnp.where(alone, 1, other) + by_row([2 * len([t for t in pairs_of[q] if t < q]) for q in range(rows)])
    for k in direct:
        greetings = greetings + jnp.where(is_above(c, k), 0, 2)

    greetings = greetings + l * by_row([len([f for f in outs[q] if quick(f)]) for q in range(rows)])
    pacc[...] = jnp.zeros_like(pacc)
    racc[...] = jnp.zeros_like(racc)
    pl.semaphore_wait(barrier, greetings)

    @pl.when(l == 0)
    def _():
        for t in range(rows):
            below = [f for f in slots[t] if f[2] is None and f[0] < t]
            if below:
                @pl.when(p == t)
                def _():
                    for f in below:
                        for b in range(2):
                            pl.semaphore_signal(z_ready.at[outs[f[0]].index(f)], inc=2, device_id=(f[0], c, b), device_id_type=MESH)
        for k in direct:
            @pl.when(jnp.logical_not(is_above(c, k)))
            def _():
                for h in range(2):
                    pl.semaphore_signal(x_ready.at[k - 1], inc=1, device_id=(p, flip(c, k), h), device_id_type=MESH)
        pl.semaphore_signal(x_ready.at[2], inc=1, device_id=(p, c, other), device_id_type=MESH)

    load.wait()

    def z_copy(f, h, i):
        source = praw.at[0, l, pl.ds(h * half + i * piece, piece)]
        return remote(source, far_raw.at[slots[f[1]].index(f), l, pl.ds(i * piece, piece)],
                      far_sent, zr_sem.at[slots[f[1]].index(f), i], (f[1], c, h))

    def landed(ref, sem):
        remote(ref, ref, far_sent, sem, (p, c, other)).wait_recv()

    def left(ref, sem):
        remote(ref, ref, sem, zr_sem.at[0, 0], (p, c, other)).wait_send()

    def far_here(t, i):
        landed(far_raw.at[t, :, pl.ds(i * piece, piece)], zr_sem.at[t, i])

    def send_row(f, ask=False):
        ready = z_ready.at[outs[f[0]].index(f)]
        if held_back(f):
            order_of = [(h, i) for h in (1, 0) for i in range(cuts // 2)]
        else:
            order_of = [(h, i) for i in range(cuts) for h in (1, 0)]
        early = order_of.index((0, 0)) if quick(f) else 0
        for n, (h, i) in enumerate(order_of):
            if ask and n in (0, early):
                @pl.when(jnp.logical_or(early == 0, l == (1 if n else 0)))
                def _():
                    pl.semaphore_wait(ready, 2)

            z_copy(f, h, i).start()

    exchange = remote(praw.at[0, l], praw.at[0, l], own_sent, ex_sem, (p, c, other))

    @pl.when(l == 1)
    def _():
        pl.semaphore_wait(x_ready.at[2], 1)

    exchange.start()
    for q in range(rows):
        down = [f for f in outs[q] if f[1] < q]
        if down:
            @pl.when(p == q)
            def _():
                for f in down:
                    send_row(f)

    def stage(k, s):
        return {1: 1 - s, 2: s, 3: 2}.get(k, k - 1)

    def stage_here(n, u):
        landed(praw.at[0, l, pl.ds(0, half)], pr_sem.at[n, u])

    def panel_copy(k, s, u):
        at = pl.ds(s * half + u * half // 2, half // 2)
        return remote(praw.at[0, l, at], praw.at[order.index(k), l, at], own_sent, pr_sem.at[stage(k, s), u],
                      (p, flip(c, k), l))

    def pass_on(s, u):
        source, target = (2, 1) if s == 0 else (1, 2)
        at = pl.ds(s * half + u * half // 2, half // 2)
        return remote(praw.at[order.index(source), l, at], praw.at[last, l, at], own_sent, pr_sem.at[2, u],
                      (p, flip(c, target), l))

    panel_copies = {(k, s, u): panel_copy(k, s, u) for k in direct for s in range(2) for u in range(2)}
    panel_copies.update({(3, s, u): pass_on(s, u) for s in range(2) for u in range(2)})

    def forward(k, s, u):
        at = praw.at[order.index(k), l, pl.ds(s * half + u * half // 2, half // 2)]
        return remote(at, at, own_sent, fr_sem.at[stage(k, s)], (p, c, other))

    def complete(n):
        landed(praw.at[0, other], fr_sem.at[n])
        for k, s in places:
            if k and stage(k, s) == n:
                standardize(k, s)

    first = {1: (1, 0), 2: (0, 1)}
    for k in direct:
        @pl.when(jnp.logical_not(is_above(c, k)))
        def _():
            for s in first.get(k, (0, 1)):
                for u in range(2):
                    panel_copies[k, s, u].start()
    for k in direct:
        @pl.when(is_above(c, k))
        def _():
            pl.semaphore_wait(x_ready.at[k - 1], 1)
            for s in first.get(k, (0, 1)):
                for u in range(2):
                    panel_copies[k, s, u].start()
    for q in range(rows):
        up = [f for f in outs[q] if f[1] > q]
        if up:
            @pl.when(p == q)
            def _():
                for f in up:
                    send_row(f, ask=True)

    step = 32

    def scale(low, high):
        low, high = low.astype(jnp.float32), high.astype(jnp.float32)
        total = jnp.sum(low, axis=1, keepdims=True) + jnp.sum(high, axis=1, keepdims=True)
        squares = jnp.sum(low * low + high * high, axis=1, keepdims=True)
        average = total / samples
        variance = squares / samples - average * average
        gain = lax.rsqrt(variance + epsilon)
        return (((low - average) * gain).astype(jnp.bfloat16), ((high - average) * gain).astype(jnp.bfloat16))

    def standardize(k, s):
        n, place = order.index(k), places.index((k, s))
        for i in range(half // step):
            at = pl.ds(s * half + i * step, step)
            low, high = scale(praw[n, 0, at, :], praw[n, 1, at, :])
            at = pl.ds(place * half + i * step, step)
            panel[at, 0:part] = low
            panel[at, part:samples] = high

    def slot_at(t):
        return (1 + t) * half

    def standardize_far(t, first, stop):
        for j in range(first // piece, stop // piece):
            at = pl.ds(j * piece, piece)
            low, high = scale(far_raw[t, 0, at, :], far_raw[t, 1, at, :])
            at = pl.ds(slot_at(t) + j * piece, piece)
            stack[at, 0:part] = low
            stack[at, part:samples] = high

    def turn(start, end):
        for at in range(start * half, end * half, 128):
            across[:, at:at + 128] = panel[at:at + 128, :].T

    def pairs(first, stop, start, end, turned=False):
        if turned:
            product = jnp.dot(stack[first:stop, :], across[:, start * half:end * half], preferred_element_type=jnp.float32)
        else:
            product = lax.dot_general(
                stack[first:stop, :], panel[start * half:end * half, :], (((1,), (1,)), ((), ())),
                preferred_element_type=jnp.float32
            )
        shifted = product * (0.5 / samples) + 0.5
        square = shifted * shifted
        fourth = square * square
        eighth = fourth * fourth
        value = eighth * fourth
        width = value.shape[1]
        pacc[:, start * half:end * half] += jnp.sum(value.reshape((stop - first) // 8, 8, width), axis=0)
        skipped = max(half - first, 0)
        if first + skipped < stop:
            value = value[skipped:]
            lanes = value[:, 0:128]
            for j in range(1, width // 128):
                lanes = lanes + value[:, j * 128:(j + 1) * 128]
            racc[first + skipped - half:stop - half, :] += lanes

    exchange.wait_recv()
    for s in range(2):
        standardize(0, s)
    stack[0:half, :] = panel[pl.ds(pl.multiple_of(l * half, half), half), :]
    pairs(0, half, 0, 2)
    turn(0, 2)

    relays = [f for f in flows if f[2] is not None]

    def passed(f):
        return slots[f[2]].index((f[0], f[2], None))

    def relay_copy(f, b, i):
        at, t = pl.ds(i * piece, piece), slots[f[1]].index(f)
        return remote(far_raw.at[passed(f), b, at], far_raw.at[t, b, at],
                      far_sent, zr_sem.at[t, i], (f[1], c, l))

    def relay(n, i):
        for f in relays[n:n + 1]:
            @pl.when(p == f[2])
            def _():
                far_here(passed(f), i)
                for b in range(2):
                    relay_copy(f, b, i).start()

    for n, i in [(1, 0), (0, 0), (1, 1)]:
        relay(n, i)
    for u in range(2):
        stage_here(0, u)
        for s in range(2):
            panel_copies[3, s, u].start()
            forward(2 - s, s, u).start()
    for n, i in [(0, 1), (1, 2)]:
        relay(n, i)
    complete(0)
    pairs(0, half, 2, 4)
    relay(0, 2)
    relay(1, 3)
    for f in flows:
        if held_back(f):
            @pl.when(p == f[0])
            def _():
                for i in range(cuts // 2, cuts):
                    for h in ((1, 0) if i < cuts - 1 else (0, 1)):
                        z_copy(f, h, i).start()
    turn(2, 4)
    for u in range(2):
        stage_here(1, u)
        for s in range(2):
            forward(1 + s, s, u).start()
    relay(0, 3)

    def take_far(t, i):
        passing = [f[2] for f in relays if passed(f) == t]
        if passing:
            @pl.when(p != passing[0])
            def _():
                far_here(t, i)
        else:
            far_here(t, i)

    def back_copy(f):
        t, j = slots[f[1]].index(f), back[f[0]].index(f)
        return remote(rsrc.at[t], rdst.at[j], parts_sent, parts_here, (f[0], c, l))

    def give_back(t):
        turned = racc[t * half:(t + 1) * half, :].T
        rsrc[t] = jnp.sum(turned.reshape(128 // 8, 8, half), axis=0)
        for q in range(rows):
            if t < len(slots[q]):
                @pl.when(p == q)
                def _():
                    back_copy(slots[q][t]).start()

    depth = max(len(slots[q]) for q in range(rows))
    n_slots = by_row([len(slots[q]) for q in range(rows)])
    middle = half + half // 2

    def take_block(t):
        for i in range(cuts):
            take_far(t, i)
        standardize_far(t, 0, half)

    soon = by_row([2 if any(f[2] == q for f in flows) else 1 for q in range(rows)])
    for i in range(cuts // 2):
        take_far(0, i)
    standardize_far(0, 0, half // 2)
    pairs(half, middle, 0, 4, True)
    for t in range(1, depth):
        @pl.when(jnp.minimum(n_slots, soon) > t)
        def _():
            take_block(t)
            pairs(slot_at(t), slot_at(t) + half, 0, 4, True)

    complete(1)
    for k in direct[2:]:
        for u in range(2):
            stage_here(stage(k, 0), u)
            for s in range(2):
                forward(k, s, u).start()
        complete(stage(k, 0))
    pairs(0, middle, 4, ends - 2)
    for u in range(2):
        stage_here(2, u)
        for s in range(2):
            forward(3, s, u).start()
    turn(4, ends - 2)
    for t in range(1, depth):
        @pl.when(n_slots > t)
        def _():
            @pl.when(soon > t)
            def _():
                pairs(slot_at(t), slot_at(t) + half, 4, ends - 2, True)

            @pl.when(soon <= t)
            def _():
                take_block(t)
                pairs(slot_at(t), slot_at(t) + half, 0, ends - 2, True)

    def part_copy(k, h):
        return remote(psrc.at[2 * k + h], pdst.at[2 * k + l], parts_sent, parts_here, (p, flip(c, k), h))

    def take_last():
        for i in range(cuts // 2, cuts):
            take_far(0, i)
        standardize_far(0, half // 2, half)

    def finish_panel():
        complete(2)
        for t in range(1, depth):
            @pl.when(n_slots > t)
            def _():
                pairs(slot_at(t), slot_at(t) + half, ends - 2, ends)
                give_back(t)

    def send_parts(k):
        for h in (1, 0):
            place = places.index((k, h))
            psrc[2 * k + h] = pacc[:, place * half:(place + 1) * half]
            if k:
                part_copy(k, h).start()

    kind = by_row([2 if any(held_back(f) for f in slots[q]) else 1 if slots[q] and slots[q][0][2] is not None else 0
                   for q in range(rows)])

    @pl.when(kind == 2)
    def _():
        finish_panel()
        pairs(0, middle, ends - 2, ends)
        turn(ends - 2, ends)
        final = 2 * half - piece
        for i in range(cuts // 2, cuts - 1):
            take_far(0, i)
        standardize_far(0, half // 2, half - piece)
        pairs(middle, final, 0, ends, True)
        take_far(0, cuts - 1)
        standardize_far(0, half - piece, half)
        pairs(final, 2 * half, ends - 2, ends, True)
        send_parts(3)
        pairs(final, 2 * half, 0, ends - 2, True)

    @pl.when(kind == 1)
    def _():
        finish_panel()
        take_last()
        pairs(0, 2 * half, ends - 2, ends)
        send_parts(3)
        pairs(middle, 2 * half, 0, ends - 2, True)

    @pl.when(kind == 0)
    def _():
        take_last()
        pairs(middle, 2 * half, 0, ends - 2, True)
        finish_panel()
        pairs(0, 2 * half, ends - 2, ends)
        send_parts(3)

    sums_first = p < rows // 2

    for k in direct:
        send_parts(k)

    @pl.when(jnp.logical_not(sums_first))
    def _():
        give_back(0)

    send_parts(0)
    part_copy(0, other).start()

    @pl.when(sums_first)
    def _():
        give_back(0)

    left(panel.at[pl.ds(0, (2 * cols - 1) * half)], own_sent)
    for q in range(rows):
        @pl.when(p == q)
        def _():
            blocks = len(outs[q]) + len([f for f in relays if f[2] == q])
            if blocks:
                left(praw.at[pl.ds(0, blocks), l], far_sent)
            left(psrc.at[pl.ds(0, 2 * cols - 1 + len(slots[q]))], parts_sent)

    for q in range(rows):
        @pl.when(p == q)
        def _():
            landed(pdst.at[pl.ds(0, 2 * cols - 1 + len(back[q]))], parts_here)
            more = psrc[l] - 1.0 / 8
            for j in range(len(back[q])):
                more = more + rdst[j]
            psrc[l] = more
    total = psrc[l] + pdst[other]
    for n in range(2, 2 * cols):
        total = total + pdst[n]
    out_ref[...] = jnp.sum(total, axis=0)


def solution(mesh):
    rows, cols = mesh.shape["row"], mesh.shape["col"]
    flows = plan(rows)
    depth = max(len([f for f in flows if f[1] == q]) for q in range(rows))
    fan = max(len([f for f in flows if f[0] == q]) for q in range(rows))
    dma = lambda *shape: pltpu.SemaphoreType.DMA(shape)

    def on_device(expression):
        genes, part = expression.shape
        half, samples = genes // 2, 2 * part
        bf16, f32 = jnp.bfloat16, jnp.float32
        summed = pl.pallas_call(
            functools.partial(kernel, rows, cols),
            out_shape=jax.ShapeDtypeStruct((half,), f32),
            in_specs=[pl.BlockSpec(memory_space=pl.ANY)],
            out_specs=pl.BlockSpec(memory_space=pltpu.VMEM),
            scratch_shapes=[
                pltpu.VMEM((cols, 2, genes, part), bf16),
                pltpu.VMEM((cols * genes, samples), bf16),
                pltpu.VMEM((samples, cols * genes), bf16),
                pltpu.VMEM((depth, 2, half, part), bf16),
                pltpu.VMEM(((1 + depth) * half, samples), bf16),
                pltpu.VMEM((8, cols * genes), f32),
                pltpu.VMEM((depth * half, 128), f32),
                pltpu.VMEM((2 * cols + depth, 8, half), f32),
                pltpu.VMEM((2 * cols + fan, 8, half), f32),
                pltpu.VMEM((depth, 8, half), f32),
                pltpu.VMEM((fan, 8, half), f32),
                *[pltpu.SemaphoreType.DMA] * 4,
                dma(cols - 1, 2), dma(cols - 1), dma(depth, 4),
                pltpu.SemaphoreType.DMA,
                pltpu.SemaphoreType.REGULAR((cols - 1,)),
                pltpu.SemaphoreType.REGULAR((max(len([f for f in flows if f[0] == q and f[2] is None]) for q in range(rows)),)),
            ],
            compiler_params=pltpu.CompilerParams(collective_id=0, has_side_effects=True, vmem_limit_bytes=48000000),
        )(pltpu.with_memory_space_constraint(expression, pltpu.HBM))
        return summed

    return jax.shard_map(
        on_device,
        mesh=mesh,
        in_specs=(P(("row", "col"), "layer"),),
        out_specs=P(("row", "col", "layer")),
        check_vma=False,
    )
```

```python
import functools

import jax
import jax.numpy as jnp
from jax import lax
from jax.experimental import pallas as pl
from jax.experimental.pallas import tpu as pltpu
from jax.sharding import PartitionSpec as P

MESH = pl.DeviceIdType.MESH
epsilon = 1e-05


def flip(c, k):
    bit = 1
    while bit <= k:
        if k & bit:
            c = c + bit - 2 * bit * lax.rem(lax.div(c, bit), 2)
        bit *= 2
    return c


def is_above(c, k):
    top = 1 << (k.bit_length() - 1)
    return lax.rem(lax.div(c, top), 2) == 0


def plan(rows):
    if rows == 4:
        return [(3, 1, None), (0, 1, None), (3, 0, 1), (1, 2, None), (0, 2, 1), (2, 3, None)]
    flows = []
    for d in range(1, rows // 2 + 1):
        for s in range(rows if 2 * d < rows else rows // 2):
            flows.append((s, (s + d) % rows, None))
    return flows


def kernel(rows, cols, x_ref, out_ref, praw, panel, across, far_raw, stack, pacc, racc, psrc, pdst, rsrc, rdst,
           ex_sem, own_sent, far_sent, parts_sent,
           pr_sem, fr_sem, zr_sem, parts_here, x_ready, z_ready):
    p, c, l = lax.axis_index("row"), lax.axis_index("col"), lax.axis_index("layer")
    genes, part = x_ref.shape
    half = genes // 2
    cuts = 4
    piece = half // cuts
    samples = 2 * part
    other = 1 - l
    order = [k for k in range(cols) if k != 3] + [3]
    direct = [k for k in range(1, cols) if k != 3]
    last = cols - 1
    places = [(0, 0), (0, 1), (1, 1), (2, 0), (1, 0), (2, 1)] + [(k, s) for k in order[3:] for s in range(2)]
    ends = len(places)
    flows = plan(rows)
    slots = {t: [f for f in flows if f[1] == t] for t in range(rows)}
    outs = {s: [f for f in flows if f[0] == s and f[2] is None] for s in range(rows)}
    back = {s: [f for f in flows if f[0] == s] for s in range(rows)}
    pairs_of = {q: sorted({f[1] for f in flows if f[0] == q} | {f[0] for f in flows if f[1] == q}) for q in range(rows)}

    def held_back(f):
        return rows == 4 and f == (1, 2, None)

    def quick(f):
        return rows == 4 and f in ((0, 1, None), (1, 2, None))

    def remote(src, dst, send, recv, device):
        return pltpu.make_async_remote_copy(
            src_ref=src, dst_ref=dst, send_sem=send, recv_sem=recv, device_id=device, device_id_type=MESH
        )

    def by_row(values):
        value = values[0]
        for q in range(1, rows):
            value = jnp.where(p == q, values[q], value)
        return value

    def at_row(q, condition=True):
        return pl.when(p == q)

    load = pltpu.make_async_copy(x_ref, praw.at[0, l], parts_sent)
    load.start()

    barrier = pltpu.get_barrier_semaphore()

    def greet(device):
        pl.semaphore_signal(barrier, inc=1, device_id=device, device_id_type=MESH)

    alone = jnp.logical_and(p == 0, c == 0)

    @pl.when(jnp.logical_or(alone, l == 1))
    def _():
        greet((p, c, other))

    for k in direct:
        @pl.when(is_above(c, k))
        def _():
            for h in range(2):
                greet((p, flip(c, k), h))
    for q in range(rows):
        above = [t for t in pairs_of[q] if t > q]
        if above or any(quick(f) for f in slots[q]):
            @pl.when(p == q)
            def _():
                for t in above:
                    for h in range(2):
                        greet((t, c, h))
                for f in slots[q]:
                    if quick(f):
                        @pl.when(l == 1)
                        def _():
                            greet((f[0], c, 1))
    greetings = jnp.where(alone, 1, other) + by_row([2 * len([t for t in pairs_of[q] if t < q]) for q in range(rows)])
    for k in direct:
        greetings = greetings + jnp.where(is_above(c, k), 0, 2)

    greetings = greetings + l * by_row([len([f for f in outs[q] if quick(f)]) for q in range(rows)])
    pacc[...] = jnp.zeros_like(pacc)
    racc[...] = jnp.zeros_like(racc)
    pl.semaphore_wait(barrier, greetings)

    @pl.when(l == 0)
    def _():
        for t in range(rows):
            below = [f for f in slots[t] if f[2] is None and f[0] < t]
            if below:
                @pl.when(p == t)
                def _():
                    for f in below:
                        for b in range(2):
                            pl.semaphore_signal(z_ready.at[outs[f[0]].index(f)], inc=2, device_id=(f[0], c, b), device_id_type=MESH)
        for k in direct:
            @pl.when(jnp.logical_not(is_above(c, k)))
            def _():
                for h in range(2):
                    pl.semaphore_signal(x_ready.at[k - 1], inc=1, device_id=(p, flip(c, k), h), device_id_type=MESH)
        pl.semaphore_signal(x_ready.at[2], inc=1, device_id=(p, c, other), device_id_type=MESH)

    load.wait()

    def z_copy(f, h, i):
        source = praw.at[0, l, pl.ds(h * half + i * piece, piece)]
        return remote(source, far_raw.at[slots[f[1]].index(f), l, pl.ds(i * piece, piece)],
                      far_sent, zr_sem.at[slots[f[1]].index(f), i], (f[1], c, h))

    def landed(ref, sem):
        remote(ref, ref, far_sent, sem, (p, c, other)).wait_recv()

    def left(ref, sem):
        remote(ref, ref, sem, zr_sem.at[0, 0], (p, c, other)).wait_send()

    def far_here(t, i):
        landed(far_raw.at[t, :, pl.ds(i * piece, piece)], zr_sem.at[t, i])

    def send_row(f, ask=False):
        ready = z_ready.at[outs[f[0]].index(f)]
        if held_back(f):
            order_of = [(h, i) for h in (1, 0) for i in range(cuts // 2)]
        else:
            order_of = [(h, i) for i in range(cuts) for h in (1, 0)]
        early = order_of.index((0, 0)) if quick(f) else 0
        for n, (h, i) in enumerate(order_of):
            if ask and n in (0, early):
                @pl.when(jnp.logical_or(early == 0, l == (1 if n else 0)))
                def _():
                    pl.semaphore_wait(ready, 2)

            z_copy(f, h, i).start()

    exchange = remote(praw.at[0, l], praw.at[0, l], own_sent, ex_sem, (p, c, other))

    @pl.when(l == 1)
    def _():
        pl.semaphore_wait(x_ready.at[2], 1)

    exchange.start()
    for q in range(rows):
        down = [f for f in outs[q] if f[1] < q]
        if down:
            @pl.when(p == q)
            def _():
                for f in down:
                    send_row(f)

    def stage(k, s):
        return {1: 1 - s, 2: s, 3: 2}.get(k, k - 1)

    def stage_here(n, u):
        if n:
            landed(praw.at[0, l, pl.ds(0, half)], pr_sem.at[2 * n + u - 1])
        elif u == 0:
            landed(praw.at[0, l], pr_sem.at[0])

    def panel_copy(k, s, u):
        at = pl.ds(s * half + u * half // 2, half // 2)
        return remote(praw.at[0, l, at], praw.at[order.index(k), l, at], own_sent, pr_sem.at[max(2 * stage(k, s) + u - 1, 0)],
                      (p, flip(c, k), l))

    def pass_on(s, u):
        source, target = (2, 1) if s == 0 else (1, 2)
        at = pl.ds(s * half + u * half // 2, half // 2)
        return remote(praw.at[order.index(source), l, at], praw.at[last, l, at], own_sent, pr_sem.at[3 + u],
                      (p, flip(c, target), l))

    panel_copies = {(k, s, u): panel_copy(k, s, u) for k in direct for s in range(2) for u in range(2)}
    panel_copies.update({(3, s, u): pass_on(s, u) for s in range(2) for u in range(2)})

    def forward(k, s, u):
        at = praw.at[order.index(k), l, pl.ds(s * half + u * half // 2, half // 2)]
        return remote(at, at, own_sent, fr_sem.at[stage(k, s)], (p, c, other))

    def complete(n):
        landed(praw.at[0, other], fr_sem.at[n])
        for k, s in places:
            if k and stage(k, s) == n:
                standardize(k, s)

    first = {1: (1, 0), 2: (0, 1)}
    for k in direct:
        @pl.when(jnp.logical_not(is_above(c, k)))
        def _():
            for s in first.get(k, (0, 1)):
                for u in range(2):
                    panel_copies[k, s, u].start()
    for k in direct:
        @pl.when(is_above(c, k))
        def _():
            pl.semaphore_wait(x_ready.at[k - 1], 1)
            for s in first.get(k, (0, 1)):
                for u in range(2):
                    panel_copies[k, s, u].start()
    for q in range(rows):
        up = [f for f in outs[q] if f[1] > q]
        if up:
            @pl.when(p == q)
            def _():
                for f in up:
                    send_row(f, ask=True)

    step = 32

    def scale(low, high):
        low, high = low.astype(jnp.float32), high.astype(jnp.float32)
        total = jnp.sum(low, axis=1, keepdims=True) + jnp.sum(high, axis=1, keepdims=True)
        squares = jnp.sum(low * low + high * high, axis=1, keepdims=True)
        average = total / samples
        variance = squares / samples - average * average
        gain = lax.rsqrt(variance + epsilon)
        return (((low - average) * gain).astype(jnp.bfloat16), ((high - average) * gain).astype(jnp.bfloat16))

    def standardize(k, s):
        n, place = order.index(k), places.index((k, s))
        for i in range(half // step):
            at = pl.ds(s * half + i * step, step)
            low, high = scale(praw[n, 0, at, :], praw[n, 1, at, :])
            at = pl.ds(place * half + i * step, step)
            panel[at, 0:part] = low
            panel[at, part:samples] = high

    def slot_at(t):
        return (1 + t) * half

    def standardize_far(t, first, stop):
        for j in range(first // piece, stop // piece):
            at = pl.ds(j * piece, piece)
            low, high = scale(far_raw[t, 0, at, :], far_raw[t, 1, at, :])
            at = pl.ds(slot_at(t) + j * piece, piece)
            stack[at, 0:part] = low
            stack[at, part:samples] = high

    def turn(start, end):
        for at in range(start * half, end * half, 128):
            across[:, at:at + 128] = panel[at:at + 128, :].T

    def pairs(first, stop, start, end, turned=False):
        if turned:
            product = jnp.dot(stack[first:stop, :], across[:, start * half:end * half], preferred_element_type=jnp.float32)
        else:
            product = lax.dot_general(
                stack[first:stop, :], panel[start * half:end * half, :], (((1,), (1,)), ((), ())),
                preferred_element_type=jnp.float32
            )
        shifted = product * (0.5 / samples) + 0.5
        square = shifted * shifted
        fourth = square * square
        eighth = fourth * fourth
        value = eighth * fourth
        width = value.shape[1]
        pacc[:, start * half:end * half] += jnp.sum(value.reshape((stop - first) // 8, 8, width), axis=0)
        skipped = max(half - first, 0)
        if first + skipped < stop:
            value = value[skipped:]
            lanes = value[:, 0:128]
            for j in range(1, width // 128):
                lanes = lanes + value[:, j * 128:(j + 1) * 128]
            racc[first + skipped - half:stop - half, :] += lanes

    exchange.wait_recv()
    for s in range(2):
        standardize(0, s)
    stack[0:half, :] = panel[pl.ds(pl.multiple_of(l * half, half), half), :]
    pairs(0, half, 0, 2)
    turn(0, 2)

    relays = [f for f in flows if f[2] is not None]

    def passed(f):
        return slots[f[2]].index((f[0], f[2], None))

    def relay_copy(f, b, i):
        at, t = pl.ds(i * piece, piece), slots[f[1]].index(f)
        return remote(far_raw.at[passed(f), b, at], far_raw.at[t, b, at],
                      far_sent, zr_sem.at[t, i], (f[1], c, l))

    def relay(n, i):
        for f in relays[n:n + 1]:
            @pl.when(p == f[2])
            def _():
                far_here(passed(f), i)
                for b in range(2):
                    relay_copy(f, b, i).start()

    for n, i in [(1, 0), (0, 0), (1, 1)]:
        relay(n, i)
    for u in range(2):
        stage_here(0, u)
        for s in range(2):
            panel_copies[3, s, u].start()
            forward(2 - s, s, u).start()
    for n, i in [(0, 1), (1, 2)]:
        relay(n, i)
    complete(0)
    pairs(0, half, 2, 4)
    relay(0, 2)
    relay(1, 3)
    for f in flows:
        if held_back(f):
            @pl.when(p == f[0])
            def _():
                for i in range(cuts // 2, cuts):
                    for h in ((1, 0) if i < cuts - 1 else (0, 1)):
                        z_copy(f, h, i).start()
    turn(2, 4)
    for u in range(2):
        stage_here(1, u)
        for s in range(2):
            forward(1 + s, s, u).start()
    relay(0, 3)

    def take_far(t, i):
        passing = [f[2] for f in relays if passed(f) == t]
        if passing:
            @pl.when(p != passing[0])
            def _():
                far_here(t, i)
        else:
            far_here(t, i)

    def back_copy(f):
        t, j = slots[f[1]].index(f), back[f[0]].index(f)
        return remote(rsrc.at[t], rdst.at[j], parts_sent, parts_here, (f[0], c, l))

    def give_back(t):
        turned = racc[t * half:(t + 1) * half, :].T
        rsrc[t] = jnp.sum(turned.reshape(128 // 8, 8, half), axis=0)
        for q in range(rows):
            if t < len(slots[q]):
                @pl.when(p == q)
                def _():
                    back_copy(slots[q][t]).start()

    depth = max(len(slots[q]) for q in range(rows))
    n_slots = by_row([len(slots[q]) for q in range(rows)])
    middle = half + half // 2

    def take_block(t):
        for i in range(cuts):
            take_far(t, i)
        standardize_far(t, 0, half)

    soon = by_row([2 if any(f[2] == q for f in flows) else 1 for q in range(rows)])
    for i in range(cuts // 2):
        take_far(0, i)
    standardize_far(0, 0, half // 2)
    pairs(half, middle, 0, 4, True)
    for t in range(1, depth):
        @pl.when(jnp.minimum(n_slots, soon) > t)
        def _():
            take_block(t)
            pairs(slot_at(t), slot_at(t) + half, 0, 4, True)

    complete(1)
    for k in direct[2:]:
        for u in range(2):
            stage_here(stage(k, 0), u)
            for s in range(2):
                forward(k, s, u).start()
        complete(stage(k, 0))
    pairs(0, middle, 4, ends - 2)
    for u in range(2):
        stage_here(2, u)
        for s in range(2):
            forward(3, s, u).start()
    turn(4, ends - 2)
    for t in range(1, depth):
        @pl.when(n_slots > t)
        def _():
            @pl.when(soon > t)
            def _():
                pairs(slot_at(t), slot_at(t) + half, 4, ends - 2, True)

            @pl.when(soon <= t)
            def _():
                take_block(t)
                pairs(slot_at(t), slot_at(t) + half, 0, ends - 2, True)

    def part_copy(k, h):
        return remote(psrc.at[2 * k + h], pdst.at[2 * k + l], parts_sent, parts_here, (p, flip(c, k), h))

    def take_last():
        for i in range(cuts // 2, cuts):
            take_far(0, i)
        standardize_far(0, half // 2, half)

    def finish_panel():
        complete(2)
        for t in range(1, depth):
            @pl.when(n_slots > t)
            def _():
                pairs(slot_at(t), slot_at(t) + half, ends - 2, ends)
                give_back(t)

    def send_parts(k):
        for h in (1, 0):
            place = places.index((k, h))
            psrc[2 * k + h] = pacc[:, place * half:(place + 1) * half]
            if k:
                part_copy(k, h).start()

    kind = by_row([2 if any(held_back(f) for f in slots[q]) else 1 if slots[q] and slots[q][0][2] is not None else 0
                   for q in range(rows)])

    @pl.when(kind == 2)
    def _():
        finish_panel()
        pairs(0, middle, ends - 2, ends)
        turn(ends - 2, ends)
        final = 2 * half - piece
        for i in range(cuts // 2, cuts - 1):
            take_far(0, i)
        standardize_far(0, half // 2, half - piece)
        pairs(middle, final, 0, ends, True)
        take_far(0, cuts - 1)
        standardize_far(0, half - piece, half)
        pairs(final, 2 * half, ends - 2, ends, True)
        send_parts(3)
        pairs(final, 2 * half, 0, ends - 2, True)

    @pl.when(kind == 1)
    def _():
        finish_panel()
        take_last()
        pairs(0, 2 * half, ends - 2, ends)
        send_parts(3)
        pairs(middle, 2 * half, 0, ends - 2, True)

    @pl.when(kind == 0)
    def _():
        take_last()
        pairs(middle, 2 * half, 0, ends - 2, True)
        finish_panel()
        pairs(0, 2 * half, ends - 2, ends)
        send_parts(3)

    sums_first = p < rows // 2

    for k in direct:
        send_parts(k)

    @pl.when(jnp.logical_not(sums_first))
    def _():
        give_back(0)

    send_parts(0)
    part_copy(0, other).start()

    @pl.when(sums_first)
    def _():
        give_back(0)

    left(panel.at[pl.ds(0, (2 * cols - 1) * half)], own_sent)
    for q in range(rows):
        @pl.when(p == q)
        def _():
            blocks = len(outs[q]) + len([f for f in relays if f[2] == q])
            if blocks:
                left(praw.at[pl.ds(0, blocks), l], far_sent)
            left(psrc.at[pl.ds(0, 2 * cols - 1 + len(slots[q]))], parts_sent)

    for q in range(rows):
        @pl.when(p == q)
        def _():
            landed(pdst.at[pl.ds(0, 2 * cols - 1 + len(back[q]))], parts_here)
            more = psrc[l] - 1.0 / 8
            for j in range(len(back[q])):
                more = more + rdst[j]
            psrc[l] = more
    total = psrc[l] + pdst[other]
    for n in range(2, 2 * cols):
        total = total + pdst[n]
    out_ref[...] = jnp.sum(total, axis=0)


def solution(mesh):
    rows, cols = mesh.shape["row"], mesh.shape["col"]
    flows = plan(rows)
    depth = max(len([f for f in flows if f[1] == q]) for q in range(rows))
    fan = max(len([f for f in flows if f[0] == q]) for q in range(rows))
    dma = lambda *shape: pltpu.SemaphoreType.DMA(shape)

    def on_device(expression):
        genes, part = expression.shape
        half, samples = genes // 2, 2 * part
        bf16, f32 = jnp.bfloat16, jnp.float32
        summed = pl.pallas_call(
            functools.partial(kernel, rows, cols),
            out_shape=jax.ShapeDtypeStruct((half,), f32),
            in_specs=[pl.BlockSpec(memory_space=pl.ANY)],
            out_specs=pl.BlockSpec(memory_space=pltpu.VMEM),
            scratch_shapes=[
                pltpu.VMEM((cols, 2, genes, part), bf16),
                pltpu.VMEM((cols * genes, samples), bf16),
                pltpu.VMEM((samples, cols * genes), bf16),
                pltpu.VMEM((depth, 2, half, part), bf16),
                pltpu.VMEM(((1 + depth) * half, samples), bf16),
                pltpu.VMEM((8, cols * genes), f32),
                pltpu.VMEM((depth * half, 128), f32),
                pltpu.VMEM((2 * cols + depth, 8, half), f32),
                pltpu.VMEM((2 * cols + fan, 8, half), f32),
                pltpu.VMEM((depth, 8, half), f32),
                pltpu.VMEM((fan, 8, half), f32),
                *[pltpu.SemaphoreType.DMA] * 4,
                dma(2 * cols - 3), dma(cols - 1), dma(depth, 4),
                pltpu.SemaphoreType.DMA,
                pltpu.SemaphoreType.REGULAR((cols - 1,)),
                pltpu.SemaphoreType.REGULAR((max(len([f for f in flows if f[0] == q and f[2] is None]) for q in range(rows)),)),
            ],
            compiler_params=pltpu.CompilerParams(collective_id=0, has_side_effects=True, vmem_limit_bytes=48000000),
        )(pltpu.with_memory_space_constraint(expression, pltpu.HBM))
        return summed

    return jax.shard_map(
        on_device,
        mesh=mesh,
        in_specs=(P(("row", "col"), "layer"),),
        out_specs=P(("row", "col", "layer")),
        check_vma=False,
    )
```
